256 devices in a mesh: seq: 32 (over y, z), head: 4 (over x), rep: 2 (over core).
Axes of the slice: x: 4, y: 4, z: 8, core: 2. Of those that a mesh axis runs over, the one named last changes fastest.
Arguments:
- hidden: bfloat16 [65536, 8192], P(('seq', 'rep')), may hold values from -6 to 6
- key_weight: bfloat16 [8192, 1024], P(('seq', 'rep'), 'head'), may hold values from -0.0625 to 0.0625
- value_weight: bfloat16 [8192, 1024], P(('seq', 'rep'), 'head'), may hold values from -0.0625 to 0.0625
- group_scale: float32 [2, 1024], P(None, 'head'), may hold values from 0.05 to 0.4
- new_kv: bfloat16 [4, 256, 2, 1024], P(None, 'seq', None, 'head'), may hold values from -6 to 6
- decode_query: bfloat16 [4, 256, 8192], P(None, 'seq', 'head'), may hold values from -400 to 400
- page_table: int32 [256, 32], replicated, may hold values from 0 to 2047, as said below
- lengths: int32 [256], replicated, may hold values from 1 to 1024
Outputs:
- kv_cache: bfloat16 [65536, 2, 1024], P(('seq', 'rep'), None, 'head')
- smoothing: float32 [1024], P('head')
- attention: bfloat16 [4, 256, 8192], P(None, 'seq', 'head')
The draws below stay inside these ranges and needn't reach their ends.
Inputs may be any that keep to these rules, and one draw needn't show every extreme that they name: `page_table`: page p holds prefilled tokens p * 32 to p * 32 + 31. Slot j of request r is live when j * 32 < lengths[r]. Over the live slots of one parity of j of the 8 requests r with one value of r // 8, at most 2 pages lie in any one block of 32 consecutive pages; this bound is reached.
All inputs are finite; a program needn't handle non-finite values.
Results may differ from the reference program's by a relative error of at most 0.007.
The reference program's roundings to bfloat16 on the way count: a program that leaves them out, or rounds other values in their place, can miss the bound.
Values may be sent and summed in bfloat16 or wider, within the bound.
A program may use at most 128 MiB of HBM per device.

```python
import math
import jax
import jax.numpy as jnp
from jax import lax

D = 8192
KVH = 8
HD = 128
QH = 64
PTOK_DEV = 1024
REQ_DEV = 8
PAGE = 32
MAXPAGES = 32
STEPS = 4
TOKENS = 65536
BATCH = 256
N_SEQ = 32
N_REP = 2


def page_plan(key):
    base_key = jax.random.fold_in(key, 7)
    key_length, key_full, key_order, key_spare, key_page = jax.random.split(base_key, 5)
    groups = N_SEQ
    owners = N_REP
    sources = N_SEQ * N_REP
    pages_dev = PTOK_DEV // PAGE
    entries = REQ_DEV * MAXPAGES
    lengths = jax.random.randint(key_length, (BATCH,), 1, MAXPAGES * PAGE + 1, dtype=jnp.int32)
    full_group = jax.random.randint(key_full, (), 0, groups, dtype=jnp.int32)
    group_of = jnp.arange(BATCH, dtype=jnp.int32) // REQ_DEV
    lengths = jnp.where(group_of == full_group, MAXPAGES * PAGE, lengths).astype(jnp.int32)
    slot_ids = jnp.arange(MAXPAGES, dtype=jnp.int32)
    live_slots = (slot_ids[None, :] * PAGE < lengths[:, None]).reshape(groups, entries)
    owner_of = jnp.broadcast_to(slot_ids % owners, (BATCH, MAXPAGES)).reshape(groups, entries)
    orders = jax.vmap(lambda subkey: jax.random.permutation(subkey, sources))(jax.random.split(key_order, groups * owners))
    orders = orders.reshape(groups, owners, sources).astype(jnp.int32)
    source_ids = jax.random.randint(key_spare, (groups, entries), 0, sources, dtype=jnp.int32)
    for owner_value in range(owners):
        owned_mask = live_slots & (owner_of == owner_value)
        counted = jnp.cumsum(owned_mask.astype(jnp.int32), axis=1) - 1
        picked = jnp.take_along_axis(orders[:, owner_value, :], jnp.maximum(counted, 0) % sources, axis=1)
        source_ids = jnp.where(owned_mask, picked, source_ids)
    within = jax.random.randint(key_page, (groups, entries), 0, pages_dev, dtype=jnp.int32)
    page_ids = (source_ids * pages_dev + within).reshape(BATCH, MAXPAGES).astype(jnp.int32)
    return (page_ids, lengths)


def draw_page_table(key, part):
    return page_plan(key)[0]


def draw_lengths(key, part):
    return page_plan(key)[1]


def draw_decode_query(key, part):
    base_key = jax.random.fold_in(key, 31)
    drawn = jnp.clip(jax.random.normal(base_key, (STEPS, BATCH, QH * HD), jnp.float32), -5.0, 5.0)
    return drawn.astype(jnp.bfloat16)


def shard_levels(key, shape, cuts, low, largest):
    def one(position, shards_of):
        steps = jax.random.uniform(jax.random.fold_in(jax.random.fold_in(key, 6), position), (shards_of,), jnp.float32, low / len(cuts), largest / len(cuts))
        return jnp.repeat(jnp.exp(steps), shape[position] // shards_of).reshape((-1,) + (1,) * (len(shape) - position - 1))

    level = one(*cuts[0])
    for cut in cuts[1:]:
        level = level * one(*cut)
    return level


def normal_values(rng, extent, deviation, bound, shards=(), kind=jnp.bfloat16):
    values = jax.random.normal(rng, extent, jnp.float32) * deviation
    if len(shards) > 0:
        values = shard_levels(rng, extent, shards, -0.22, 0.18) * values
    return jnp.clip(values, min=-bound, max=bound).astype(kind)


def setup_inputs(seed: int = 0) -> dict:
    arg_keys = jax.random.split(jax.random.key(seed), 9)
    hidden = normal_values(arg_keys[0], (TOKENS, D), 1.0, 6.0, ((0, 64),))
    key_weight = normal_values(arg_keys[1], (D, KVH * HD), D ** -0.5, 0.0625, ((0, 64), (1, 4)))
    value_weight = normal_values(arg_keys[2], (D, KVH * HD), D ** -0.5, 0.0625, ((0, 64), (1, 4)))
    group_scale = jnp.clip(jnp.exp(math.log(0.4) - 2.0794415 * jax.random.uniform(arg_keys[3], (2, KVH * HD), jnp.float32) ** shard_levels(arg_keys[3], (2, KVH * HD), ((1, 4),), -0.2, 0.2)), 0.05, 0.4)
    new_kv = normal_values(arg_keys[4], (STEPS, BATCH, 2, KVH * HD), 1.0, 6.0, ((1, 32), (3, 4)))
    decode_query = draw_decode_query(jax.random.fold_in(arg_keys[8], 71), 0)
    page_table = draw_page_table(jax.random.fold_in(arg_keys[8], 71), 0)
    lengths = draw_lengths(jax.random.fold_in(arg_keys[8], 71), 0)
    return dict(hidden=hidden, key_weight=key_weight, value_weight=value_weight, group_scale=group_scale, new_kv=new_kv, decode_query=decode_query, page_table=page_table, lengths=lengths)


EPSILON = 1e-05
NEGATIVE = -1e+30

def clipped(raw_keys, raw_values, smooth, group_scale):
    keys_out = jnp.clip(raw_keys / smooth, -8.0 * group_scale[0], 7.0 * group_scale[0])
    values_out = jnp.clip(raw_values, -8.0 * group_scale[1], 7.0 * group_scale[1])
    return (keys_out, values_out)

def reference(hidden, key_weight, value_weight, group_scale, new_kv, decode_query, page_table, lengths):
    raw_keys = jnp.dot(hidden, key_weight, preferred_element_type=jnp.float32)
    raw_values = jnp.dot(hidden, value_weight, preferred_element_type=jnp.float32)
    smoothing = jnp.sqrt(lax.optimization_barrier(jnp.max(jnp.abs(raw_keys), axis=0)) + EPSILON)
    keys_clip, values_clip = clipped(raw_keys, raw_values, smoothing, group_scale)
    kv_cache = jnp.stack([keys_clip, values_clip], axis=1).astype(jnp.bfloat16)
    fresh_keys, fresh_values = clipped(new_kv[:, :, 0].astype(jnp.float32), new_kv[:, :, 1].astype(jnp.float32), smoothing, group_scale)
    fresh = jnp.stack([fresh_keys, fresh_values], axis=2).astype(jnp.bfloat16)
    group_size = QH // KVH
    smooth_query = jnp.repeat(smoothing.reshape(KVH, HD), group_size, axis=0).reshape(-1)
    queries = (decode_query.astype(jnp.float32) * smooth_query).astype(jnp.bfloat16)
    context = MAXPAGES * PAGE
    offsets = jnp.arange(PAGE, dtype=jnp.int32)
    score_scale = HD ** (-0.5)
    causal = jnp.arange(STEPS)[None, :] <= jnp.arange(STEPS)[:, None]

    def per_request(request_item):
        table_row, length, query_row, fresh_row = request_item
        row_ids = (table_row[:, None] * PAGE + offsets[None, :]).reshape(-1).astype(jnp.int32)
        cache_rows = jnp.take(kv_cache, row_ids, axis=0)
        keys_all = jnp.concatenate([cache_rows[:, 0], fresh_row[:, 0]], axis=0).astype(jnp.float32).reshape(context + STEPS, KVH, HD)
        values_all = jnp.concatenate([cache_rows[:, 1], fresh_row[:, 1]], axis=0).astype(jnp.float32).reshape(context + STEPS, KVH, HD)
        valid_cache = jnp.broadcast_to(jnp.arange(context)[None, :] < length, (STEPS, context))
        valid_keys = jnp.concatenate([valid_cache, causal], axis=1)
        query_heads = query_row.astype(jnp.float32).reshape(STEPS, KVH, group_size, HD)
        scores = jnp.einsum('tkgd,nkd->tkgn', query_heads, keys_all) * score_scale
        key_mask = valid_keys[:, None, None, :]
        scores = jnp.where(key_mask, scores, NEGATIVE)
        row_max = lax.optimization_barrier(jnp.max(scores, axis=-1, keepdims=True))
        expd = jnp.where(key_mask, jnp.exp(scores - row_max), 0.0)
        totals = lax.optimization_barrier(jnp.sum(expd, axis=-1))
        rounded = lax.optimization_barrier(expd.astype(jnp.bfloat16)).astype(jnp.float32)
        summed = jnp.einsum('tkgn,nkd->tkgd', rounded, values_all)
        return (summed / totals[..., None]).reshape(STEPS, QH * HD).astype(jnp.bfloat16)
    per_batch = lax.map(per_request, (page_table, lengths, jnp.swapaxes(queries, 0, 1), jnp.swapaxes(fresh, 0, 1)))
    attention = jnp.swapaxes(per_batch, 0, 1)
    return (kv_cache, smoothing, attention)
```

```python
import functools

import jax
import jax.numpy as jnp
from jax import lax
from jax.experimental import pallas as pl
from jax.experimental.pallas import tpu as pltpu
from jax.sharding import PartitionSpec as P

KVH = 8
HD = 128
QH = 64
PAGE = 32
NY = 4
NZ = 8
CHIPS = NY * NZ


EPSILON = 1e-05
NEGATIVE = -1e30


class Torus:
    def __init__(self):
        seq = lax.axis_index("seq")
        self.y, self.z = lax.div(seq, NZ), lax.rem(seq, NZ)
        self.core = lax.axis_index("rep")

    def at(self, dy, dz):
        y = lax.rem(self.y + (dy + NY), NY)
        z = lax.rem(self.z + (dz + NZ), NZ)
        return y * NZ + z


class Stream:
    def __init__(self, torus, number, block, send_sem, recv_sem, swap):
        self.torus, self.number, self.block = torus, number, block
        self.send_sem, self.recv_sem, self.swap = send_sem, recv_sem, swap

    def copy(self, blk, dy, dz):
        ref = self.block(blk, self.torus.core)
        return pltpu.make_async_remote_copy(
            src_ref=ref,
            dst_ref=ref,
            send_sem=self.send_sem,
            recv_sem=self.recv_sem.at[blk],
            device_id={"seq": self.torus.at(dy, dz)},
            device_id_type=pl.DeviceIdType.MESH,
        )

    def across(self, blk):
        if self.swap is None:
            return
        ref = self.block(blk, self.torus.core)
        pltpu.make_async_remote_copy(
            src_ref=ref,
            dst_ref=ref,
            send_sem=self.swap[0],
            recv_sem=self.swap[1],
            device_id={"rep": 1 - self.torus.core},
            device_id_type=pl.DeviceIdType.MESH,
        ).start()

    def arrived(self, dy, dz):
        blk = self.torus.at(dy, dz)
        self.copy(blk, 1, 0).wait_recv()
        return blk

    def along_z(self, blk, right, left):
        if right:
            self.copy(blk, 0, 1).start()
        if left:
            self.copy(blk, 0, -1).start()

    def along_y(self, blk, up, down):
        if up:
            self.copy(blk, 1, 0).start()
        if down:
            self.copy(blk, -1, 0).start()

    def step_z_first(self, st):
        turn_right = self.number % 2 == 0
        far = -4 if turn_right else 4
        reach = [[0], [-1, 1], [-2, 2], [-3, 3], [far]]
        if st == 0:
            blk = self.torus.at(0, 0)
            self.along_z(blk, True, True)
            self.along_y(blk, True, True)
            self.across(blk)
        if 1 <= st <= 4:
            for dz in reach[st]:
                blk = self.arrived(0, dz)
                onward = st < 3 or (st == 3 and (dz < 0) == turn_right)
                self.along_z(blk, onward and dz < 0, onward and dz > 0)
                self.along_y(blk, True, True)
                self.across(blk)
        if 1 <= st <= 5:
            for dz in reach[st - 1]:
                for dy in (-1, 1):
                    blk = self.arrived(dy, dz)
                    even = dz % 2 == 0
                    self.along_y(blk, even and dy < 0, not even and dy > 0)
                    self.across(blk)
        if 2 <= st <= 6:
            for dz in reach[st - 2]:
                self.across(self.arrived(2, dz))

    def step_y_first(self, st):
        even = self.number % 2 == 0
        if st == 0:
            blk = self.torus.at(0, 0)
            self.along_z(blk, True, True)
            self.along_y(blk, True, True)
            self.across(blk)
        if st == 1:
            for dy in (-1, 1):
                blk = self.arrived(dy, 0)
                self.along_y(blk, even and dy < 0, not even and dy > 0)
                self.along_z(blk, True, True)
                self.across(blk)
        if st == 2:
            blk = self.arrived(2, 0)
            self.along_z(blk, True, True)
            self.across(blk)
        for dy, first in ((0, 0), (-1, 1), (1, 1), (2, 2)):
            k = st - first
            turn_right = (self.number + dy) % 2 == 0
            if 1 <= k <= 3:
                for dz in (-k, k):
                    blk = self.arrived(dy, dz)
                    onward = k < 3 or (dz < 0) == turn_right
                    self.along_z(blk, onward and dz < 0, onward and dz > 0)
                    self.across(blk)
            if k == 4:
                self.across(self.arrived(dy, -4 if turn_right else 4))

    def step(self, st):
        @pl.when(self.torus.core == 0)
        def _():
            self.step_z_first(st)

        @pl.when(self.torus.core == 1)
        def _():
            self.step_y_first(st)

    def swap_copy(self, refs):
        return pltpu.make_async_remote_copy(
            src_ref=refs,
            dst_ref=refs,
            send_sem=self.swap[0],
            recv_sem=self.swap[1],
            device_id={"rep": 1 - self.torus.core},
            device_id_type=pl.DeviceIdType.MESH,
        )

    def sent_copy(self, refs):
        return pltpu.make_async_remote_copy(
            src_ref=refs,
            dst_ref=refs,
            send_sem=self.send_sem,
            recv_sem=self.recv_sem.at[0],
            device_id={"rep": 1 - self.torus.core},
            device_id_type=pl.DeviceIdType.MESH,
        )


STEPS_GATHER = 7


def greet(torus):
    barrier = pltpu.get_barrier_semaphore()
    for dy, dz in ((1, 0), (-1, 0), (0, 1), (0, -1)):
        pl.semaphore_signal(
            barrier,
            inc=1,
            device_id={"seq": torus.at(dy, dz)},
            device_id_type=pl.DeviceIdType.MESH,
        )
    pl.semaphore_signal(
        barrier,
        inc=1,
        device_id={"rep": 1 - torus.core},
        device_id_type=pl.DeviceIdType.MESH,
    )
    pl.semaphore_wait(barrier, 5)


def project_kernel(
    hidden_hbm, wk_hbm, wv_hbm, scale_ref,
    keys_ref, values_ref, smooth_ref,
    hid, wk, wv, mx, acc,
    local_sem, hid_sem, send_sem, recv_sem, swap_sem,
):
    torus = Torus()
    me, core = torus.at(0, 0), torus.core
    tokens = hidden_hbm.shape[0]
    depth = hidden_hbm.shape[1]
    parts = 4
    width = depth // parts
    own_k = pltpu.make_async_copy(wk_hbm, wk.at[me, core], local_sem.at[0])
    own_v = pltpu.make_async_copy(wv_hbm, wv.at[me, core], local_sem.at[1])
    own_k.start()
    own_v.start()
    hid_copies = [
        pltpu.make_async_copy(
            hidden_hbm.at[:, pl.ds(k * width, width)],
            hid.at[:, pl.ds(k * width, width)],
            hid_sem.at[k],
        )
        for k in range(parts)
    ]
    for copy in hid_copies:
        copy.start()
    greet(torus)
    own_k.wait()

    def stream(number, refs, swap=True):
        return Stream(
            torus,
            number,
            lambda blk, c: refs.at[blk, c],
            send_sem.at[number],
            recv_sem.at[number],
            (swap_sem.at[number, 0], swap_sem.at[number, 1]) if swap else None,
        )

    s_k, s_v, s_m = stream(0, wk), stream(1, wv), stream(2, mx)
    rows = 512

    def multiply(weights, out, k):
        if k == 0:
            out[...] = jnp.zeros_like(out)
        blocks = weights.shape[0] // parts

        def one(m, carry):
            at = pl.ds(pl.multiple_of(m * rows, rows), rows)
            w = weights[k * blocks : (k + 1) * blocks].reshape(width, weights.shape[3])
            out[at, :] += jnp.dot(
                hid[at, k * width : (k + 1) * width], w, preferred_element_type=jnp.float32
            )
            return carry

        lax.fori_loop(0, tokens // rows, one, 0)

    lag = {0: 0, 1: 3, 2: 9}
    for i in range(9 + STEPS_GATHER):
        if i == lag[1]:
            own_v.wait()
        for s in (s_k, s_v, s_m):
            st = i - lag[s.number]
            if 0 <= st < STEPS_GATHER:
                s.step(st)
        if i == 6:
            s_k.swap_copy(wk.at[:, 1 - core]).wait_recv()
        if i in (7, 8):
            for k in ((0, 1) if i == 7 else (2, 3)):
                hid_copies[k].wait()
                multiply(wk, acc.at[0], k)
        if i == 8:
            mx[me, core] = jnp.max(
                jnp.abs(acc[0]).reshape(tokens // 8, 8, acc.shape[2]), axis=0
            )
        if i == 9:
            s_v.swap_copy(wv.at[:, 1 - core]).wait_recv()
        if i in (10, 11, 12, 13):
            multiply(wv, acc.at[1], i - 10)
        if i == 14:
            values_ref[...] = jnp.clip(
                acc[1], -8.0 * scale_ref[1:2, :], 7.0 * scale_ref[1:2, :]
            ).astype(jnp.bfloat16)
    s_m.swap_copy(mx.at[:, 1 - core]).wait_recv()
    peak = jnp.max(mx[...].reshape(2 * CHIPS, 8, mx.shape[3]), axis=0)
    smooth = jnp.sqrt(jnp.max(peak, axis=0, keepdims=True) + EPSILON)
    smooth_ref[...] = smooth
    keys_ref[...] = jnp.clip(
        acc[0] / smooth, -8.0 * scale_ref[0:1, :], 7.0 * scale_ref[0:1, :]
    ).astype(jnp.bfloat16)
    for s, refs in ((s_k, wk), (s_v, wv), (s_m, mx)):
        s.sent_copy(refs.at[pl.ds(0, CHIPS - 1), core]).wait_send()
        s.swap_copy(refs.at[:, core]).wait_send()


def project(hidden, key_weight, value_weight, group_scale):
    tokens, depth = hidden.shape
    rows, columns = key_weight.shape
    any_spec = pl.BlockSpec(memory_space=pl.ANY)
    vmem = pl.BlockSpec(memory_space=pltpu.VMEM)
    return pl.pallas_call(
        project_kernel,
        out_shape=(
            jax.ShapeDtypeStruct((tokens, columns), jnp.bfloat16),
            jax.ShapeDtypeStruct((tokens, columns), jnp.bfloat16),
            jax.ShapeDtypeStruct((1, columns), jnp.float32),
        ),
        in_specs=[any_spec, any_spec, any_spec, vmem],
        out_specs=(vmem, vmem, vmem),
        scratch_shapes=[
            pltpu.VMEM((tokens, depth), jnp.bfloat16),
            pltpu.VMEM((CHIPS, 2, rows, columns), jnp.bfloat16),
            pltpu.VMEM((CHIPS, 2, rows, columns), jnp.bfloat16),
            pltpu.VMEM((CHIPS, 2, 8, columns), jnp.float32),
            pltpu.VMEM((2, tokens, columns), jnp.float32),
            pltpu.SemaphoreType.DMA((2,)),
            pltpu.SemaphoreType.DMA((4,)),
            pltpu.SemaphoreType.DMA((3,)),
            pltpu.SemaphoreType.DMA((3, CHIPS)),
            pltpu.SemaphoreType.DMA((3, 2)),
        ],
        compiler_params=pltpu.CompilerParams(
            collective_id=0, has_side_effects=True, vmem_limit_bytes=50 * 2**20
        ),
        name="project",
    )(hidden, key_weight, value_weight, group_scale)


def from_everyone(shard, axis):
    devices = lax.axis_size(axis)
    return lax.all_to_all(
        jnp.broadcast_to(shard[None], (devices, *shard.shape)), axis, 0, 0, tiled=True
    )


def collected_together(shard, axis):
    leaves = jax.tree.leaves(shard)
    order = sorted(range(len(leaves)), key=lambda k: -leaves[k].size)
    width = (1, *leaves[order[0]].shape)[-1]
    lines = [
        jnp.pad(leaves[k].reshape(-1), (0, -leaves[k].size % width)).reshape(-1, width)
        for k in order
    ]
    both, at, found = (from_everyone(jnp.concatenate(lines), axis), 0, {})
    for k, line in zip(order, lines):
        section = both[:, at : at + len(line)].reshape(len(both), -1)
        found[k] = section[:, : leaves[k].size].reshape(-1, *leaves[k].shape)
        at += len(line)
    numbers = iter(range(len(leaves)))
    return jax.tree.map(lambda _: found[next(numbers)], shard)


def combined_pairwise(pieces, combine):
    while len(jax.tree.leaves(pieces)[0]) > 1:
        pieces = jax.vmap(combine)(
            *(jax.tree.map(lambda part: part[side::2], pieces) for side in (0, 1))
        )
    return jax.tree.map(lambda part: part[0], pieces)


def joined_all(shard, axis, combine):
    pieces = collected_together(shard, axis)
    return combined_pairwise(pieces, combine)


def clipped(raw_keys, raw_values, smooth, group_scale):
    keys_out = jnp.clip(raw_keys / smooth, -8.0 * group_scale[0], 7.0 * group_scale[0])
    values_out = jnp.clip(raw_values, -8.0 * group_scale[1], 7.0 * group_scale[1])
    return (keys_out, values_out)


def combine(earlier, latter):
    highest = jnp.maximum(earlier[0], latter[0])
    left_scale = jnp.exp(earlier[0] - highest)
    right_scale = jnp.exp(latter[0] - highest)
    return (
        highest,
        earlier[1] * left_scale + latter[1] * right_scale,
        earlier[2] * left_scale[..., None] + latter[2] * right_scale[..., None],
    )


def on_device(
    hidden, key_weight, value_weight, group_scale, new_kv, decode_query, page_table, lengths
):
    tokens = hidden.shape[0]
    columns = key_weight.shape[1]
    heads_kv = columns // HD
    group_size = QH // KVH
    keys_clip, values_clip, smoothing = project(hidden, key_weight, value_weight, group_scale)
    smoothing = smoothing.reshape(columns)
    kv_cache = jnp.stack([keys_clip, values_clip], axis=1)
    groups = lax.axis_size("seq")
    owners = lax.axis_size("rep")
    sources = groups * owners
    pages_dev = tokens // PAGE
    requests = page_table.shape[0]
    slot_count = page_table.shape[1]
    per_group = requests // groups
    entries = per_group * slot_count
    capacity = entries // (owners * sources)
    page_pool = kv_cache.reshape(pages_dev, PAGE, 2, columns)
    slot_ids = jnp.arange(slot_count, dtype=jnp.int32)
    live_slots = (slot_ids[None, :] * PAGE < lengths[:, None]).reshape(groups, entries)
    owner_of = jnp.broadcast_to(slot_ids % owners, (requests, slot_count)).reshape(groups, entries)
    source_of = (page_table // pages_dev).reshape(groups, entries)
    local_of = (page_table % pages_dev).reshape(groups, entries)
    my_index = lax.axis_index(("seq", "rep"))
    owner_hot = owner_of[:, None, :] == jnp.arange(owners, dtype=jnp.int32)[None, :, None]
    sending = live_slots[:, None, :] & owner_hot & (source_of == my_index)[:, None, :]
    send_rank = jnp.cumsum(sending.astype(jnp.int32), axis=2) - 1
    chosen = sending[:, :, None, :] & (
        send_rank[:, :, None, :] == jnp.arange(capacity, dtype=jnp.int32)[None, None, :, None]
    )
    send_page = jnp.sum(jnp.where(chosen, local_of[:, None, None, :], 0), axis=3)
    send_live = jnp.any(chosen, axis=3)
    outgoing = jnp.where(
        send_live[..., None, None, None], page_pool[send_page], jnp.zeros((), jnp.bfloat16)
    )
    incoming = lax.all_to_all(
        outgoing.reshape((sources,) + outgoing.shape[2:]),
        ("seq", "rep"),
        split_axis=0,
        concat_axis=0,
        tiled=True,
    )
    received = incoming.reshape((sources * capacity,) + incoming.shape[-3:])
    my_group = lax.axis_index("seq")
    my_owner = lax.axis_index("rep")
    mine_table = lax.dynamic_slice_in_dim(page_table, my_group * per_group, per_group, 0)
    mine_length = lax.dynamic_slice_in_dim(lengths, my_group * per_group, per_group, 0)
    half_slots = slot_count // owners
    owned_table = lax.dynamic_index_in_dim(
        mine_table.reshape(per_group, half_slots, owners), my_owner, 2, keepdims=False
    )
    owned_slot = jnp.arange(half_slots, dtype=jnp.int32) * owners + my_owner
    owned_live = owned_slot[None, :] * PAGE < mine_length[:, None]
    owned_source = (owned_table // pages_dev).reshape(-1)
    flat_live = owned_live.reshape(-1)
    source_hot = (
        owned_source[:, None] == jnp.arange(sources, dtype=jnp.int32)[None, :]
    ) & flat_live[:, None]
    running = jnp.cumsum(source_hot.astype(jnp.int32), axis=0)
    arrival = jnp.sum(jnp.where(source_hot, running, 0), axis=1) - 1
    slot_index = jnp.where(flat_live, owned_source * capacity + arrival, 0)
    owned_pages = received[slot_index].reshape(per_group, half_slots * PAGE, 2, columns)
    position = (owned_slot[:, None] * PAGE + jnp.arange(PAGE, dtype=jnp.int32)[None, :]).reshape(-1)
    valid_keys = position[None, :] < mine_length[:, None]
    score_scale = HD ** (-0.5)
    smooth_query = jnp.repeat(smoothing.reshape(heads_kv, HD), group_size, axis=0).reshape(-1)
    queries = (decode_query.astype(jnp.float32) * smooth_query).astype(jnp.bfloat16)
    step_count = queries.shape[0]
    queries = queries.reshape(step_count, per_group, heads_kv, group_size, HD)
    cache_keys = owned_pages[:, :, 0].reshape(per_group, -1, heads_kv, HD)
    cache_values = owned_pages[:, :, 1].reshape(per_group, -1, heads_kv, HD)
    scores = (
        jnp.einsum("trkgd,rnkd->rktgn", queries, cache_keys, preferred_element_type=jnp.float32)
        * score_scale
    )
    key_mask = valid_keys[:, None, None, None, :]
    scores = jnp.where(key_mask, scores, NEGATIVE)
    row_max = jnp.max(scores, axis=-1)
    weights = jnp.where(key_mask, jnp.exp(scores - row_max[..., None]), 0.0)
    row_total = jnp.sum(weights, axis=-1)
    summed = jnp.einsum(
        "rktgn,rnkd->rktgd",
        weights.astype(jnp.bfloat16),
        cache_values,
        preferred_element_type=jnp.float32,
    )
    merged = joined_all((row_max, row_total, summed), "rep", combine)
    fresh_keys, fresh_values = clipped(
        new_kv[:, :, 0].astype(jnp.float32),
        new_kv[:, :, 1].astype(jnp.float32),
        smoothing,
        group_scale,
    )
    fresh_keys = fresh_keys.astype(jnp.bfloat16).reshape(step_count, per_group, heads_kv, HD)
    fresh_values = fresh_values.astype(jnp.bfloat16).reshape(step_count, per_group, heads_kv, HD)
    fresh_scores = (
        jnp.einsum("trkgd,urkd->rktgu", queries, fresh_keys, preferred_element_type=jnp.float32)
        * score_scale
    )
    causal = jnp.arange(step_count)[None, :] <= jnp.arange(step_count)[:, None]
    causal_mask = causal[None, None, :, None, :]
    fresh_scores = jnp.where(causal_mask, fresh_scores, NEGATIVE)
    fresh_max = jnp.max(fresh_scores, axis=-1)
    fresh_weights = jnp.where(causal_mask, jnp.exp(fresh_scores - fresh_max[..., None]), 0.0)
    fresh_total = jnp.sum(fresh_weights, axis=-1)
    fresh_summed = jnp.einsum(
        "rktgu,urkd->rktgd",
        fresh_weights.astype(jnp.bfloat16),
        fresh_values,
        preferred_element_type=jnp.float32,
    )
    final_max, final_total, final_summed = combine(merged, (fresh_max, fresh_total, fresh_summed))
    attention = (final_summed / final_total[..., None]).astype(jnp.bfloat16)
    attention = attention.transpose(2, 0, 1, 3, 4).reshape(
        step_count, per_group, heads_kv * group_size * HD
    )
    return (kv_cache, smoothing, attention)


def solution(mesh):
    placed = (
        P(("seq", "rep"), None),
        P(("seq", "rep"), "head"),
        P(("seq", "rep"), "head"),
        P(None, "head"),
        P(None, "seq", None, "head"),
        P(None, "seq", "head"),
        P(),
        P(),
    )
    return jax.shard_map(
        on_device,
        mesh=mesh,
        in_specs=placed,
        out_specs=(P(("seq", "rep"), None, "head"), P("head"), P(None, "seq", "head")),
        check_vma=False,
    )
```

```python
import functools

import jax
import jax.numpy as jnp
from jax import lax
from jax.experimental import pallas as pl
from jax.experimental.pallas import tpu as pltpu
from jax.sharding import PartitionSpec as P

KVH = 8
HD = 128
QH = 64
PAGE = 32
NY = 4
NZ = 8
CHIPS = NY * NZ


EPSILON = 1e-05
NEGATIVE = -1e30


class Torus:
    def __init__(self):
        seq = lax.axis_index("seq")
        self.y, self.z = lax.div(seq, NZ), lax.rem(seq, NZ)
        self.core = lax.axis_index("rep")

    def at(self, dy, dz):
        y = lax.rem(self.y + (dy + NY), NY)
        z = lax.rem(self.z + (dz + NZ), NZ)
        return y * NZ + z


class Stream:
    def __init__(self, torus, number, block, send_sem, recv_sem, swap):
        self.torus, self.number, self.block = torus, number, block
        self.send_sem, self.recv_sem, self.swap = send_sem, recv_sem, swap

    def copy(self, blk, dy, dz):
        ref = self.block(blk, self.torus.core)
        return pltpu.make_async_remote_copy(
            src_ref=ref,
            dst_ref=ref,
            send_sem=self.send_sem,
            recv_sem=self.recv_sem.at[blk],
            device_id={"seq": self.torus.at(dy, dz)},
            device_id_type=pl.DeviceIdType.MESH,
        )

    def across(self, blk):
        if self.swap is None:
            return
        ref = self.block(blk, self.torus.core)
        pltpu.make_async_remote_copy(
            src_ref=ref,
            dst_ref=ref,
            send_sem=self.swap[0],
            recv_sem=self.swap[1],
            device_id={"rep": 1 - self.torus.core},
            device_id_type=pl.DeviceIdType.MESH,
        ).start()

    def arrived(self, dy, dz):
        blk = self.torus.at(dy, dz)
        self.copy(blk, 1, 0).wait_recv()
        return blk

    def along_z(self, blk, right, left):
        if right:
            self.copy(blk, 0, 1).start()
        if left:
            self.copy(blk, 0, -1).start()

    def along_y(self, blk, up, down):
        if up:
            self.copy(blk, 1, 0).start()
        if down:
            self.copy(blk, -1, 0).start()

    def step_z_first(self, st):
        turn_right = self.number % 2 == 0
        far = -4 if turn_right else 4
        reach = [[0], [-1, 1], [-2, 2], [-3, 3], [far]]
        if st == 0:
            blk = self.torus.at(0, 0)
            self.along_z(blk, True, True)
            self.along_y(blk, True, True)
            self.across(blk)
        if 1 <= st <= 4:
            for dz in reach[st]:
                blk = self.arrived(0, dz)
                onward = st < 3 or (st == 3 and (dz < 0) == turn_right)
                self.along_z(blk, onward and dz < 0, onward and dz > 0)
                self.along_y(blk, True, True)
                self.across(blk)
        if 1 <= st <= 5:
            for dz in reach[st - 1]:
                for dy in (-1, 1):
                    blk = self.arrived(dy, dz)
                    even = dz % 2 == 0
                    self.along_y(blk, even and dy < 0, not even and dy > 0)
                    self.across(blk)
        if 2 <= st <= 6:
            for dz in reach[st - 2]:
                self.across(self.arrived(2, dz))

    def step_y_first(self, st):
        even = self.number % 2 == 0
        if st == 0:
            blk = self.torus.at(0, 0)
            self.along_z(blk, True, True)
            self.along_y(blk, True, True)
            self.across(blk)
        if st == 1:
            for dy in (-1, 1):
                blk = self.arrived(dy, 0)
                self.along_y(blk, even and dy < 0, not even and dy > 0)
                self.along_z(blk, True, True)
                self.across(blk)
        if st == 2:
            blk = self.arrived(2, 0)
            self.along_z(blk, True, True)
            self.across(blk)
        for dy, first in ((0, 0), (-1, 1), (1, 1), (2, 2)):
            k = st - first
            turn_right = (self.number + dy) % 2 == 0
            if 1 <= k <= 3:
                for dz in (-k, k):
                    blk = self.arrived(dy, dz)
                    onward = k < 3 or (dz < 0) == turn_right
                    self.along_z(blk, onward and dz < 0, onward and dz > 0)
                    self.across(blk)
            if k == 4:
                self.across(self.arrived(dy, -4 if turn_right else 4))

    def step(self, st):
        @pl.when(self.torus.core == 0)
        def _():
            self.step_z_first(st)

        @pl.when(self.torus.core == 1)
        def _():
            self.step_y_first(st)

    def swap_copy(self, refs):
        return pltpu.make_async_remote_copy(
            src_ref=refs,
            dst_ref=refs,
            send_sem=self.swap[0],
            recv_sem=self.swap[1],
            device_id={"rep": 1 - self.torus.core},
            device_id_type=pl.DeviceIdType.MESH,
        )

    def sent_copy(self, refs):
        return pltpu.make_async_remote_copy(
            src_ref=refs,
            dst_ref=refs,
            send_sem=self.send_sem,
            recv_sem=self.recv_sem.at[0],
            device_id={"rep": 1 - self.torus.core},
            device_id_type=pl.DeviceIdType.MESH,
        )


STEPS_GATHER = 7
def greet(torus):
    barrier = pltpu.get_barrier_semaphore()
    for dy, dz in ((1, 0), (-1, 0), (0, 1), (0, -1)):
        pl.semaphore_signal(
            barrier,
            inc=1,
            device_id={"seq": torus.at(dy, dz)},
            device_id_type=pl.DeviceIdType.MESH,
        )
    pl.semaphore_signal(
        barrier,
        inc=1,
        device_id={"rep": 1 - torus.core},
        device_id_type=pl.DeviceIdType.MESH,
    )
    pl.semaphore_wait(barrier, 5)


SLOTS = 8


def find_kernel(table_ref, length_ref, found_ref):
    chip = lax.axis_index("seq")
    table = table_ref[...]
    slots, requests = table.shape
    slot = lax.broadcasted_iota(jnp.int32, table.shape, 0)
    lane = lax.broadcasted_iota(jnp.int32, table.shape, 1)
    left = length_ref[...] - slot * PAGE
    mine = ((left > 0) & (table // (2 * PAGE) == chip)).astype(jnp.float32)
    row = lax.broadcasted_iota(jnp.int32, (slots, slots), 0)
    column = lax.broadcasted_iota(jnp.int32, (slots, slots), 1)
    above = jnp.dot(
        (column < row).astype(jnp.float32), mine, preferred_element_type=jnp.float32
    )
    whole = jnp.broadcast_to(jnp.sum(mine, axis=0, keepdims=True), (8, requests))
    a = lax.broadcasted_iota(jnp.int32, (requests, requests), 0)
    b = lax.broadcasted_iota(jnp.int32, (requests, requests), 1)
    same = a // 8 == b // 8
    before = jnp.dot(
        whole, (same & (a < b)).astype(jnp.float32), preferred_element_type=jnp.float32
    )
    rank = jnp.where(mine > 0.0, above + before[0:1], -1.0)
    fields = (
        (lane % 8).astype(jnp.float32),
        (table % (2 * PAGE)).astype(jnp.float32),
        jnp.minimum(left, PAGE).astype(jnp.float32),
    )
    picked = jnp.concatenate(
        [
            jnp.sum(jnp.where(rank == e, field, 0.0), axis=0, keepdims=True)
            for field in fields
            for e in range(SLOTS)
        ],
        axis=0,
    )
    spread = jnp.dot(picked, same.astype(jnp.float32), preferred_element_type=jnp.float32)
    found_ref[...] = spread.astype(jnp.int32)


def find_pages(page_table, lengths):
    requests, slots = page_table.shape
    return pl.pallas_call(
        find_kernel,
        out_shape=jax.ShapeDtypeStruct((3 * SLOTS, requests), jnp.int32),
        name="find_pages",
    )(page_table.T, lengths.reshape(1, requests))


Y_AXIS, Z_AXIS = 0, 1


def below(keys, queries):
    return lax.dot_general(
        keys, queries, (((1,), (1,)), ((), ())), preferred_element_type=jnp.float32
    )


def weighed(values, weights):
    return lax.dot_general(
        values, weights, (((0,), (0,)), ((), ())), preferred_element_type=jnp.float32
    )


def attend(keys, values, queries, mask):
    scores = jnp.where(mask, below(keys, queries) * HD ** (-0.5), NEGATIVE)
    top = jnp.max(scores, axis=0, keepdims=True)
    weights = jnp.where(mask, jnp.exp(scores - top), 0.0)
    total = jnp.sum(weights, axis=0, keepdims=True)
    return top, total, weighed(values, weights.astype(jnp.bfloat16))


def fold(parts):
    top = functools.reduce(jnp.maximum, [p[0] for p in parts])
    scales = [jnp.exp(p[0] - top) for p in parts]
    total = functools.reduce(jnp.add, [p[1] * s for p, s in zip(parts, scales)])
    summed = functools.reduce(jnp.add, [p[2] * s for p, s in zip(parts, scales)])
    return top, total, summed


class Partials:
    def __init__(self, torus, part, stat, out, out_stat, got, got_stat, send_sem, recv_sem):
        self.torus, self.part, self.stat = torus, part, stat
        self.out, self.out_stat = out, out_stat
        self.got, self.got_stat = got, got_stat
        self.send_sem, self.recv_sem = send_sem, recv_sem

    def copies(self, g, axis, way):
        step = 1 - 2 * way
        peer = self.torus.at(step, 0) if axis == Y_AXIS else self.torus.at(0, step)
        return [
            pltpu.make_async_remote_copy(
                src_ref=src.at[g],
                dst_ref=dst.at[axis, way, g],
                send_sem=self.send_sem.at[k],
                recv_sem=self.recv_sem.at[k, axis, way, g],
                device_id={"seq": peer},
                device_id_type=pl.DeviceIdType.MESH,
            )
            for k, (src, dst) in enumerate(
                ((self.out, self.got), (self.out_stat, self.got_stat))
            )
        ]

    def gathered(self, g, arrivals, more=()):
        parts = [(self.stat[g, 0:1], self.stat[g, 1:2], self.part[g]), *more]
        for axis, way in arrivals:
            for copy in self.copies(g, axis, way):
                copy.wait_recv()
            stat = self.got_stat[axis, way, g]
            parts.append((stat[0:1], stat[1:2], self.got[axis, way, g].astype(jnp.float32)))
        return fold(parts) if len(parts) > 1 else parts[0]

    def send(self, dy, dz, arrivals, axis, way):
        g = self.torus.at(dy, dz)
        top, total, summed = self.gathered(g, arrivals)
        self.out[g] = summed.astype(jnp.bfloat16)
        self.out_stat[g] = jnp.concatenate([top, total], axis=0)
        for copy in self.copies(g, axis, way):
            copy.start()

    def y_first(self):
        order = (4, -3, 3, -2, 2, -1, 1, 0)
        up, down = (Y_AXIS, 0), (Y_AXIS, 1)
        for dz in order:
            self.send(2, dz, (), Y_AXIS, dz % 2)
        for dz in order:
            if dz % 2:
                self.send(1, dz, (), *up)
            else:
                self.send(-1, dz, (), *down)
        for dz in order:
            if dz % 2:
                self.send(-1, dz, (down,), *down)
            else:
                self.send(1, dz, (up,), *up)
        self.send(0, 4, (up, down), Z_AXIS, 0)
        self.send(0, -3, (up, down), Z_AXIS, 1)
        for dz in (3, -2, 2, -1, 1):
            way = 0 if dz > 0 else 1
            self.send(0, dz, (up, down, (Z_AXIS, way)), Z_AXIS, way)
    def z_first(self):
        right, left = (Z_AXIS, 0), (Z_AXIS, 1)
        rows = (2, 1, -1, 0)
        for dy in rows:
            self.send(dy, 4, (), Z_AXIS, dy % 2)
        for dy in rows:
            for dz in (3, -3) if dy % 2 else (-3, 3):
                way = 0 if dz > 0 else 1
                self.send(dy, dz, ((Z_AXIS, way),) if way == dy % 2 else (), Z_AXIS, way)
        for k in (2, 1):
            for dy in rows:
                self.send(dy, k, (right,), *right)
                self.send(dy, -k, (left,), *left)
        self.send(2, 0, (right, left), Y_AXIS, 0)
        self.send(-1, 0, (right, left), Y_AXIS, 1)
        self.send(1, 0, (right, left, (Y_AXIS, 0)), Y_AXIS, 0)


def decode_kernel(
    hidden_hbm, wk_hbm, wv_hbm, query_hbm, scale_ref, new_ref, found_ref,
    keys_ref, values_ref, smooth_ref, att_ref,
    hid, wk, wv, mx, qs, acc, kbuf, vbuf, kout, vout, part, stat, out, out_stat, got, got_stat,
    att_out,
    local_sem, hid_sem, send_sem, recv_sem, swap_sem, half_sem, part_send, part_recv,
):
    torus = Torus()
    me, core = torus.at(0, 0), torus.core
    tokens, depth = hidden_hbm.shape
    columns = wk_hbm.shape[1]
    steps_reqs = query_hbm.shape[0]
    half_q = query_hbm.shape[1] // 2
    heads = half_q // HD
    pages = tokens // PAGE
    parts = 4
    width = depth // parts
    own_k = pltpu.make_async_copy(wk_hbm, wk.at[me, core], local_sem.at[0])
    own_v = pltpu.make_async_copy(wv_hbm, wv.at[me, core], local_sem.at[1])
    own_q = pltpu.make_async_copy(
        query_hbm.at[:, pl.ds(pl.multiple_of(core * half_q, half_q), half_q)],
        qs.at[me],
        local_sem.at[2],
    )
    own_k.start()
    own_v.start()
    own_q.start()
    hid_copies = [
        pltpu.make_async_copy(
            hidden_hbm.at[:, pl.ds(k * width, width)],
            hid.at[:, pl.ds(k * width, width)],
            hid_sem.at[k],
        )
        for k in range(parts)
    ]
    for copy in hid_copies:
        copy.start()
    greet(torus)
    own_k.wait()

    def stream(number, block, swap=True):
        return Stream(
            torus,
            number,
            block,
            send_sem.at[number],
            recv_sem.at[number],
            (swap_sem.at[number, 0], swap_sem.at[number, 1]) if swap else None,
        )

    s_k = stream(0, lambda blk, c: wk.at[blk, c])
    s_v = stream(1, lambda blk, c: wv.at[blk, c])
    s_m = stream(2, lambda blk, c: mx.at[blk, c])
    s_q = stream(3, lambda blk, c: qs.at[blk], swap=False)
    rows = 512

    def multiply(weights, to, k):
        if k == 0:
            to[...] = jnp.zeros_like(to)
        blocks = weights.shape[0] // parts

        def one(m, carry):
            at = pl.ds(pl.multiple_of(m * rows, rows), rows)
            w = weights[k * blocks : (k + 1) * blocks].reshape(width, weights.shape[3])
            to[at, :] += jnp.dot(
                hid[at, k * width : (k + 1) * width], w, preferred_element_type=jnp.float32
            )
            return carry

        lax.fori_loop(0, tokens // rows, one, 0)

    mine = pl.ds(pl.multiple_of(core * HD, HD), HD)
    theirs = pl.ds(pl.multiple_of((1 - core) * HD, HD), HD)
    my_pages = pl.ds(pl.multiple_of(core * pages, pages), pages)
    their_pages = pl.ds(pl.multiple_of((1 - core) * pages, pages), pages)

    def half(k, leaving, whole, at):
        return pltpu.make_async_remote_copy(
            src_ref=leaving,
            dst_ref=whole.at[at],
            send_sem=half_sem.at[k, 0],
            recv_sem=half_sem.at[k, 1],
            device_id={"rep": 1 - core},
            device_id_type=pl.DeviceIdType.MESH,
        )

    def share(k, full, whole, leaving):
        leaving[...] = full[:, theirs].reshape(leaving.shape)
        whole[my_pages] = full[:, mine].reshape(leaving.shape)
        half(k, leaving, whole, my_pages).start()

    lag = {0: 0, 1: 3, 2: 9, 3: 6}
    for i in range(9 + STEPS_GATHER):
        if i == lag[1]:
            own_v.wait()
        if i == lag[3]:
            own_q.wait()
        for s in (s_k, s_v, s_q, s_m):
            st = i - lag[s.number]
            if 0 <= st < STEPS_GATHER:
                s.step(st)
        if i == 6:
            s_k.swap_copy(wk.at[:, 1 - core]).wait_recv()
        if i in (7, 8):
            for k in ((0, 1) if i == 7 else (2, 3)):
                hid_copies[k].wait()
                multiply(wk, acc.at[0], k)
        if i == 8:
            mx[me, core] = jnp.max(
                jnp.abs(acc[0]).reshape(tokens // 8, 8, columns), axis=0
            )
        if i == 9:
            s_v.swap_copy(wv.at[:, 1 - core]).wait_recv()
        if i in (10, 11, 12, 13):
            multiply(wv, acc.at[1], i - 10)
        if i == 14:
            values_ref[...] = jnp.clip(
                acc[1], -8.0 * scale_ref[1:2, :], 7.0 * scale_ref[1:2, :]
            ).astype(jnp.bfloat16)
            share(0, values_ref, vbuf, vout)
    s_m.swap_copy(mx.at[:, 1 - core]).wait_recv()
    peak = jnp.max(mx[...].reshape(2 * CHIPS, 8, columns), axis=0)
    smooth = jnp.sqrt(jnp.max(peak, axis=0, keepdims=True) + EPSILON)
    smooth_ref[...] = smooth
    keys_ref[...] = jnp.clip(
        acc[0] / smooth, -8.0 * scale_ref[0:1, :], 7.0 * scale_ref[0:1, :]
    ).astype(jnp.bfloat16)
    share(1, keys_ref, kbuf, kout)

    my_smooth = smooth_ref[:, mine]

    def queries_of(g):
        return jnp.concatenate(
            [
                (qs[g, :, h * HD : (h + 1) * HD].astype(jnp.float32) * my_smooth).astype(
                    jnp.bfloat16
                )
                for h in range(heads)
            ],
            axis=0,
        )

    across = heads * steps_reqs
    lane = lax.broadcasted_iota(jnp.int32, (PAGE, across), 1)
    key = lax.broadcasted_iota(jnp.int32, (PAGE, across), 0)
    request = lane % 8

    fresh_keys = jnp.clip(
        new_ref[:, mine].astype(jnp.float32) / my_smooth,
        -8.0 * scale_ref[0:1, mine],
        7.0 * scale_ref[0:1, mine],
    ).astype(jnp.bfloat16)
    fresh_values = jnp.clip(
        new_ref[:, pl.ds(pl.multiple_of(columns + core * HD, HD), HD)].astype(jnp.float32),
        -8.0 * scale_ref[1:2, mine],
        7.0 * scale_ref[1:2, mine],
    ).astype(jnp.bfloat16)
    fresh_mask = (key % 8 == request) & (key // 8 <= (lane // 8) % (steps_reqs // 8))
    fresh = attend(fresh_keys, fresh_values, queries_of(me), fresh_mask)

    half(0, vout, vbuf, their_pages).wait_recv()
    half(1, kout, kbuf, their_pages).wait_recv()

    def one_group(g):
        keys, values, masks = [], [], []
        for e in range(SLOTS):
            who, page, count = (found_ref[SLOTS * f + e, g * 8] for f in range(3))
            keys.append(kbuf[page])
            values.append(vbuf[page])
            masks.append((request == who) & (key < count))
        top, total, summed = attend(
            jnp.concatenate(keys, axis=0),
            jnp.concatenate(values, axis=0),
            queries_of(g),
            jnp.concatenate(masks, axis=0),
        )
        part[g] = summed
        stat[g] = jnp.concatenate([top, total], axis=0)

    def groups(i, carry):
        one_group(2 * i)
        one_group(2 * i + 1)
        return carry

    lax.fori_loop(0, CHIPS // 2, groups, 0)

    partials = Partials(
        torus, part, stat, out, out_stat, got, got_stat, part_send, part_recv
    )

    @pl.when(core == 0)
    def _():
        partials.y_first()

    @pl.when(core == 1)
    def _():
        partials.z_first()

    top, total, summed = partials.gathered(
        me, ((Y_AXIS, 0), (Y_AXIS, 1), (Z_AXIS, 0), (Z_AXIS, 1)), more=(fresh,)
    )
    done = (summed / total).T.astype(jnp.bfloat16)
    for h in range(heads):
        att_out[:, h * HD : (h + 1) * HD] = done[h * steps_reqs : (h + 1) * steps_reqs]
    own_att = pl.ds(pl.multiple_of(core * half_q, half_q), half_q)
    last = pltpu.make_async_remote_copy(
        src_ref=att_out,
        dst_ref=att_ref.at[:, own_att],
        send_sem=half_sem.at[2, 0],
        recv_sem=half_sem.at[2, 1],
        device_id={"rep": 1 - core},
        device_id_type=pl.DeviceIdType.MESH,
    )
    last.start()
    att_ref[:, own_att] = att_out[...]

    for s, refs in ((s_k, wk), (s_v, wv), (s_m, mx)):
        s.sent_copy(refs.at[pl.ds(0, CHIPS - 1), core]).wait_send()
        s.swap_copy(refs.at[:, core]).wait_send()
    s_q.sent_copy(qs.at[pl.ds(0, CHIPS - 1)]).wait_send()
    half(0, vout, vbuf, my_pages).wait_send()
    half(1, kout, kbuf, my_pages).wait_send()
    for k, refs in enumerate((out, out_stat)):
        pltpu.make_async_remote_copy(
            src_ref=refs.at[pl.ds(0, CHIPS - 1)],
            dst_ref=refs.at[pl.ds(0, CHIPS - 1)],
            send_sem=part_send.at[k],
            recv_sem=part_recv.at[k, 0, 0, 0],
            device_id={"rep": 1 - core},
            device_id_type=pl.DeviceIdType.MESH,
        ).wait_send()
    last.wait()


def decode(hidden, key_weight, value_weight, queries, group_scale, new_kv, found):
    tokens, depth = hidden.shape
    rows, columns = key_weight.shape
    step_reqs, q_columns = queries.shape
    pages = tokens // PAGE
    across = q_columns // 2 // HD * step_reqs
    bf16, f32 = jnp.bfloat16, jnp.float32
    any_spec = pl.BlockSpec(memory_space=pl.ANY)
    vmem = pl.BlockSpec(memory_space=pltpu.VMEM)
    smem = pl.BlockSpec(memory_space=pltpu.SMEM)
    return pl.pallas_call(
        decode_kernel,
        out_shape=(
            jax.ShapeDtypeStruct((tokens, columns), bf16),
            jax.ShapeDtypeStruct((tokens, columns), bf16),
            jax.ShapeDtypeStruct((1, columns), f32),
            jax.ShapeDtypeStruct((step_reqs, q_columns), bf16),
        ),
        in_specs=[any_spec, any_spec, any_spec, any_spec, vmem, vmem, smem],
        out_specs=(vmem, vmem, vmem, vmem),
        scratch_shapes=[
            pltpu.VMEM((tokens, depth), bf16),
            pltpu.VMEM((CHIPS, 2, rows, columns), bf16),
            pltpu.VMEM((CHIPS, 2, rows, columns), bf16),
            pltpu.VMEM((CHIPS, 2, 8, columns), f32),
            pltpu.VMEM((CHIPS, step_reqs, q_columns // 2), bf16),
            pltpu.VMEM((2, tokens, columns), f32),
            pltpu.VMEM((2 * pages, PAGE, HD), bf16),
            pltpu.VMEM((2 * pages, PAGE, HD), bf16),
            pltpu.VMEM((pages, PAGE, HD), bf16),
            pltpu.VMEM((pages, PAGE, HD), bf16),
            pltpu.VMEM((CHIPS, HD, across), f32),
            pltpu.VMEM((CHIPS, 2, across), f32),
            pltpu.VMEM((CHIPS, HD, across), bf16),
            pltpu.VMEM((CHIPS, 2, across), f32),
            pltpu.VMEM((2, 2, CHIPS, HD, across), bf16),
            pltpu.VMEM((2, 2, CHIPS, 2, across), f32),
            pltpu.VMEM((step_reqs, q_columns // 2), bf16),
            pltpu.SemaphoreType.DMA((3,)),
            pltpu.SemaphoreType.DMA((4,)),
            pltpu.SemaphoreType.DMA((4,)),
            pltpu.SemaphoreType.DMA((4, CHIPS)),
            pltpu.SemaphoreType.DMA((3, 2)),
            pltpu.SemaphoreType.DMA((3, 2)),
            pltpu.SemaphoreType.DMA((2,)),
            pltpu.SemaphoreType.DMA((2, 2, 2, CHIPS)),
        ],
        compiler_params=pltpu.CompilerParams(
            collective_id=0, has_side_effects=True, vmem_limit_bytes=60 * 2**20
        ),
        name="decode",
    )(hidden, key_weight, value_weight, queries, group_scale, new_kv, found)


def on_device(
    hidden, key_weight, value_weight, group_scale, new_kv, decode_query, page_table, lengths
):
    steps, requests, q_columns = decode_query.shape
    columns = key_weight.shape[1]
    found = find_pages(page_table, lengths)
    keys, values, smoothing, attention = decode(
        hidden,
        key_weight,
        value_weight,
        decode_query.reshape(steps * requests, q_columns),
        group_scale,
        new_kv.reshape(steps * requests, 2 * columns),
        found,
    )
    kv_cache = jnp.stack([keys, values], axis=1)
    return (
        kv_cache,
        smoothing.reshape(columns),
        attention.reshape(steps, requests, q_columns),
    )


def solution(mesh):
    placed = (
        P(("seq", "rep"), None),
        P(("seq", "rep"), "head"),
        P(("seq", "rep"), "head"),
        P(None, "head"),
        P(None, "seq", None, "head"),
        P(None, "seq", "head"),
        P(),
        P(),
    )
    return jax.shard_map(
        on_device,
        mesh=mesh,
        in_specs=placed,
        out_specs=(P(("seq", "rep"), None, "head"), P("head"), P(None, "seq", "head")),
        check_vma=False,
    )
```

```python
import functools

import jax
import jax.numpy as jnp
from jax import lax
from jax.experimental import pallas as pl
from jax.experimental.pallas import tpu as pltpu
from jax.sharding import PartitionSpec as P

KVH = 8
HD = 128
QH = 64
PAGE = 32
NY = 4
NZ = 8
CHIPS = NY * NZ


EPSILON = 1e-05
NEGATIVE = -1e30


class Torus:
    def __init__(self):
        seq = lax.axis_index("seq")
        self.y, self.z = lax.div(seq, NZ), lax.rem(seq, NZ)
        self.core = lax.axis_index("rep")

    def at(self, dy, dz):
        y = lax.rem(self.y + (dy + NY), NY)
        z = lax.rem(self.z + (dz + NZ), NZ)
        return y * NZ + z


class Stream:
    def __init__(self, torus, number, block, send_sem, recv_sem, swap, both_z=False):
        self.torus, self.number, self.block, self.both_z = torus, number, block, both_z
        self.send_sem, self.recv_sem, self.swap = send_sem, recv_sem, swap

    def copy(self, blk, dy, dz):
        ref = self.block(blk, self.torus.core)
        return pltpu.make_async_remote_copy(
            src_ref=ref,
            dst_ref=ref,
            send_sem=self.send_sem,
            recv_sem=self.recv_sem.at[blk],
            device_id={"seq": self.torus.at(dy, dz)},
            device_id_type=pl.DeviceIdType.MESH,
        )

    def across(self, blk):
        if self.swap is None:
            return
        ref = self.block(blk, self.torus.core)
        pltpu.make_async_remote_copy(
            src_ref=ref,
            dst_ref=ref,
            send_sem=self.swap[0],
            recv_sem=self.swap[1].at[lax.div(blk, NZ)],
            device_id={"rep": 1 - self.torus.core},
            device_id_type=pl.DeviceIdType.MESH,
        ).start()

    def arrived(self, dy, dz):
        blk = self.torus.at(dy, dz)
        self.copy(blk, 1, 0).wait_recv()
        return blk

    def along_z(self, blk, right, left):
        if right:
            self.copy(blk, 0, 1).start()
        if left:
            self.copy(blk, 0, -1).start()

    def along_y(self, blk, up, down):
        if up:
            self.copy(blk, 1, 0).start()
        if down:
            self.copy(blk, -1, 0).start()

    def step_z_first(self, st):
        turn_right = self.number % 2 == 0
        far = -4 if turn_right else 4
        reach = [[0], [-1, 1], [-2, 2], [-3, 3], [far]]
        if st == 0:
            blk = self.torus.at(0, 0)
            self.along_z(blk, True, True)
            self.along_y(blk, True, True)
            self.across(blk)
        if 1 <= st <= 4:
            for dz in reach[st]:
                blk = self.arrived(0, dz)
                onward = st < 3 or (st == 3 and (dz < 0) == turn_right)
                self.along_z(blk, onward and dz < 0, onward and dz > 0)
                self.along_y(blk, True, True)
                self.across(blk)
        if 1 <= st <= 5:
            for dz in reach[st - 1]:
                for dy in (-1, 1):
                    blk = self.arrived(dy, dz)
                    even = dz % 2 == 0
                    self.along_y(blk, even and dy < 0, not even and dy > 0)
                    self.across(blk)
        if 2 <= st <= 6:
            for dz in reach[st - 2]:
                self.across(self.arrived(2, dz))

    def step_y_first(self, st):
        even = self.number % 2 == 0
        if st == 0:
            blk = self.torus.at(0, 0)
            self.along_z(blk, True, True)
            self.along_y(blk, True, True)
            self.across(blk)
        if st == 1:
            for dy in (-1, 1):
                blk = self.arrived(dy, 0)
                self.along_y(blk, even and dy < 0, not even and dy > 0)
                self.along_z(blk, True, True)
                self.across(blk)
        if st == 2:
            blk = self.arrived(2, 0)
            self.along_z(blk, True, True)
            self.across(blk)
        for dy, first in ((0, 0), (-1, 1), (1, 1), (2, 2)):
            k = st - first
            turn_right = (self.number + dy) % 2 == 0
            if 1 <= k <= 3:
                for dz in (-k, k):
                    blk = self.arrived(dy, dz)
                    onward = k < 3 or (dz < 0) == turn_right
                    self.along_z(blk, onward and dz < 0, onward and dz > 0)
                    self.across(blk)
            if k == 4:
                self.across(self.arrived(dy, -4 if turn_right else 4))

    def step(self, st):
        if self.both_z:
            self.step_z_first(st)
            return

        @pl.when(self.torus.core == 0)
        def _():
            self.step_z_first(st)

        @pl.when(self.torus.core == 1)
        def _():
            self.step_y_first(st)

    def swap_copy(self, refs, row=0):
        return pltpu.make_async_remote_copy(
            src_ref=refs,
            dst_ref=refs,
            send_sem=self.swap[0],
            recv_sem=self.swap[1].at[row],
            device_id={"rep": 1 - self.torus.core},
            device_id_type=pl.DeviceIdType.MESH,
        )

    def sent_copy(self, refs):
        return pltpu.make_async_remote_copy(
            src_ref=refs,
            dst_ref=refs,
            send_sem=self.send_sem,
            recv_sem=self.recv_sem.at[0],
            device_id={"rep": 1 - self.torus.core},
            device_id_type=pl.DeviceIdType.MESH,
        )


STEPS_GATHER = 7
QUERY_LAG = 3
def friends(torus):
    ring = [(torus.at(0, dz), torus.core) for dz in (1, -1, 2, -2, 3, -3, 4)]
    ring += [(torus.at(0, dz), 1 - torus.core) for dz in (0, 1, -1, 2, -2, 3, -3, 4)]
    return ring, [(torus.at(dy, 0), torus.core) for dy in (1, -1, 2)]


def greet(torus):
    barrier = pltpu.get_barrier_semaphore()
    ring, column = friends(torus)
    for place, core in ring + column:
        pl.semaphore_signal(
            barrier,
            inc=1,
            device_id={"seq": place, "rep": core},
            device_id_type=pl.DeviceIdType.MESH,
        )
    pl.semaphore_wait(barrier, len(ring) + len(column))


SLOTS = 8


def find_kernel(table_ref, length_ref, found_ref):
    chip = lax.axis_index("seq")
    table = table_ref[...]
    slots, requests = table.shape
    slot = lax.broadcasted_iota(jnp.int32, table.shape, 0)
    lane = lax.broadcasted_iota(jnp.int32, table.shape, 1)
    left = length_ref[...] - slot * PAGE
    mine = ((left > 0) & (table // (2 * PAGE) == chip)).astype(jnp.float32)
    row = lax.broadcasted_iota(jnp.int32, (slots, slots), 0)
    column = lax.broadcasted_iota(jnp.int32, (slots, slots), 1)
    above = jnp.dot(
        (column < row).astype(jnp.float32), mine, preferred_element_type=jnp.float32
    )
    whole = jnp.broadcast_to(jnp.sum(mine, axis=0, keepdims=True), (8, requests))
    a = lax.broadcasted_iota(jnp.int32, (requests, requests), 0)
    b = lax.broadcasted_iota(jnp.int32, (requests, requests), 1)
    same = a // 8 == b // 8
    before = jnp.dot(
        whole, (same & (a < b)).astype(jnp.float32), preferred_element_type=jnp.float32
    )
    rank = jnp.where(mine > 0.0, above + before[0:1], -1.0)
    fields = (
        (lane % 8).astype(jnp.float32),
        (table % (2 * PAGE)).astype(jnp.float32),
        jnp.minimum(left, PAGE).astype(jnp.float32),
    )
    picked = jnp.concatenate(
        [
            jnp.sum(jnp.where(rank == e, field, 0.0), axis=0, keepdims=True)
            for field in fields
            for e in range(SLOTS)
        ],
        axis=0,
    )
    spread = jnp.dot(picked, same.astype(jnp.float32), preferred_element_type=jnp.float32)
    found_ref[...] = spread.astype(jnp.int32)


def find_pages(page_table, lengths):
    requests, slots = page_table.shape
    return pl.pallas_call(
        find_kernel,
        out_shape=jax.ShapeDtypeStruct((3 * SLOTS, requests), jnp.int32),
        name="find_pages",
    )(page_table.T, lengths.reshape(1, requests))


Y_AXIS, Z_AXIS = 0, 1


def below(keys, queries):
    return lax.dot_general(
        keys, queries, (((1,), (1,)), ((), ())), preferred_element_type=jnp.float32
    )


def weighed(values, weights):
    return lax.dot_general(
        values, weights, (((0,), (0,)), ((), ())), preferred_element_type=jnp.float32
    )


def attend(keys, values, queries, mask):
    scores = jnp.where(mask, below(keys, queries) * HD ** (-0.5), NEGATIVE)
    top = jnp.max(scores, axis=0, keepdims=True)
    weights = jnp.where(mask, jnp.exp(scores - top), 0.0)
    total = jnp.sum(weights, axis=0, keepdims=True)
    return top, total, weighed(values, weights.astype(jnp.bfloat16))


def fold(parts):
    top = functools.reduce(jnp.maximum, [p[0] for p in parts])
    scales = [jnp.exp(p[0] - top) for p in parts]
    total = functools.reduce(jnp.add, [p[1] * s for p, s in zip(parts, scales)])
    summed = functools.reduce(jnp.add, [p[2] * s for p, s in zip(parts, scales)])
    return top, total, summed


class Partials:
    def __init__(self, torus, part, stat, out, out_stat, got, got_stat, send_sem, recv_sem):
        self.torus, self.part, self.stat = torus, part, stat
        self.out, self.out_stat = out, out_stat
        self.got, self.got_stat = got, got_stat
        self.send_sem, self.recv_sem = send_sem, recv_sem

    def copies(self, g, axis, way):
        step = 1 - 2 * way
        peer = self.torus.at(step, 0) if axis == Y_AXIS else self.torus.at(0, step)
        return [
            pltpu.make_async_remote_copy(
                src_ref=src.at[g],
                dst_ref=dst.at[axis, way, g],
                send_sem=self.send_sem.at[k],
                recv_sem=self.recv_sem.at[k, axis, way, g],
                device_id={"seq": peer},
                device_id_type=pl.DeviceIdType.MESH,
            )
            for k, (src, dst) in enumerate(
                ((self.out, self.got), (self.out_stat, self.got_stat))
            )
        ]

    def gathered(self, g, arrivals, more=()):
        parts = [(self.stat[g, 0:1], self.stat[g, 1:2], self.part[g]), *more]
        for axis, way in arrivals:
            for copy in self.copies(g, axis, way):
                copy.wait_recv()
            stat = self.got_stat[axis, way, g]
            parts.append((stat[0:1], stat[1:2], self.got[axis, way, g].astype(jnp.float32)))
        return fold(parts) if len(parts) > 1 else parts[0]

    def send(self, dy, dz, arrivals, axis, way):
        g = self.torus.at(dy, dz)
        top, total, summed = self.gathered(g, arrivals)
        self.out[g] = summed.astype(jnp.bfloat16)
        self.out_stat[g] = jnp.concatenate([top, total], axis=0)
        for copy in self.copies(g, axis, way):
            copy.start()

    def y_first(self, attend_to):
        order = (4, -3, 3, -2, 2, -1, 1, 0)
        up, down = (Y_AXIS, 0), (Y_AXIS, 1)

        def row(dy):
            attend_to(NZ, lambda k: self.torus.at(dy, 4 - k))

        row(2)
        for dz in order:
            self.send(2, dz, (), Y_AXIS, dz % 2)
        row(1)
        for dz in order:
            if dz % 2:
                self.send(1, dz, (), *up)
        row(-1)
        for dz in order:
            if dz % 2 == 0:
                self.send(-1, dz, (), *down)
        for dz in order:
            if dz % 2:
                self.send(-1, dz, (down,), *down)
            else:
                self.send(1, dz, (up,), *up)
        row(0)
        self.send(0, 4, (up, down), Z_AXIS, 0)
        self.send(0, -3, (up, down), Z_AXIS, 1)
        for dz in (3, -2, 2, -1, 1):
            way = 0 if dz > 0 else 1
            self.send(0, dz, (up, down, (Z_AXIS, way)), Z_AXIS, way)

    def z_first(self, attend_to):
        right, left = (Z_AXIS, 0), (Z_AXIS, 1)
        rows = (2, 1, -1, 0)

        def columns(dz, count):
            attend_to(
                count,
                lambda k: self.torus.at(
                    2 - lax.rem(k, NY), dz * (1 - 2 * lax.div(k, NY)) if dz else 0
                ),
            )

        columns(4, NY)
        for dy in rows:
            self.send(dy, 4, (), Z_AXIS, dy % 2)
        columns(3, 2 * NY)
        for dy in rows:
            way = 1 - dy % 2
            self.send(dy, -3 if way else 3, (), Z_AXIS, way)
        for dy in rows:
            way = dy % 2
            self.send(dy, -3 if way else 3, ((Z_AXIS, way),), Z_AXIS, way)
        for dz in (2, 1):
            columns(dz, 2 * NY)
            for dy in rows:
                self.send(dy, dz, (right,), *right)
                self.send(dy, -dz, (left,), *left)
        columns(0, NY)
        self.send(2, 0, (right, left), Y_AXIS, 0)
        self.send(-1, 0, (right, left), Y_AXIS, 1)
        self.send(1, 0, (right, left, (Y_AXIS, 0)), Y_AXIS, 0)


def decode_kernel(
    hidden_hbm, wk_hbm, wv_hbm, query_hbm, scale_ref, new_ref, found_ref,
    keys_ref, values_ref, smooth_ref, att_ref,
    hid, wk, wv, mz, my, qs, acc, kbuf, vbuf, kout, vout, part, stat, out, out_stat, got, got_stat,
    att_out,
    local_sem, hid_sem, send_sem, recv_sem, swap_send, swap_recv, peak_sem, half_sem,
    part_send, part_recv,
):
    torus = Torus()
    me, core = torus.at(0, 0), torus.core
    tokens, depth = hidden_hbm.shape
    columns = wk_hbm.shape[1]
    steps_reqs = query_hbm.shape[0]
    half_q = query_hbm.shape[1] // 2
    heads = half_q // HD
    pages = tokens // PAGE
    parts = 4
    width = depth // parts
    own_k = pltpu.make_async_copy(wk_hbm, wk.at[me, core], local_sem.at[0])
    own_v = pltpu.make_async_copy(wv_hbm, wv.at[me, core], local_sem.at[1])
    own_q = [
        pltpu.make_async_copy(
            query_hbm.at[
                pl.ds(k * (steps_reqs // 2), steps_reqs // 2),
                pl.ds(pl.multiple_of(core * half_q, half_q), half_q),
            ],
            qs.at[me, k],
            local_sem.at[2 + k],
        )
        for k in range(2)
    ]
    own_k.start()
    own_v.start()
    for copy in own_q:
        copy.start()
    hid_copies = [
        pltpu.make_async_copy(
            hidden_hbm.at[:, pl.ds(k * width, width)],
            hid.at[:, pl.ds(k * width, width)],
            hid_sem.at[k],
        )
        for k in range(parts)
    ]
    for copy in hid_copies:
        copy.start()
    greet(torus)
    own_k.wait()

    def stream(number, block, swap=True, both_z=False):
        return Stream(
            torus,
            number,
            block,
            send_sem.at[number],
            recv_sem.at[number],
            (swap_send.at[number], swap_recv.at[number]) if swap else None,
            both_z,
        )

    s_k = stream(0, lambda blk, c: wk.at[blk, c])
    s_v = stream(1, lambda blk, c: wv.at[blk, c])
    s_qa = stream(2, lambda blk, c: qs.at[blk, 0], swap=False)
    s_qb = stream(3, lambda blk, c: qs.at[blk, 1], swap=False, both_z=True)
    rows = 512

    def multiply(stream, weights, to, dy):
        y = lax.rem(torus.y + (dy + NY), NY)
        blocks = pl.ds(pl.multiple_of(y * NZ, NZ), NZ)
        stream.swap_copy(weights.at[blocks, 1 - core], y).wait_recv()

        def one(m, carry):
            at = pl.ds(pl.multiple_of(m * rows, rows), rows)
            w = weights[blocks].reshape(width, weights.shape[3])
            product = jnp.dot(
                hid[at, pl.ds(pl.multiple_of(y * width, width), width)],
                w,
                preferred_element_type=jnp.float32,
            )
            to[at, :] = product if dy == 0 else to[at, :] + product
            return carry

        lax.fori_loop(0, tokens // rows, one, 0)

    mine = pl.ds(pl.multiple_of(core * HD, HD), HD)
    theirs = pl.ds(pl.multiple_of((1 - core) * HD, HD), HD)
    my_pages = pl.ds(pl.multiple_of(core * pages, pages), pages)
    their_pages = pl.ds(pl.multiple_of((1 - core) * pages, pages), pages)

    def half(k, leaving, whole, at):
        return pltpu.make_async_remote_copy(
            src_ref=leaving,
            dst_ref=whole.at[at],
            send_sem=half_sem.at[k, 0],
            recv_sem=half_sem.at[k, 1],
            device_id={"rep": 1 - core},
            device_id_type=pl.DeviceIdType.MESH,
        )

    def share(k, full, whole, leaving):
        leaving[...] = full[:, theirs].reshape(leaving.shape)
        whole[my_pages] = full[:, mine].reshape(leaving.shape)
        half(k, leaving, whole, my_pages).start()

    ring, column = friends(torus)
    place = core * NZ + torus.z

    def peak_copy(refs, slot, k, target):
        return pltpu.make_async_remote_copy(
            src_ref=refs.at[slot],
            dst_ref=refs.at[slot],
            send_sem=peak_sem.at[k, 0],
            recv_sem=peak_sem.at[k, 1],
            device_id={"seq": target[0], "rep": target[1]},
            device_id_type=pl.DeviceIdType.MESH,
        )

    def tell(refs, slot, k, peers):
        for target in peers:
            peak_copy(refs, slot, k, target).start()

    def heard(refs, k, peers):
        return peak_copy(refs, pl.ds(0, len(peers)), k, peers[0])

    q_lag = QUERY_LAG
    for i in range(q_lag + STEPS_GATHER):
        if i == 0:
            own_v.wait()
        if i == q_lag:
            for copy in own_q:
                copy.wait()
        for stream_i, start in ((s_k, 0), (s_v, 0), (s_qa, q_lag), (s_qb, q_lag)):
            if 0 <= i - start < STEPS_GATHER:
                stream_i.step(i - start)
        if i == 5:
            for copy in hid_copies:
                copy.wait()
            multiply(s_k, wk, acc.at[0], 0)
            multiply(s_v, wv, acc.at[1], 0)
        if i == 6:
            multiply(s_k, wk, acc.at[0], 1)
            multiply(s_k, wk, acc.at[0], -1)
            multiply(s_k, wk, acc.at[0], 2)
            mz[place] = jnp.max(jnp.abs(acc[0]).reshape(tokens // 8, 8, columns), axis=0)
            tell(mz, place, 0, ring)
        if i == 7:
            multiply(s_v, wv, acc.at[1], 1)
            multiply(s_v, wv, acc.at[1], -1)
        if i == 8:
            heard(mz, 0, ring).wait_recv()
            my[torus.y] = jnp.max(mz[...], axis=0)
            tell(my, torus.y, 1, column)
            multiply(s_v, wv, acc.at[1], 2)
        if i == 9:
            values_ref[...] = jnp.clip(
                acc[1], -8.0 * scale_ref[1:2, :], 7.0 * scale_ref[1:2, :]
            ).astype(jnp.bfloat16)
            share(0, values_ref, vbuf, vout)
    heard(my, 1, column).wait_recv()
    peak = jnp.max(my[...], axis=0)
    smooth = jnp.sqrt(jnp.max(peak, axis=0, keepdims=True) + EPSILON)
    smooth_ref[...] = smooth
    keys_ref[...] = jnp.clip(
        acc[0] / smooth, -8.0 * scale_ref[0:1, :], 7.0 * scale_ref[0:1, :]
    ).astype(jnp.bfloat16)
    share(1, keys_ref, kbuf, kout)

    my_smooth = smooth_ref[:, mine]

    def queries_of(g):
        return jnp.concatenate(
            [
                (
                    qs[g, :, :, h * HD : (h + 1) * HD]
                    .reshape(steps_reqs, HD)
                    .astype(jnp.float32)
                    * my_smooth
                ).astype(jnp.bfloat16)
                for h in range(heads)
            ],
            axis=0,
        )

    across = heads * steps_reqs
    lane = lax.broadcasted_iota(jnp.int32, (PAGE, across), 1)
    key = lax.broadcasted_iota(jnp.int32, (PAGE, across), 0)
    request = lane % 8

    fresh_keys = jnp.clip(
        new_ref[:, mine].astype(jnp.float32) / my_smooth,
        -8.0 * scale_ref[0:1, mine],
        7.0 * scale_ref[0:1, mine],
    ).astype(jnp.bfloat16)
    fresh_values = jnp.clip(
        new_ref[:, pl.ds(pl.multiple_of(columns + core * HD, HD), HD)].astype(jnp.float32),
        -8.0 * scale_ref[1:2, mine],
        7.0 * scale_ref[1:2, mine],
    ).astype(jnp.bfloat16)
    fresh_mask = (key % 8 == request) & (key // 8 <= (lane // 8) % (steps_reqs // 8))
    fresh = attend(fresh_keys, fresh_values, queries_of(me), fresh_mask)

    half(0, vout, vbuf, their_pages).wait_recv()
    half(1, kout, kbuf, their_pages).wait_recv()

    def one_group(g):
        keys, values, masks = [], [], []
        for e in range(SLOTS):
            who, page, count = (found_ref[SLOTS * f + e, g * 8] for f in range(3))
            keys.append(kbuf[page])
            values.append(vbuf[page])
            masks.append((request == who) & (key < count))
        top, total, summed = attend(
            jnp.concatenate(keys, axis=0),
            jnp.concatenate(values, axis=0),
            queries_of(g),
            jnp.concatenate(masks, axis=0),
        )
        part[g] = summed
        stat[g] = jnp.concatenate([top, total], axis=0)

    def attend_to(count, group):
        def two(i, carry):
            one_group(group(2 * i))
            one_group(group(2 * i + 1))
            return carry

        lax.fori_loop(0, count // 2, two, 0)

    partials = Partials(
        torus, part, stat, out, out_stat, got, got_stat, part_send, part_recv
    )

    @pl.when(core == 0)
    def _():
        partials.y_first(attend_to)

    @pl.when(core == 1)
    def _():
        partials.z_first(attend_to)

    top, total, summed = partials.gathered(
        me, ((Y_AXIS, 0), (Y_AXIS, 1), (Z_AXIS, 0), (Z_AXIS, 1)), more=(fresh,)
    )
    done = (summed / total).T.astype(jnp.bfloat16)
    for h in range(heads):
        att_out[:, h * HD : (h + 1) * HD] = done[h * steps_reqs : (h + 1) * steps_reqs]
    own_att = pl.ds(pl.multiple_of(core * half_q, half_q), half_q)
    last = pltpu.make_async_remote_copy(
        src_ref=att_out,
        dst_ref=att_ref.at[:, own_att],
        send_sem=half_sem.at[2, 0],
        recv_sem=half_sem.at[2, 1],
        device_id={"rep": 1 - core},
        device_id_type=pl.DeviceIdType.MESH,
    )
    last.start()
    att_ref[:, own_att] = att_out[...]

    for s, refs in ((s_k, wk), (s_v, wv)):
        s.sent_copy(refs.at[pl.ds(0, CHIPS - 1), core]).wait_send()
        s.swap_copy(refs.at[:, core]).wait_send()
    s_qa.sent_copy(qs.at[pl.ds(0, CHIPS - 1), 0]).wait_send()
    s_qb.sent_copy(qs.at[pl.ds(0, CHIPS - 1), 1]).wait_send()
    heard(mz, 0, ring).wait_send()
    heard(my, 1, column).wait_send()
    half(0, vout, vbuf, my_pages).wait_send()
    half(1, kout, kbuf, my_pages).wait_send()
    for k, refs in enumerate((out, out_stat)):
        pltpu.make_async_remote_copy(
            src_ref=refs.at[pl.ds(0, CHIPS - 1)],
            dst_ref=refs.at[pl.ds(0, CHIPS - 1)],
            send_sem=part_send.at[k],
            recv_sem=part_recv.at[k, 0, 0, 0],
            device_id={"rep": 1 - core},
            device_id_type=pl.DeviceIdType.MESH,
        ).wait_send()
    last.wait()


def decode(hidden, key_weight, value_weight, queries, group_scale, new_kv, found):
    tokens, depth = hidden.shape
    rows, columns = key_weight.shape
    step_reqs, q_columns = queries.shape
    pages = tokens // PAGE
    across = q_columns // 2 // HD * step_reqs
    bf16, f32 = jnp.bfloat16, jnp.float32
    any_spec = pl.BlockSpec(memory_space=pl.ANY)
    vmem = pl.BlockSpec(memory_space=pltpu.VMEM)
    smem = pl.BlockSpec(memory_space=pltpu.SMEM)
    return pl.pallas_call(
        decode_kernel,
        out_shape=(
            jax.ShapeDtypeStruct((tokens, columns), bf16),
            jax.ShapeDtypeStruct((tokens, columns), bf16),
            jax.ShapeDtypeStruct((1, columns), f32),
            jax.ShapeDtypeStruct((step_reqs, q_columns), bf16),
        ),
        in_specs=[any_spec, any_spec, any_spec, any_spec, vmem, vmem, smem],
        out_specs=(vmem, vmem, vmem, vmem),
        scratch_shapes=[
            pltpu.VMEM((tokens, depth), bf16),
            pltpu.VMEM((CHIPS, 2, rows, columns), bf16),
            pltpu.VMEM((CHIPS, 2, rows, columns), bf16),
            pltpu.VMEM((2 * NZ, 8, columns), f32),
            pltpu.VMEM((NY, 8, columns), f32),
            pltpu.VMEM((CHIPS, 2, step_reqs // 2, q_columns // 2), bf16),
            pltpu.VMEM((2, tokens, columns), f32),
            pltpu.VMEM((2 * pages, PAGE, HD), bf16),
            pltpu.VMEM((2 * pages, PAGE, HD), bf16),
            pltpu.VMEM((pages, PAGE, HD), bf16),
            pltpu.VMEM((pages, PAGE, HD), bf16),
            pltpu.VMEM((CHIPS, HD, across), f32),
            pltpu.VMEM((CHIPS, 2, across), f32),
            pltpu.VMEM((CHIPS, HD, across), bf16),
            pltpu.VMEM((CHIPS, 2, across), f32),
            pltpu.VMEM((2, 2, CHIPS, HD, across), bf16),
            pltpu.VMEM((2, 2, CHIPS, 2, across), f32),
            pltpu.VMEM((step_reqs, q_columns // 2), bf16),
            pltpu.SemaphoreType.DMA((4,)),
            pltpu.SemaphoreType.DMA((4,)),
            pltpu.SemaphoreType.DMA((4,)),
            pltpu.SemaphoreType.DMA((4, CHIPS)),
            pltpu.SemaphoreType.DMA((2,)),
            pltpu.SemaphoreType.DMA((2, NY)),
            pltpu.SemaphoreType.DMA((2, 2)),
            pltpu.SemaphoreType.DMA((3, 2)),
            pltpu.SemaphoreType.DMA((2,)),
            pltpu.SemaphoreType.DMA((2, 2, 2, CHIPS)),
        ],
        compiler_params=pltpu.CompilerParams(
            collective_id=0, has_side_effects=True, vmem_limit_bytes=60 * 2**20
        ),
        name="decode",
    )(hidden, key_weight, value_weight, queries, group_scale, new_kv, found)


def finish_kernel(keys, values, smooth, att, cache_ref, smooth_ref, att_ref):
    cache_ref[:, 0, :] = keys[...]
    cache_ref[:, 1, :] = values[...]
    smooth_ref[...] = smooth[...]
    att_ref[...] = att[...]


def finish(keys, values, smooth, att):
    tokens, columns = keys.shape
    tiles = 4
    rows, wide = tokens // tiles, att.shape[1] // tiles
    return pl.pallas_call(
        finish_kernel,
        grid=(tiles,),
        out_shape=(
            jax.ShapeDtypeStruct((tokens, 2, columns), keys.dtype),
            jax.ShapeDtypeStruct(smooth.shape, smooth.dtype),
            jax.ShapeDtypeStruct(att.shape, att.dtype),
        ),
        in_specs=[
            pl.BlockSpec((rows, columns), lambda i: (i, 0)),
            pl.BlockSpec((rows, columns), lambda i: (i, 0)),
            pl.BlockSpec(smooth.shape, lambda i: (0, 0)),
            pl.BlockSpec((att.shape[0], wide), lambda i: (0, i)),
        ],
        out_specs=(
            pl.BlockSpec((rows, 2, columns), lambda i: (i, 0, 0)),
            pl.BlockSpec(smooth.shape, lambda i: (0, 0)),
            pl.BlockSpec((att.shape[0], wide), lambda i: (0, i)),
        ),
        name="finish",
    )(keys, values, smooth, att)


def on_device(
    hidden, key_weight, value_weight, group_scale, new_kv, decode_query, page_table, lengths
):
    steps, requests, q_columns = decode_query.shape
    columns = key_weight.shape[1]
    found = find_pages(page_table, lengths)
    keys, values, smoothing, attention = decode(
        hidden,
        key_weight,
        value_weight,
        decode_query.reshape(steps * requests, q_columns),
        group_scale,
        new_kv.reshape(steps * requests, 2 * columns),
        found,
    )
    kv_cache, smoothing, attention = finish(keys, values, smoothing, attention)
    return (
        kv_cache,
        smoothing.reshape(columns),
        attention.reshape(steps, requests, q_columns),
    )


def solution(mesh):
    placed = (
        P(("seq", "rep"), None),
        P(("seq", "rep"), "head"),
        P(("seq", "rep"), "head"),
        P(None, "head"),
        P(None, "seq", None, "head"),
        P(None, "seq", "head"),
        P(),
        P(),
    )
    return jax.shard_map(
        on_device,
        mesh=mesh,
        in_specs=placed,
        out_specs=(P(("seq", "rep"), None, "head"), P("head"), P(None, "seq", "head")),
        check_vma=False,
    )
```

```python
import functools

import jax
import jax.numpy as jnp
from jax import lax
from jax.experimental import pallas as pl
from jax.experimental.pallas import tpu as pltpu
from jax.sharding import PartitionSpec as P

KVH = 8
HD = 128
QH = 64
PAGE = 32
NY = 4
NZ = 8
CHIPS = NY * NZ


EPSILON = 1e-05
NEGATIVE = -1e30


class Torus:
    def __init__(self):
        seq = lax.axis_index("seq")
        self.y, self.z = lax.div(seq, NZ), lax.rem(seq, NZ)
        self.core = lax.axis_index("rep")

    def at(self, dy, dz):
        y = lax.rem(self.y + (dy + NY), NY)
        z = lax.rem(self.z + (dz + NZ), NZ)
        return y * NZ + z


class Stream:
    def __init__(self, torus, number, block, send_sem, recv_sem, swap, both_z=False):
        self.torus, self.number, self.block, self.both_z = torus, number, block, both_z
        self.send_sem, self.recv_sem, self.swap = send_sem, recv_sem, swap

    def copy(self, blk, dy, dz):
        ref = self.block(blk, self.torus.core)
        return pltpu.make_async_remote_copy(
            src_ref=ref,
            dst_ref=ref,
            send_sem=self.send_sem,
            recv_sem=self.recv_sem.at[blk],
            device_id={"seq": self.torus.at(dy, dz)},
            device_id_type=pl.DeviceIdType.MESH,
        )

    def across(self, blk):
        if self.swap is None:
            return
        ref = self.block(blk, self.torus.core)
        pltpu.make_async_remote_copy(
            src_ref=ref,
            dst_ref=ref,
            send_sem=self.swap[0],
            recv_sem=self.swap[1].at[lax.div(blk, NZ)],
            device_id={"rep": 1 - self.torus.core},
            device_id_type=pl.DeviceIdType.MESH,
        ).start()

    def arrived(self, dy, dz):
        blk = self.torus.at(dy, dz)
        self.copy(blk, 1, 0).wait_recv()
        return blk

    def along_z(self, blk, right, left):
        if right:
            self.copy(blk, 0, 1).start()
        if left:
            self.copy(blk, 0, -1).start()

    def along_y(self, blk, up, down):
        if up:
            self.copy(blk, 1, 0).start()
        if down:
            self.copy(blk, -1, 0).start()

    def step_z_first(self, st):
        turn_right = self.number % 2 == 0
        far = -4 if turn_right else 4
        reach = [[0], [-1, 1], [-2, 2], [-3, 3], [far]]
        if st == 0:
            blk = self.torus.at(0, 0)
            self.along_z(blk, True, True)
            self.along_y(blk, True, True)
            self.across(blk)
        if 1 <= st <= 4:
            for dz in reach[st]:
                blk = self.arrived(0, dz)
                onward = st < 3 or (st == 3 and (dz < 0) == turn_right)
                self.along_z(blk, onward and dz < 0, onward and dz > 0)
                self.along_y(blk, True, True)
                self.across(blk)
        if 1 <= st <= 5:
            for dz in reach[st - 1]:
                for dy in (-1, 1):
                    blk = self.arrived(dy, dz)
                    even = dz % 2 == 0
                    self.along_y(blk, even and dy < 0, not even and dy > 0)
                    self.across(blk)
        if 2 <= st <= 6:
            for dz in reach[st - 2]:
                self.across(self.arrived(2, dz))

    def step_y_first(self, st):
        even = self.number % 2 == 0
        if st == 0:
            blk = self.torus.at(0, 0)
            self.along_z(blk, True, True)
            self.along_y(blk, True, True)
            self.across(blk)
        if st == 1:
            for dy in (-1, 1):
                blk = self.arrived(dy, 0)
                self.along_y(blk, even and dy < 0, not even and dy > 0)
                self.along_z(blk, True, True)
                self.across(blk)
        if st == 2:
            blk = self.arrived(2, 0)
            self.along_z(blk, True, True)
            self.across(blk)
        for dy, first in ((0, 0), (-1, 1), (1, 1), (2, 2)):
            k = st - first
            turn_right = (self.number + dy) % 2 == 0
            if 1 <= k <= 3:
                for dz in (-k, k):
                    blk = self.arrived(dy, dz)
                    onward = k < 3 or (dz < 0) == turn_right
                    self.along_z(blk, onward and dz < 0, onward and dz > 0)
                    self.across(blk)
            if k == 4:
                self.across(self.arrived(dy, -4 if turn_right else 4))

    def step(self, st):
        if self.both_z:
            self.step_z_first(st)
            return

        @pl.when(self.torus.core == 0)
        def _():
            self.step_z_first(st)

        @pl.when(self.torus.core == 1)
        def _():
            self.step_y_first(st)

    def swap_copy(self, refs, row=0):
        return pltpu.make_async_remote_copy(
            src_ref=refs,
            dst_ref=refs,
            send_sem=self.swap[0],
            recv_sem=self.swap[1].at[row],
            device_id={"rep": 1 - self.torus.core},
            device_id_type=pl.DeviceIdType.MESH,
        )

    def sent_copy(self, refs):
        return pltpu.make_async_remote_copy(
            src_ref=refs,
            dst_ref=refs,
            send_sem=self.send_sem,
            recv_sem=self.recv_sem.at[0],
            device_id={"rep": 1 - self.torus.core},
            device_id_type=pl.DeviceIdType.MESH,
        )


STEPS_GATHER = 7
QUERY_LAG = 2
def friends(torus):
    ring = [(torus.at(0, dz), torus.core) for dz in (1, -1, 2, -2, 3, -3, 4)]
    ring += [(torus.at(0, dz), 1 - torus.core) for dz in (0, 1, -1, 2, -2, 3, -3, 4)]
    return ring, [(torus.at(dy, 0), torus.core) for dy in (1, -1, 2)]


def greet(torus):
    barrier = pltpu.get_barrier_semaphore()
    ring, column = friends(torus)
    for place, core in ring + column:
        pl.semaphore_signal(
            barrier,
            inc=1,
            device_id={"seq": place, "rep": core},
            device_id_type=pl.DeviceIdType.MESH,
        )
    pl.semaphore_wait(barrier, len(ring) + len(column))


SLOTS = 8


def find_kernel(table_ref, length_ref, found_ref):
    chip = lax.axis_index("seq")
    table = table_ref[...]
    slots, requests = table.shape
    slot = lax.broadcasted_iota(jnp.int32, table.shape, 0)
    lane = lax.broadcasted_iota(jnp.int32, table.shape, 1)
    left = length_ref[...] - slot * PAGE
    mine = ((left > 0) & (table // (2 * PAGE) == chip)).astype(jnp.float32)
    row = lax.broadcasted_iota(jnp.int32, (slots, slots), 0)
    column = lax.broadcasted_iota(jnp.int32, (slots, slots), 1)
    above = jnp.dot(
        (column < row).astype(jnp.float32), mine, preferred_element_type=jnp.float32
    )
    whole = jnp.broadcast_to(jnp.sum(mine, axis=0, keepdims=True), (8, requests))
    a = lax.broadcasted_iota(jnp.int32, (requests, requests), 0)
    b = lax.broadcasted_iota(jnp.int32, (requests, requests), 1)
    same = a // 8 == b // 8
    before = jnp.dot(
        whole, (same & (a < b)).astype(jnp.float32), preferred_element_type=jnp.float32
    )
    rank = jnp.where(mine > 0.0, above + before[0:1], -1.0)
    fields = (
        (lane % 8).astype(jnp.float32),
        (table % (2 * PAGE)).astype(jnp.float32),
        jnp.minimum(left, PAGE).astype(jnp.float32),
    )
    picked = jnp.concatenate(
        [
            jnp.sum(jnp.where(rank == e, field, 0.0), axis=0, keepdims=True)
            for field in fields
            for e in range(SLOTS)
        ],
        axis=0,
    )
    spread = jnp.dot(picked, same.astype(jnp.float32), preferred_element_type=jnp.float32)
    found_ref[...] = spread.astype(jnp.int32)


def find_pages(page_table, lengths):
    requests, slots = page_table.shape
    return pl.pallas_call(
        find_kernel,
        out_shape=jax.ShapeDtypeStruct((3 * SLOTS, requests), jnp.int32),
        name="find_pages",
    )(page_table.T, lengths.reshape(1, requests))


Y_AXIS, Z_AXIS = 0, 1


def below(keys, queries):
    return lax.dot_general(
        keys, queries, (((1,), (1,)), ((), ())), preferred_element_type=jnp.float32
    )


def weighed(values, weights):
    return lax.dot_general(
        values, weights, (((0,), (0,)), ((), ())), preferred_element_type=jnp.float32
    )


def attend(keys, values, queries, mask):
    scores = jnp.where(mask, below(keys, queries) * HD ** (-0.5), NEGATIVE)
    top = jnp.max(scores, axis=0, keepdims=True)
    weights = jnp.where(mask, jnp.exp(scores - top), 0.0)
    total = jnp.sum(weights, axis=0, keepdims=True)
    return top, total, weighed(values, weights.astype(jnp.bfloat16))


def fold(parts):
    top = functools.reduce(jnp.maximum, [p[0] for p in parts])
    scales = [jnp.exp(p[0] - top) for p in parts]
    total = functools.reduce(jnp.add, [p[1] * s for p, s in zip(parts, scales)])
    summed = functools.reduce(jnp.add, [p[2] * s for p, s in zip(parts, scales)])
    return top, total, summed


class Partials:
    def __init__(self, torus, part, stat, out, out_stat, got, got_stat, send_sem, recv_sem):
        self.torus, self.part, self.stat = torus, part, stat
        self.out, self.out_stat = out, out_stat
        self.got, self.got_stat = got, got_stat
        self.send_sem, self.recv_sem = send_sem, recv_sem

    def copies(self, g, axis, way, slot=None, peer=None):
        step = 1 - 2 * way
        if peer is None:
            peer = self.torus.at(step, 0) if axis == Y_AXIS else self.torus.at(0, step)
        slot = g if slot is None else slot
        return [
            pltpu.make_async_remote_copy(
                src_ref=src.at[g],
                dst_ref=dst.at[axis, way, slot],
                send_sem=self.send_sem.at[k],
                recv_sem=self.recv_sem.at[k, axis, way, slot],
                device_id={"seq": peer},
                device_id_type=pl.DeviceIdType.MESH,
            )
            for k, (src, dst) in enumerate(
                ((self.out, self.got), (self.out_stat, self.got_stat))
            )
        ]

    def kept(self, at):
        return self.stat[at, 0:1], self.stat[at, 1:2], self.part[at]

    def keep(self, at, top, total, summed):
        self.part[at] = summed
        self.stat[at] = jnp.concatenate([top, total], axis=0)

    def gathered(self, g, arrivals, more=()):
        parts = [self.kept(g), *more]
        for axis, way, *direct in arrivals:
            slot = direct[0] if direct else g
            for copy in self.copies(g, axis, way, slot):
                copy.wait_recv()
            stat = self.got_stat[axis, way, slot]
            parts.append((stat[0:1], stat[1:2], self.got[axis, way, slot].astype(jnp.float32)))
        return fold(parts) if len(parts) > 1 else parts[0]

    def send(self, dy, dz, arrivals, axis, way, slot=None, peer=None):
        g = self.torus.at(dy, dz)
        top, total, summed = self.gathered(g, arrivals)
        self.out[g] = summed.astype(jnp.bfloat16)
        self.out_stat[g] = jnp.concatenate([top, total], axis=0)
        for copy in self.copies(g, axis, way, slot, peer):
            copy.start()

    def finish(self, arrivals, fresh):
        me = self.torus.at(0, 0)
        self.keep(me, *self.gathered(me, arrivals, more=(self.kept(fresh),)))

    def y_first(self, attend_to, chores):
        order = (4, -3, 3, -2, 2, -1, 1, 0)
        up, down = (Y_AXIS, 0), (Y_AXIS, 1)

        def row(dy):
            attend_to(NZ, lambda k: self.torus.at(dy, 4 - k))

        row(2)
        for dz in order:
            self.send(2, dz, (), Y_AXIS, dz % 2)
        row(1)
        for dz in order:
            if dz % 2:
                self.send(1, dz, (), *up)
        row(-1)
        for dz in order:
            if dz % 2 == 0:
                self.send(-1, dz, (), *down)
        for dz in order:
            if dz % 2:
                self.send(-1, dz, (down,), *down)
            else:
                self.send(1, dz, (up,), *up)
        row(0)
        me = self.torus.at(0, 0)
        for dz in order[:-1]:
            self.send(0, dz, (up, down), Z_AXIS, 0, me, self.torus.at(0, dz))
        for chore in chores:
            chore()
        straight = [(Z_AXIS, 0, self.torus.at(0, dz)) for dz in (1, -1, 2, -2, 3, -3, 4)]
        self.finish((up, down, *straight), CHIPS)

    def z_first(self, attend_to, chores):
        right, left = (Z_AXIS, 0), (Z_AXIS, 1)
        rows = (2, 1, -1, 0)

        def columns(dz, count):
            attend_to(
                count,
                lambda k: self.torus.at(
                    2 - lax.rem(k, NY), dz * (1 - 2 * lax.div(k, NY)) if dz else 0
                ),
            )

        columns(4, NY)
        for dy in rows:
            self.send(dy, 4, (), Z_AXIS, dy % 2)
        columns(3, 2 * NY)
        for dy in rows:
            way = 1 - dy % 2
            self.send(dy, -3 if way else 3, (), Z_AXIS, way)
        for dy in rows:
            way = dy % 2
            self.send(dy, -3 if way else 3, ((Z_AXIS, way),), Z_AXIS, way)
        for dz in (2, 1):
            columns(dz, 2 * NY)
            for dy in rows:
                self.send(dy, dz, (right,), *right)
                self.send(dy, -dz, (left,), *left)
        columns(0, NY)
        chores[0]()
        self.send(2, 0, (right, left), Y_AXIS, 0)
        self.send(-1, 0, (right, left), Y_AXIS, 1)
        for chore in chores[1:3]:
            chore()
        self.send(1, 0, (right, left, (Y_AXIS, 0)), Y_AXIS, 0)
        for chore in chores[3:]:
            chore()
        self.finish((right, left, (Y_AXIS, 0), (Y_AXIS, 1)), CHIPS)


def decode_kernel(
    hidden_hbm, wk_hbm, wv_hbm, query_hbm, scale_ref, new_ref, found_ref,
    cache_ref, smooth_ref, att_ref,
    hid, wk, wv, mz, my, qs, acc, kraw, kbuf, vbuf, vout, fresh_kv, part, stat, out, out_stat, got, got_stat,
    att_out,
    local_sem, hid_sem, send_sem, recv_sem, swap_send, swap_recv, peak_sem, half_sem,
    part_send, part_recv,
):
    torus = Torus()
    me, core = torus.at(0, 0), torus.core
    tokens, depth = hidden_hbm.shape
    columns = wk_hbm.shape[1]
    steps_reqs = query_hbm.shape[0]
    half_q = query_hbm.shape[1] // 2
    heads = half_q // HD
    pages = tokens // PAGE
    parts = 4
    width = depth // parts
    own_k = pltpu.make_async_copy(wk_hbm, wk.at[me, core], local_sem.at[0])
    own_v = pltpu.make_async_copy(wv_hbm, wv.at[me, core], local_sem.at[1])
    own_q = [
        pltpu.make_async_copy(
            query_hbm.at[
                pl.ds(k * (steps_reqs // 2), steps_reqs // 2),
                pl.ds(pl.multiple_of(core * half_q, half_q), half_q),
            ],
            qs.at[me, k],
            local_sem.at[2 + k],
        )
        for k in range(2)
    ]
    own_k.start()
    own_v.start()
    for copy in own_q:
        copy.start()
    hid_copies = [
        pltpu.make_async_copy(
            hidden_hbm.at[:, pl.ds(k * width, width)],
            hid.at[:, pl.ds(k * width, width)],
            hid_sem.at[k],
        )
        for k in range(parts)
    ]
    for copy in hid_copies:
        copy.start()
    greet(torus)
    own_k.wait()

    def stream(number, block, swap=True, both_z=False):
        return Stream(
            torus,
            number,
            block,
            send_sem.at[number],
            recv_sem.at[number],
            (swap_send.at[number], swap_recv.at[number]) if swap else None,
            both_z,
        )

    s_k = stream(0, lambda blk, c: wk.at[blk, c])
    s_v = stream(1, lambda blk, c: wv.at[blk, c])
    s_qa = stream(2, lambda blk, c: qs.at[blk, 0], swap=False)
    s_qb = stream(3, lambda blk, c: qs.at[blk, 1], swap=False, both_z=True)
    rows = 512

    def multiply(stream, weights, to, dy):
        y = lax.rem(torus.y + (dy + NY), NY)
        blocks = pl.ds(pl.multiple_of(y * NZ, NZ), NZ)
        stream.swap_copy(weights.at[blocks, 1 - core], y).wait_recv()

        def one(m, carry):
            at = pl.ds(pl.multiple_of(m * rows, rows), rows)
            w = weights[blocks].reshape(width, weights.shape[3])
            product = jnp.dot(
                hid[at, pl.ds(pl.multiple_of(y * width, width), width)],
                w,
                preferred_element_type=jnp.float32,
            )
            to[at, :] = product if dy == 0 else to[at, :] + product
            return carry

        lax.fori_loop(0, tokens // rows, one, 0)

    mine = pl.ds(pl.multiple_of(core * HD, HD), HD)
    theirs = pl.ds(pl.multiple_of((1 - core) * HD, HD), HD)
    my_pages = pl.ds(pl.multiple_of(core * pages, pages), pages)
    their_pages = pl.ds(pl.multiple_of((1 - core) * pages, pages), pages)

    def to_partner(k, src, dst):
        return pltpu.make_async_remote_copy(
            src_ref=src,
            dst_ref=dst,
            send_sem=half_sem.at[k, 0],
            recv_sem=half_sem.at[k, 1],
            device_id={"rep": 1 - core},
            device_id_type=pl.DeviceIdType.MESH,
        )

    def clip(x, kind, lanes):
        scale = scale_ref[kind : kind + 1, lanes]
        return jnp.clip(x, -8.0 * scale, 7.0 * scale).astype(jnp.bfloat16)

    keys_over = to_partner(0, acc.at[0, :, theirs], kraw)
    values_over = to_partner(1, vout, vbuf.at[my_pages])

    ring, column = friends(torus)
    place = core * NZ + torus.z

    def peak_copy(refs, slot, k, target):
        return pltpu.make_async_remote_copy(
            src_ref=refs.at[slot],
            dst_ref=refs.at[slot],
            send_sem=peak_sem.at[k, 0],
            recv_sem=peak_sem.at[k, 1],
            device_id={"seq": target[0], "rep": target[1]},
            device_id_type=pl.DeviceIdType.MESH,
        )

    def tell(refs, slot, k, peers):
        for target in peers:
            peak_copy(refs, slot, k, target).start()

    def heard(refs, k, peers):
        return peak_copy(refs, pl.ds(0, len(peers)), k, peers[0])

    q_lag = QUERY_LAG
    for i in range(q_lag + STEPS_GATHER):
        if i == 0:
            own_v.wait()
        if i == q_lag:
            for copy in own_q:
                copy.wait()
        for stream_i, start in ((s_k, 0), (s_v, 0), (s_qa, q_lag), (s_qb, q_lag)):
            if i == 5 and stream_i is s_qa:
                for copy in hid_copies:
                    copy.wait()
                multiply(s_k, wk, acc.at[0], 0)
            if 0 <= i - start < STEPS_GATHER:
                stream_i.step(i - start)
        if i == 0:
            for kind in range(2):
                fresh_kv[kind] = (
                    new_ref[:, :, kind, :].astype(jnp.float32).reshape(steps_reqs, columns)
                )
        if i == 5:
            multiply(s_k, wk, acc.at[0], 1)
            multiply(s_k, wk, acc.at[0], -1)
        if i == 6:
            multiply(s_k, wk, acc.at[0], 2)
            mz[place] = jnp.max(jnp.abs(acc[0]).reshape(tokens // 8, 8, columns), axis=0)
            tell(mz, place, 0, ring)
            keys_over.start()
            multiply(s_v, wv, acc.at[1], 0)
        if i == 7:
            multiply(s_v, wv, acc.at[1], 1)
            multiply(s_v, wv, acc.at[1], -1)
        if i == 8:
            heard(mz, 0, ring).wait_recv()
            my[torus.y] = jnp.max(mz[...], axis=0)
            tell(my, torus.y, 1, column)
            multiply(s_v, wv, acc.at[1], 2)
            vout[...] = clip(acc[1, :, theirs], 1, theirs).reshape(vout.shape)
            values_over.start()
            vbuf[my_pages] = clip(acc[1, :, mine], 1, mine).reshape(vout.shape)
    heard(my, 1, column).wait_recv()
    peak = jnp.max(my[...], axis=0)
    smooth_ref[...] = jnp.sqrt(jnp.max(peak, axis=0, keepdims=True) + EPSILON)
    my_smooth = smooth_ref[:, mine]

    def queries_of(g):
        return jnp.concatenate(
            [
                (
                    qs[g, :, :, h * HD : (h + 1) * HD]
                    .reshape(steps_reqs, HD)
                    .astype(jnp.float32)
                    * my_smooth
                ).astype(jnp.bfloat16)
                for h in range(heads)
            ],
            axis=0,
        )

    across = heads * steps_reqs
    lane = lax.broadcasted_iota(jnp.int32, (PAGE, across), 1)
    key = lax.broadcasted_iota(jnp.int32, (PAGE, across), 0)
    request = lane % 8

    kbuf[my_pages] = clip(acc[0, :, mine] / my_smooth, 0, mine).reshape(vout.shape)
    keys_over.wait_recv()
    kbuf[their_pages] = clip(kraw[...] / my_smooth, 0, mine).reshape(vout.shape)
    to_partner(1, vout, vbuf.at[their_pages]).wait_recv()

    def one_group(g):
        keys, values, masks = [], [], []
        for e in range(SLOTS):
            who, page, count = (found_ref[SLOTS * f + e, g * 8] for f in range(3))
            keys.append(kbuf[page])
            values.append(vbuf[page])
            masks.append((request == who) & (key < count))
        top, total, summed = attend(
            jnp.concatenate(keys, axis=0),
            jnp.concatenate(values, axis=0),
            queries_of(g),
            jnp.concatenate(masks, axis=0),
        )
        part[g] = summed
        stat[g] = jnp.concatenate([top, total], axis=0)

    def attend_to(count, group):
        def two(i, carry):
            one_group(group(2 * i))
            one_group(group(2 * i + 1))
            return carry

        lax.fori_loop(0, count // 2, two, 0)

    partials = Partials(
        torus, part, stat, out, out_stat, got, got_stat, part_send, part_recv
    )

    def write_cache(quarter):
        def chore():
            at = pl.ds(quarter * (tokens // 4), tokens // 4)
            every = slice(None)
            cache_ref[at] = jnp.stack(
                [
                    clip(acc[0, at, :] / smooth_ref[...], 0, every),
                    clip(acc[1, at, :], 1, every),
                ],
                axis=1,
            )

        return chore

    def attend_fresh():
        mask = (key % 8 == request) & (key // 8 <= (lane // 8) % (steps_reqs // 8))
        partials.keep(
            CHIPS,
            *attend(
                clip(fresh_kv[0, :, mine] / my_smooth, 0, mine),
                clip(fresh_kv[1, :, mine], 1, mine),
                queries_of(me),
                mask,
            ),
        )

    chores = [*(write_cache(quarter) for quarter in range(4)), attend_fresh]

    @pl.when(core == 0)
    def _():
        partials.y_first(attend_to, chores)

    @pl.when(core == 1)
    def _():
        partials.z_first(attend_to, chores)

    top, total, summed = partials.kept(me)
    done = (summed / total).T.astype(jnp.bfloat16)
    for h in range(heads):
        att_out[:, h * HD : (h + 1) * HD] = done[h * steps_reqs : (h + 1) * steps_reqs]
    own_att = pl.ds(pl.multiple_of(core * half_q, half_q), half_q)
    last = to_partner(2, att_out, att_ref.at[:, own_att])
    last.start()
    att_ref[:, own_att] = att_out[...]

    for s, refs in ((s_k, wk), (s_v, wv)):
        s.sent_copy(refs.at[pl.ds(0, CHIPS - 1), core]).wait_send()
        s.swap_copy(refs.at[:, core]).wait_send()
    s_qa.sent_copy(qs.at[pl.ds(0, CHIPS - 1), 0]).wait_send()
    s_qb.sent_copy(qs.at[pl.ds(0, CHIPS - 1), 1]).wait_send()
    heard(mz, 0, ring).wait_send()
    heard(my, 1, column).wait_send()
    keys_over.wait_send()
    values_over.wait_send()
    for k, refs in enumerate((out, out_stat)):
        pltpu.make_async_remote_copy(
            src_ref=refs.at[pl.ds(0, CHIPS - 1)],
            dst_ref=refs.at[pl.ds(0, CHIPS - 1)],
            send_sem=part_send.at[k],
            recv_sem=part_recv.at[k, 0, 0, 0],
            device_id={"rep": 1 - core},
            device_id_type=pl.DeviceIdType.MESH,
        ).wait_send()
    last.wait()


def decode(hidden, key_weight, value_weight, queries, group_scale, new_kv, found):
    tokens, depth = hidden.shape
    rows, columns = key_weight.shape
    step_reqs, q_columns = queries.shape
    pages = tokens // PAGE
    across = q_columns // 2 // HD * step_reqs
    bf16, f32 = jnp.bfloat16, jnp.float32
    any_spec = pl.BlockSpec(memory_space=pl.ANY)
    vmem = pl.BlockSpec(memory_space=pltpu.VMEM)
    smem = pl.BlockSpec(memory_space=pltpu.SMEM)
    return pl.pallas_call(
        decode_kernel,
        out_shape=(
            jax.ShapeDtypeStruct((tokens, 2, columns), bf16),
            jax.ShapeDtypeStruct((1, columns), f32),
            jax.ShapeDtypeStruct((step_reqs, q_columns), bf16),
        ),
        in_specs=[any_spec, any_spec, any_spec, any_spec, vmem, vmem, smem],
        out_specs=(vmem, vmem, vmem),
        scratch_shapes=[
            pltpu.VMEM((tokens, depth), bf16),
            pltpu.VMEM((CHIPS, 2, rows, columns), bf16),
            pltpu.VMEM((CHIPS, 2, rows, columns), bf16),
            pltpu.VMEM((2 * NZ, 8, columns), f32),
            pltpu.VMEM((NY, 8, columns), f32),
            pltpu.VMEM((CHIPS, 2, step_reqs // 2, q_columns // 2), bf16),
            pltpu.VMEM((2, tokens, columns), f32),
            pltpu.VMEM((tokens, HD), f32),
            pltpu.VMEM((2 * pages, PAGE, HD), bf16),
            pltpu.VMEM((2 * pages, PAGE, HD), bf16),
            pltpu.VMEM((pages, PAGE, HD), bf16),
            pltpu.VMEM((2, step_reqs, columns), f32),
            pltpu.VMEM((CHIPS + 1, HD, across), f32),
            pltpu.VMEM((CHIPS + 1, 2, across), f32),
            pltpu.VMEM((CHIPS, HD, across), bf16),
            pltpu.VMEM((CHIPS, 2, across), f32),
            pltpu.VMEM((2, 2, CHIPS, HD, across), bf16),
            pltpu.VMEM((2, 2, CHIPS, 2, across), f32),
            pltpu.VMEM((step_reqs, q_columns // 2), bf16),
            pltpu.SemaphoreType.DMA((4,)),
            pltpu.SemaphoreType.DMA((4,)),
            pltpu.SemaphoreType.DMA((4,)),
            pltpu.SemaphoreType.DMA((4, CHIPS)),
            pltpu.SemaphoreType.DMA((2,)),
            pltpu.SemaphoreType.DMA((2, NY)),
            pltpu.SemaphoreType.DMA((2, 2)),
            pltpu.SemaphoreType.DMA((3, 2)),
            pltpu.SemaphoreType.DMA((2,)),
            pltpu.SemaphoreType.DMA((2, 2, 2, CHIPS)),
        ],
        compiler_params=pltpu.CompilerParams(
            collective_id=0, has_side_effects=True, vmem_limit_bytes=60 * 2**20
        ),
        name="decode",
    )(hidden, key_weight, value_weight, queries, group_scale, new_kv, found)


def finish_kernel(*refs):
    outputs = len(refs) // 3
    sem = refs[-1]
    pieces = []
    for src, dst, via in zip(refs[:outputs], refs[outputs:], refs[2 * outputs :]):
        count = 4 if len(src.shape) == 3 else 1
        rows = src.shape[0] // count
        pieces += [
            tuple(r.at[pl.ds(k * rows, rows)] for r in (src, via, dst)) for k in range(count)
        ]
    legs = []
    for k, (src, via, dst) in enumerate(pieces):
        legs.append(
            (
                pltpu.make_async_copy(src, via, sem.at[k, 0]),
                pltpu.make_async_copy(via, dst, sem.at[k, 1]),
            )
        )
    for first, _ in legs:
        first.start()
    for first, second in legs:
        first.wait()
        second.start()
    for _, second in legs:
        second.wait()


def finish(*arrays):
    any_spec = pl.BlockSpec(memory_space=pl.ANY)
    return pl.pallas_call(
        finish_kernel,
        out_shape=tuple(jax.ShapeDtypeStruct(a.shape, a.dtype) for a in arrays),
        in_specs=[any_spec] * len(arrays),
        out_specs=(any_spec,) * len(arrays),
        scratch_shapes=[
            *(pltpu.VMEM(a.shape, a.dtype) for a in arrays),
            pltpu.SemaphoreType.DMA((6, 2)),
        ],
        name="finish",
    )(*arrays)


def on_device(
    hidden, key_weight, value_weight, group_scale, new_kv, decode_query, page_table, lengths
):
    steps, requests, q_columns = decode_query.shape
    columns = key_weight.shape[1]
    kv_cache, smoothing, attention = finish(
        *decode(
            hidden,
            key_weight,
            value_weight,
            decode_query.reshape(steps * requests, q_columns),
            group_scale,
            new_kv,
            find_pages(page_table, lengths),
        )
    )
    return (
        kv_cache,
        smoothing.reshape(columns),
        attention.reshape(steps, requests, q_columns),
    )


def solution(mesh):
    placed = (
        P(("seq", "rep"), None),
        P(("seq", "rep"), "head"),
        P(("seq", "rep"), "head"),
        P(None, "head"),
        P(None, "seq", None, "head"),
        P(None, "seq", "head"),
        P(),
        P(),
    )
    return jax.shard_map(
        on_device,
        mesh=mesh,
        in_specs=placed,
        out_specs=(P(("seq", "rep"), None, "head"), P("head"), P(None, "seq", "head")),
        check_vma=False,
    )
```

```python
import functools

import jax
import jax.numpy as jnp
from jax import lax
from jax.experimental import pallas as pl
from jax.experimental.pallas import tpu as pltpu
from jax.sharding import PartitionSpec as P

KVH = 8
HD = 128
QH = 64
PAGE = 32
NY = 4
NZ = 8
CHIPS = NY * NZ


EPSILON = 1e-05
NEGATIVE = -1e30
EMPTY = -1e29


class Torus:
    def __init__(self):
        seq = lax.axis_index("seq")
        self.y, self.z = lax.div(seq, NZ), lax.rem(seq, NZ)
        self.core = lax.axis_index("rep")

    def at(self, dy, dz):
        y = lax.rem(self.y + (dy + NY), NY)
        z = lax.rem(self.z + (dz + NZ), NZ)
        return y * NZ + z


class Stream:
    def __init__(self, torus, number, block, send_sem, recv_sem, swap, both_z=False):
        self.torus, self.number, self.block, self.both_z = torus, number, block, both_z
        self.send_sem, self.recv_sem, self.swap = send_sem, recv_sem, swap

    def copy(self, blk, dy, dz):
        ref = self.block(blk, self.torus.core)
        return pltpu.make_async_remote_copy(
            src_ref=ref,
            dst_ref=ref,
            send_sem=self.send_sem,
            recv_sem=self.recv_sem.at[blk],
            device_id={"seq": self.torus.at(dy, dz)},
            device_id_type=pl.DeviceIdType.MESH,
        )

    def across(self, blk):
        if self.swap is None:
            return
        ref = self.block(blk, self.torus.core)
        pltpu.make_async_remote_copy(
            src_ref=ref,
            dst_ref=ref,
            send_sem=self.swap[0],
            recv_sem=self.swap[1].at[lax.div(blk, NZ)],
            device_id={"rep": 1 - self.torus.core},
            device_id_type=pl.DeviceIdType.MESH,
        ).start()

    def arrived(self, dy, dz):
        blk = self.torus.at(dy, dz)
        self.copy(blk, 1, 0).wait_recv()
        return blk

    def along_z(self, blk, right, left):
        if right:
            self.copy(blk, 0, 1).start()
        if left:
            self.copy(blk, 0, -1).start()

    def along_y(self, blk, up, down):
        if up:
            self.copy(blk, 1, 0).start()
        if down:
            self.copy(blk, -1, 0).start()

    def step_z_first(self, st):
        turn_right = self.number % 2 == 0
        far = -4 if turn_right else 4
        reach = [[0], [-1, 1], [-2, 2], [-3, 3], [far]]
        if st == 0:
            blk = self.torus.at(0, 0)
            self.along_z(blk, True, True)
            self.along_y(blk, True, True)
            self.across(blk)
        if 1 <= st <= 4:
            for dz in reach[st]:
                blk = self.arrived(0, dz)
                onward = st < 3 or (st == 3 and (dz < 0) == turn_right)
                self.along_z(blk, onward and dz < 0, onward and dz > 0)
                self.along_y(blk, True, True)
                self.across(blk)
        if 1 <= st <= 5:
            for dz in reach[st - 1]:
                for dy in (-1, 1):
                    blk = self.arrived(dy, dz)
                    even = dz % 2 == 0
                    self.along_y(blk, even and dy < 0, not even and dy > 0)
                    self.across(blk)
        if 2 <= st <= 6:
            for dz in reach[st - 2]:
                self.across(self.arrived(2, dz))

    def step_y_first(self, st):
        even = self.number % 2 == 0
        if st == 0:
            blk = self.torus.at(0, 0)
            self.along_z(blk, True, True)
            self.along_y(blk, True, True)
            self.across(blk)
        if st == 1:
            for dy in (-1, 1):
                blk = self.arrived(dy, 0)
                self.along_y(blk, even and dy < 0, not even and dy > 0)
                self.along_z(blk, True, True)
                self.across(blk)
        if st == 2:
            blk = self.arrived(2, 0)
            self.along_z(blk, True, True)
            self.across(blk)
        for dy, first in ((0, 0), (-1, 1), (1, 1), (2, 2)):
            k = st - first
            turn_right = (self.number + dy) % 2 == 0
            if 1 <= k <= 3:
                for dz in (-k, k):
                    blk = self.arrived(dy, dz)
                    onward = k < 3 or (dz < 0) == turn_right
                    self.along_z(blk, onward and dz < 0, onward and dz > 0)
                    self.across(blk)
            if k == 4:
                self.across(self.arrived(dy, -4 if turn_right else 4))

    def step(self, st):
        if self.both_z:
            self.step_z_first(st)
            return

        @pl.when(self.torus.core == 0)
        def _():
            self.step_z_first(st)

        @pl.when(self.torus.core == 1)
        def _():
            self.step_y_first(st)

    def swap_copy(self, refs, row=0):
        return pltpu.make_async_remote_copy(
            src_ref=refs,
            dst_ref=refs,
            send_sem=self.swap[0],
            recv_sem=self.swap[1].at[row],
            device_id={"rep": 1 - self.torus.core},
            device_id_type=pl.DeviceIdType.MESH,
        )

    def sent_copy(self, refs):
        return pltpu.make_async_remote_copy(
            src_ref=refs,
            dst_ref=refs,
            send_sem=self.send_sem,
            recv_sem=self.recv_sem.at[0],
            device_id={"rep": 1 - self.torus.core},
            device_id_type=pl.DeviceIdType.MESH,
        )


STEPS_GATHER = 7
QUERY_LAG = 2
def friends(torus):
    ring = [(torus.at(0, dz), torus.core) for dz in (1, -1, 2, -2, 3, -3, 4)]
    ring += [(torus.at(0, dz), 1 - torus.core) for dz in (0, 1, -1, 2, -2, 3, -3, 4)]
    return ring, [(torus.at(dy, 0), torus.core) for dy in (1, -1, 2)]


def greet(torus):
    barrier = pltpu.get_barrier_semaphore()
    ring, column = friends(torus)
    for place, core in ring + column:
        pl.semaphore_signal(
            barrier,
            inc=1,
            device_id={"seq": place, "rep": core},
            device_id_type=pl.DeviceIdType.MESH,
        )
    pl.semaphore_wait(barrier, len(ring) + len(column))


SLOTS = 8


def find_kernel(table_ref, length_ref, found_ref):
    chip = lax.axis_index("seq")
    table = table_ref[...]
    slots, requests = table.shape
    slot = lax.broadcasted_iota(jnp.int32, table.shape, 0)
    lane = lax.broadcasted_iota(jnp.int32, table.shape, 1)
    left = length_ref[...] - slot * PAGE
    mine = ((left > 0) & (table // (2 * PAGE) == chip)).astype(jnp.float32)
    row = lax.broadcasted_iota(jnp.int32, (slots, slots), 0)
    column = lax.broadcasted_iota(jnp.int32, (slots, slots), 1)
    above = jnp.dot(
        (column < row).astype(jnp.float32), mine, preferred_element_type=jnp.float32
    )
    whole = jnp.broadcast_to(jnp.sum(mine, axis=0, keepdims=True), (8, requests))
    a = lax.broadcasted_iota(jnp.int32, (requests, requests), 0)
    b = lax.broadcasted_iota(jnp.int32, (requests, requests), 1)
    same = a // 8 == b // 8
    before = jnp.dot(
        whole, (same & (a < b)).astype(jnp.float32), preferred_element_type=jnp.float32
    )
    rank = jnp.where(mine > 0.0, above + before[0:1], -1.0)
    fields = (
        (lane % 8).astype(jnp.float32),
        (table % (2 * PAGE)).astype(jnp.float32),
        jnp.minimum(left, PAGE).astype(jnp.float32),
    )
    picked = jnp.concatenate(
        [
            jnp.sum(jnp.where(rank == e, field, 0.0), axis=0, keepdims=True)
            for field in fields
            for e in range(SLOTS)
        ],
        axis=0,
    )
    spread = jnp.dot(picked, same.astype(jnp.float32), preferred_element_type=jnp.float32)
    found_ref[...] = spread.astype(jnp.int32)


def find_pages(page_table, lengths):
    requests, slots = page_table.shape
    return pl.pallas_call(
        find_kernel,
        out_shape=jax.ShapeDtypeStruct((3 * SLOTS, requests), jnp.int32),
        name="find_pages",
    )(page_table.T, lengths.reshape(1, requests))


Y_AXIS, Z_AXIS = 0, 1


def below(keys, queries):
    return lax.dot_general(
        keys, queries, (((1,), (1,)), ((), ())), preferred_element_type=jnp.float32
    )


def weighed(values, weights):
    return lax.dot_general(
        values, weights, (((0,), (0,)), ((), ())), preferred_element_type=jnp.float32
    )


def attend(jobs):
    scores = [
        jnp.where(mask, below(keys, queries) * HD ** (-0.5), NEGATIVE)
        for keys, _, queries, mask in jobs
    ]
    tops = [jnp.maximum(jnp.max(x, axis=0, keepdims=True), EMPTY) for x in scores]
    weights = [jnp.exp(x - top) for x, top in zip(scores, tops)]
    totals = [jnp.sum(x, axis=0, keepdims=True) for x in weights]
    sums = [weighed(job[1], x.astype(jnp.bfloat16)) for job, x in zip(jobs, weights)]
    return list(zip(tops, totals, sums))


def fold(parts):
    top = functools.reduce(jnp.maximum, [p[0] for p in parts])
    scales = [jnp.exp(p[0] - top) for p in parts]
    total = functools.reduce(jnp.add, [p[1] * s for p, s in zip(parts, scales)])
    summed = functools.reduce(jnp.add, [p[2] * s for p, s in zip(parts, scales)])
    return top, total, summed


class Partials:
    def __init__(self, torus, part, stat, out, out_stat, got, got_stat, send_sem, recv_sem):
        self.torus, self.part, self.stat = torus, part, stat
        self.out, self.out_stat = out, out_stat
        self.got, self.got_stat = got, got_stat
        self.send_sem, self.recv_sem = send_sem, recv_sem

    def copies(self, g, axis, way, slot=None, peer=None):
        step = 1 - 2 * way
        if peer is None:
            peer = self.torus.at(step, 0) if axis == Y_AXIS else self.torus.at(0, step)
        slot = g if slot is None else slot
        return [
            pltpu.make_async_remote_copy(
                src_ref=src.at[g],
                dst_ref=dst.at[axis, way, slot],
                send_sem=self.send_sem.at[k],
                recv_sem=self.recv_sem.at[k, axis, way, slot],
                device_id={"seq": peer},
                device_id_type=pl.DeviceIdType.MESH,
            )
            for k, (src, dst) in enumerate(
                ((self.out, self.got), (self.out_stat, self.got_stat))
            )
        ]

    def kept(self, at):
        return self.stat[at, 0:1], self.stat[at, 1:2], self.part[at]

    def keep(self, at, top, total, summed):
        self.part[at] = summed
        self.stat[at] = jnp.concatenate([top, total], axis=0)

    def gathered(self, g, arrivals, more=()):
        parts = [self.kept(g), *more]
        for axis, way, *direct in arrivals:
            slot = direct[0] if direct else g
            for copy in self.copies(g, axis, way, slot):
                copy.wait_recv()
            stat = self.got_stat[axis, way, slot]
            parts.append((stat[0:1], stat[1:2], self.got[axis, way, slot].astype(jnp.float32)))
        return fold(parts) if len(parts) > 1 else parts[0]

    def send(self, dy, dz, arrivals, axis, way, slot=None, peer=None):
        g = self.torus.at(dy, dz)
        top, total, summed = self.gathered(g, arrivals)
        self.out[g] = summed.astype(jnp.bfloat16)
        self.out_stat[g] = jnp.concatenate([top, total], axis=0)
        for copy in self.copies(g, axis, way, slot, peer):
            copy.start()

    def finish(self, arrivals, fresh):
        me = self.torus.at(0, 0)
        self.keep(me, *self.gathered(me, arrivals, more=(self.kept(fresh),)))

    def y_first(self, attend_at, chores):
        up, down = (Y_AXIS, 0), (Y_AXIS, 1)

        def far(k):
            dz = 4 - 2 * k
            attend_at((2, dz), (2, dz - 1))
            self.send(2, dz, (), *up)
            self.send(2, dz - 1, (), *down)

        def near(k):
            dz = 4 - 2 * k
            attend_at((1, dz - 1), (-1, dz))
            self.send(1, dz - 1, (), *up)
            self.send(-1, dz, (), *down)

        def near_passing(k):
            dz = 4 - 2 * k
            attend_at((1, dz), (-1, dz - 1))
            self.send(1, dz, (up,), *up)
            self.send(-1, dz - 1, (down,), *down)

        for body in (far, near, near_passing):
            repeat(NZ // 2, body)
        repeat(NZ // 2, lambda k: attend_at((0, 4 - 2 * k), (0, 3 - 2 * k)))
        me = self.torus.at(0, 0)
        for dz in (4, -3, 3, -2, 2, -1, 1):
            self.send(0, dz, (up, down), Z_AXIS, 0, me, self.torus.at(0, dz))
        for chore in chores:
            chore()
        straight = [(Z_AXIS, 0, self.torus.at(0, dz)) for dz in (1, -1, 2, -2, 3, -3, 4)]
        self.finish((up, down, *straight), CHIPS)

    def z_first(self, attend_at, chores):
        right, left = (Z_AXIS, 0), (Z_AXIS, 1)

        def far(k):
            dy = 2 - 2 * k
            attend_at((dy, 4), (dy - 1, 4))
            self.send(dy, 4, (), *right)
            self.send(dy - 1, 4, (), *left)

        def near(k):
            dy = 2 - 2 * k
            attend_at((dy, -3), (dy - 1, 3))
            self.send(dy, -3, (), *left)
            self.send(dy - 1, 3, (), *right)

        def near_passing(k):
            dy = 2 - 2 * k
            attend_at((dy, 3), (dy - 1, -3))
            self.send(dy, 3, (right,), *right)
            self.send(dy - 1, -3, (left,), *left)

        for body in (far, near, near_passing):
            repeat(NY // 2, body)

        def both(dz):
            def body(k):
                dy = 2 - k
                attend_at((dy, dz), (dy, -dz))
                self.send(dy, dz, (right,), *right)
                self.send(dy, -dz, (left,), *left)

            return body

        for dz in (2, 1):
            repeat(NY, both(dz))
        repeat(NY // 2, lambda k: attend_at((2 - 2 * k, 0), (1 - 2 * k, 0)))
        for chore in chores[:2]:
            chore()
        me = self.torus.at(0, 0)
        for dy in (2, 1, -1):
            self.send(dy, 0, (right, left), Y_AXIS, 0, me, self.torus.at(dy, 0))
        for chore in chores[2:]:
            chore()
        straight = [(Y_AXIS, 0, self.torus.at(dy, 0)) for dy in (1, -1, 2)]
        self.finish((right, left, *straight), CHIPS)


def repeat(count, body):
    def step(k, carry):
        body(k)
        return carry

    lax.fori_loop(0, count, step, 0)


def decode_kernel(
    hidden_hbm, wk_hbm, wv_hbm, query_hbm, scale_ref, new_ref, found_ref,
    cache_ref, smooth_ref, att_ref,
    hid, wk, wv, mz, my, qs, acc, kraw, kbuf, vbuf, vout, fresh_kv, part, stat, out, out_stat, got, got_stat,
    att_out,
    local_sem, hid_sem, send_sem, recv_sem, swap_send, swap_recv, peak_sem, half_sem,
    part_send, part_recv,
):
    torus = Torus()
    me, core = torus.at(0, 0), torus.core
    tokens, depth = hidden_hbm.shape
    columns = wk_hbm.shape[1]
    steps_reqs = query_hbm.shape[0]
    half_q = query_hbm.shape[1] // 2
    heads = half_q // HD
    pages = tokens // PAGE
    parts = 4
    width = depth // parts
    own_k = pltpu.make_async_copy(wk_hbm, wk.at[me, core], local_sem.at[0])
    own_v = pltpu.make_async_copy(wv_hbm, wv.at[me, core], local_sem.at[1])
    own_q = [
        pltpu.make_async_copy(
            query_hbm.at[
                pl.ds(k * (steps_reqs // 2), steps_reqs // 2),
                pl.ds(pl.multiple_of(core * half_q, half_q), half_q),
            ],
            qs.at[me, k],
            local_sem.at[2 + k],
        )
        for k in range(2)
    ]
    own_k.start()
    own_v.start()
    for copy in own_q:
        copy.start()
    hid_copies = [
        pltpu.make_async_copy(
            hidden_hbm.at[:, pl.ds(k * width, width)],
            hid.at[:, pl.ds(k * width, width)],
            hid_sem.at[k],
        )
        for k in range(parts)
    ]
    for copy in hid_copies:
        copy.start()
    greet(torus)
    own_k.wait()

    def stream(number, block, swap=True, both_z=False):
        return Stream(
            torus,
            number,
            block,
            send_sem.at[number],
            recv_sem.at[number],
            (swap_send.at[number], swap_recv.at[number]) if swap else None,
            both_z,
        )

    s_k = stream(0, lambda blk, c: wk.at[blk, c])
    s_v = stream(1, lambda blk, c: wv.at[blk, c])
    s_qa = stream(2, lambda blk, c: qs.at[blk, 0], swap=False)
    s_qb = stream(3, lambda blk, c: qs.at[blk, 1], swap=False, both_z=True)
    rows = 512

    def multiply(stream, weights, to, dy):
        y = lax.rem(torus.y + (dy + NY), NY)
        blocks = pl.ds(pl.multiple_of(y * NZ, NZ), NZ)
        stream.swap_copy(weights.at[blocks, 1 - core], y).wait_recv()

        def one(m, carry):
            at = pl.ds(pl.multiple_of(m * rows, rows), rows)
            w = weights[blocks].reshape(width, weights.shape[3])
            product = jnp.dot(
                hid[at, pl.ds(pl.multiple_of(y * width, width), width)],
                w,
                preferred_element_type=jnp.float32,
            )
            to[at, :] = product if dy == 0 else to[at, :] + product
            return carry

        lax.fori_loop(0, tokens // rows, one, 0)

    mine = pl.ds(pl.multiple_of(core * HD, HD), HD)
    theirs = pl.ds(pl.multiple_of((1 - core) * HD, HD), HD)
    my_pages = pl.ds(pl.multiple_of(core * pages, pages), pages)
    their_pages = pl.ds(pl.multiple_of((1 - core) * pages, pages), pages)

    def to_partner(k, src, dst):
        return pltpu.make_async_remote_copy(
            src_ref=src,
            dst_ref=dst,
            send_sem=half_sem.at[k, 0],
            recv_sem=half_sem.at[k, 1],
            device_id={"rep": 1 - core},
            device_id_type=pl.DeviceIdType.MESH,
        )

    def clip(x, kind, lanes):
        scale = scale_ref[kind : kind + 1, lanes]
        return jnp.clip(x, -8.0 * scale, 7.0 * scale).astype(jnp.bfloat16)

    keys_over = to_partner(0, acc.at[0, :, theirs], kraw)
    values_over = to_partner(1, vout, vbuf.at[my_pages])

    ring, column = friends(torus)
    place = core * NZ + torus.z

    def peak_copy(refs, slot, k, target):
        return pltpu.make_async_remote_copy(
            src_ref=refs.at[slot],
            dst_ref=refs.at[slot],
            send_sem=peak_sem.at[k, 0],
            recv_sem=peak_sem.at[k, 1],
            device_id={"seq": target[0], "rep": target[1]},
            device_id_type=pl.DeviceIdType.MESH,
        )

    def tell(refs, slot, k, peers):
        for target in peers:
            peak_copy(refs, slot, k, target).start()

    def heard(refs, k, peers):
        return peak_copy(refs, pl.ds(0, len(peers)), k, peers[0])

    q_lag = QUERY_LAG
    for i in range(q_lag + STEPS_GATHER):
        if i == 0:
            own_v.wait()
        if i == q_lag:
            for copy in own_q:
                copy.wait()
        for stream_i, start in ((s_k, 0), (s_v, 0), (s_qa, q_lag), (s_qb, q_lag)):
            if i == 5 and stream_i is s_qa:
                for copy in hid_copies:
                    copy.wait()
                multiply(s_k, wk, acc.at[0], 0)
            if 0 <= i - start < STEPS_GATHER:
                stream_i.step(i - start)
        if i == 0:
            for kind in range(2):
                fresh_kv[kind] = (
                    new_ref[:, :, kind, :].astype(jnp.float32).reshape(steps_reqs, columns)
                )
        if i == 5:
            multiply(s_k, wk, acc.at[0], 1)
            multiply(s_k, wk, acc.at[0], -1)
        if i == 6:
            multiply(s_k, wk, acc.at[0], 2)
            mz[place] = jnp.max(jnp.abs(acc[0]).reshape(tokens // 8, 8, columns), axis=0)
            tell(mz, place, 0, ring)
            keys_over.start()
            multiply(s_v, wv, acc.at[1], 0)
        if i == 7:
            multiply(s_v, wv, acc.at[1], 1)
            multiply(s_v, wv, acc.at[1], -1)
        if i == 8:
            heard(mz, 0, ring).wait_recv()
            my[torus.y] = jnp.max(mz[...], axis=0)
            tell(my, torus.y, 1, column)
            multiply(s_v, wv, acc.at[1], 2)
            vout[...] = clip(acc[1, :, theirs], 1, theirs).reshape(vout.shape)
            values_over.start()
            vbuf[my_pages] = clip(acc[1, :, mine], 1, mine).reshape(vout.shape)
    heard(my, 1, column).wait_recv()
    peak = jnp.max(my[...], axis=0)
    smooth_ref[...] = jnp.sqrt(jnp.max(peak, axis=0, keepdims=True) + EPSILON)
    my_smooth = smooth_ref[:, mine]

    def queries_of(g):
        return jnp.concatenate(
            [
                (
                    qs[g, :, :, h * HD : (h + 1) * HD]
                    .reshape(steps_reqs, HD)
                    .astype(jnp.float32)
                    * my_smooth
                ).astype(jnp.bfloat16)
                for h in range(heads)
            ],
            axis=0,
        )

    across = heads * steps_reqs
    lane = lax.broadcasted_iota(jnp.int32, (PAGE, across), 1)
    key = lax.broadcasted_iota(jnp.int32, (PAGE, across), 0)
    request = lane % 8

    kbuf[my_pages] = clip(acc[0, :, mine] / my_smooth, 0, mine).reshape(vout.shape)
    keys_over.wait_recv()
    kbuf[their_pages] = clip(kraw[...] / my_smooth, 0, mine).reshape(vout.shape)
    to_partner(1, vout, vbuf.at[their_pages]).wait_recv()

    def job_of(g):
        keys, values, masks = [], [], []
        for e in range(SLOTS):
            who, page, count = (found_ref[SLOTS * f + e, g * 8] for f in range(3))
            keys.append(kbuf[page])
            values.append(vbuf[page])
            masks.append((request == who) & (key < count))
        return (
            jnp.concatenate(keys, axis=0),
            jnp.concatenate(values, axis=0),
            queries_of(g),
            jnp.concatenate(masks, axis=0),
        )

    def attend_at(*places):
        groups = [torus.at(dy, dz) for dy, dz in places]
        for g, found in zip(groups, attend([job_of(g) for g in groups])):
            partials.keep(g, *found)

    partials = Partials(
        torus, part, stat, out, out_stat, got, got_stat, part_send, part_recv
    )

    def write_cache(quarter):
        def chore():
            at = pl.ds(quarter * (tokens // 4), tokens // 4)
            every = slice(None)
            cache_ref[at] = jnp.stack(
                [
                    clip(acc[0, at, :] / smooth_ref[...], 0, every),
                    clip(acc[1, at, :], 1, every),
                ],
                axis=1,
            )

        return chore

    def attend_fresh():
        mask = (key % 8 == request) & (key // 8 <= (lane // 8) % (steps_reqs // 8))
        job = (
            clip(fresh_kv[0, :, mine] / my_smooth, 0, mine),
            clip(fresh_kv[1, :, mine], 1, mine),
            queries_of(me),
            mask,
        )
        partials.keep(CHIPS, *attend([job])[0])

    chores = [*(write_cache(quarter) for quarter in range(4)), attend_fresh]

    @pl.when(core == 0)
    def _():
        partials.y_first(attend_at, chores)

    @pl.when(core == 1)
    def _():
        partials.z_first(attend_at, chores)

    top, total, summed = partials.kept(me)
    done = (summed / total).T.astype(jnp.bfloat16)
    for h in range(heads):
        att_out[:, h * HD : (h + 1) * HD] = done[h * steps_reqs : (h + 1) * steps_reqs]
    own_att = pl.ds(pl.multiple_of(core * half_q, half_q), half_q)
    last = to_partner(2, att_out, att_ref.at[:, own_att])
    last.start()
    att_ref[:, own_att] = att_out[...]

    for s, refs in ((s_k, wk), (s_v, wv)):
        s.sent_copy(refs.at[pl.ds(0, CHIPS - 1), core]).wait_send()
        s.swap_copy(refs.at[:, core]).wait_send()
    s_qa.sent_copy(qs.at[pl.ds(0, CHIPS - 1), 0]).wait_send()
    s_qb.sent_copy(qs.at[pl.ds(0, CHIPS - 1), 1]).wait_send()
    heard(mz, 0, ring).wait_send()
    heard(my, 1, column).wait_send()
    keys_over.wait_send()
    values_over.wait_send()
    for k, refs in enumerate((out, out_stat)):
        pltpu.make_async_remote_copy(
            src_ref=refs.at[pl.ds(0, CHIPS - 1)],
            dst_ref=refs.at[pl.ds(0, CHIPS - 1)],
            send_sem=part_send.at[k],
            recv_sem=part_recv.at[k, 0, 0, 0],
            device_id={"rep": 1 - core},
            device_id_type=pl.DeviceIdType.MESH,
        ).wait_send()
    last.wait()


def decode(hidden, key_weight, value_weight, queries, group_scale, new_kv, found):
    tokens, depth = hidden.shape
    rows, columns = key_weight.shape
    step_reqs, q_columns = queries.shape
    pages = tokens // PAGE
    across = q_columns // 2 // HD * step_reqs
    bf16, f32 = jnp.bfloat16, jnp.float32
    any_spec = pl.BlockSpec(memory_space=pl.ANY)
    vmem = pl.BlockSpec(memory_space=pltpu.VMEM)
    smem = pl.BlockSpec(memory_space=pltpu.SMEM)
    return pl.pallas_call(
        decode_kernel,
        out_shape=(
            jax.ShapeDtypeStruct((tokens, 2, columns), bf16),
            jax.ShapeDtypeStruct((1, columns), f32),
            jax.ShapeDtypeStruct((step_reqs, q_columns), bf16),
        ),
        in_specs=[any_spec, any_spec, any_spec, any_spec, vmem, vmem, smem],
        out_specs=(vmem, vmem, vmem),
        scratch_shapes=[
            pltpu.VMEM((tokens, depth), bf16),
            pltpu.VMEM((CHIPS, 2, rows, columns), bf16),
            pltpu.VMEM((CHIPS, 2, rows, columns), bf16),
            pltpu.VMEM((2 * NZ, 8, columns), f32),
            pltpu.VMEM((NY, 8, columns), f32),
            pltpu.VMEM((CHIPS, 2, step_reqs // 2, q_columns // 2), bf16),
            pltpu.VMEM((2, tokens, columns), f32),
            pltpu.VMEM((tokens, HD), f32),
            pltpu.VMEM((2 * pages, PAGE, HD), bf16),
            pltpu.VMEM((2 * pages, PAGE, HD), bf16),
            pltpu.VMEM((pages, PAGE, HD), bf16),
            pltpu.VMEM((2, step_reqs, columns), f32),
            pltpu.VMEM((CHIPS + 1, HD, across), f32),
            pltpu.VMEM((CHIPS + 1, 2, across), f32),
            pltpu.VMEM((CHIPS, HD, across), bf16),
            pltpu.VMEM((CHIPS, 2, across), f32),
            pltpu.VMEM((2, 2, CHIPS, HD, across), bf16),
            pltpu.VMEM((2, 2, CHIPS, 2, across), f32),
            pltpu.VMEM((step_reqs, q_columns // 2), bf16),
            pltpu.SemaphoreType.DMA((4,)),
            pltpu.SemaphoreType.DMA((4,)),
            pltpu.SemaphoreType.DMA((4,)),
            pltpu.SemaphoreType.DMA((4, CHIPS)),
            pltpu.SemaphoreType.DMA((2,)),
            pltpu.SemaphoreType.DMA((2, NY)),
            pltpu.SemaphoreType.DMA((2, 2)),
            pltpu.SemaphoreType.DMA((3, 2)),
            pltpu.SemaphoreType.DMA((2,)),
            pltpu.SemaphoreType.DMA((2, 2, 2, CHIPS)),
        ],
        compiler_params=pltpu.CompilerParams(
            collective_id=0, has_side_effects=True, vmem_limit_bytes=60 * 2**20
        ),
        name="decode",
    )(hidden, key_weight, value_weight, queries, group_scale, new_kv, found)


def finish_kernel(*refs):
    outputs = len(refs) // 3
    sem = refs[-1]
    pieces = []
    for src, dst, via in zip(refs[:outputs], refs[outputs:], refs[2 * outputs :]):
        count = 4 if len(src.shape) == 3 else 1
        rows = src.shape[0] // count
        pieces += [
            tuple(r.at[pl.ds(k * rows, rows)] for r in (src, via, dst)) for k in range(count)
        ]
    legs = []
    for k, (src, via, dst) in enumerate(pieces):
        legs.append(
            (
                pltpu.make_async_copy(src, via, sem.at[k, 0]),
                pltpu.make_async_copy(via, dst, sem.at[k, 1]),
            )
        )
    for first, _ in legs:
        first.start()
    for first, second in legs:
        first.wait()
        second.start()
    for _, second in legs:
        second.wait()


def finish(*arrays):
    any_spec = pl.BlockSpec(memory_space=pl.ANY)
    return pl.pallas_call(
        finish_kernel,
        out_shape=tuple(jax.ShapeDtypeStruct(a.shape, a.dtype) for a in arrays),
        in_specs=[any_spec] * len(arrays),
        out_specs=(any_spec,) * len(arrays),
        scratch_shapes=[
            *(pltpu.VMEM(a.shape, a.dtype) for a in arrays),
            pltpu.SemaphoreType.DMA((6, 2)),
        ],
        name="finish",
    )(*arrays)


def on_device(
    hidden, key_weight, value_weight, group_scale, new_kv, decode_query, page_table, lengths
):
    steps, requests, q_columns = decode_query.shape
    columns = key_weight.shape[1]
    kv_cache, smoothing, attention = finish(
        *decode(
            hidden,
            key_weight,
            value_weight,
            decode_query.reshape(steps * requests, q_columns),
            group_scale,
            new_kv,
            find_pages(page_table, lengths),
        )
    )
    return (
        kv_cache,
        smoothing.reshape(columns),
        attention.reshape(steps, requests, q_columns),
    )


def solution(mesh):
    placed = (
        P(("seq", "rep"), None),
        P(("seq", "rep"), "head"),
        P(("seq", "rep"), "head"),
        P(None, "head"),
        P(None, "seq", None, "head"),
        P(None, "seq", "head"),
        P(),
        P(),
    )
    return jax.shard_map(
        on_device,
        mesh=mesh,
        in_specs=placed,
        out_specs=(P(("seq", "rep"), None, "head"), P("head"), P(None, "seq", "head")),
        check_vma=False,
    )
```

```python
import functools

import jax
import jax.numpy as jnp
from jax import lax
from jax.experimental import pallas as pl
from jax.experimental.pallas import tpu as pltpu
from jax.sharding import PartitionSpec as P

KVH = 8
HD = 128
QH = 64
PAGE = 32
NY = 4
NZ = 8
CHIPS = NY * NZ


EPSILON = 1e-05
NEGATIVE = -1e30
EMPTY = -1e29


class Torus:
    def __init__(self):
        seq = lax.axis_index("seq")
        self.y, self.z = lax.div(seq, NZ), lax.rem(seq, NZ)
        self.core = lax.axis_index("rep")

    def at(self, dy, dz):
        y = lax.rem(self.y + (dy + NY), NY)
        z = lax.rem(self.z + (dz + NZ), NZ)
        return y * NZ + z


class Stream:
    def __init__(self, torus, number, block, send_sem, recv_sem, swap, both_z=False):
        self.torus, self.number, self.block, self.both_z = torus, number, block, both_z
        self.send_sem, self.recv_sem, self.swap = send_sem, recv_sem, swap

    def copy(self, blk, dy, dz):
        ref = self.block(blk, self.torus.core)
        return pltpu.make_async_remote_copy(
            src_ref=ref,
            dst_ref=ref,
            send_sem=self.send_sem,
            recv_sem=self.recv_sem.at[blk],
            device_id={"seq": self.torus.at(dy, dz)},
            device_id_type=pl.DeviceIdType.MESH,
        )

    def across(self, blk):
        if self.swap is None:
            return
        ref = self.block(blk, self.torus.core)
        pltpu.make_async_remote_copy(
            src_ref=ref,
            dst_ref=ref,
            send_sem=self.swap[0],
            recv_sem=self.swap[1].at[lax.div(blk, NZ)],
            device_id={"rep": 1 - self.torus.core},
            device_id_type=pl.DeviceIdType.MESH,
        ).start()

    def arrived(self, dy, dz):
        blk = self.torus.at(dy, dz)
        self.copy(blk, 1, 0).wait_recv()
        return blk

    def along_z(self, blk, right, left):
        if right:
            self.copy(blk, 0, 1).start()
        if left:
            self.copy(blk, 0, -1).start()

    def along_y(self, blk, up, down):
        if up:
            self.copy(blk, 1, 0).start()
        if down:
            self.copy(blk, -1, 0).start()

    def step_z_first(self, st):
        turn_right = self.number % 2 == 0
        far = -4 if turn_right else 4
        reach = [[0], [-1, 1], [-2, 2], [-3, 3], [far]]
        if st == 0:
            blk = self.torus.at(0, 0)
            self.along_z(blk, True, True)
            self.along_y(blk, True, True)
            self.across(blk)
        if 1 <= st <= 4:
            for dz in reach[st]:
                blk = self.arrived(0, dz)
                onward = st < 3 or (st == 3 and (dz < 0) == turn_right)
                self.along_z(blk, onward and dz < 0, onward and dz > 0)
                self.along_y(blk, True, True)
                self.across(blk)
        if 1 <= st <= 5:
            for dz in reach[st - 1]:
                for dy in (-1, 1):
                    blk = self.arrived(dy, dz)
                    even = dz % 2 == 0
                    self.along_y(blk, even and dy < 0, not even and dy > 0)
                    self.across(blk)
        if 2 <= st <= 6:
            for dz in reach[st - 2]:
                self.across(self.arrived(2, dz))

    def step_y_first(self, st):
        even = self.number % 2 == 0
        if st == 0:
            blk = self.torus.at(0, 0)
            self.along_z(blk, True, True)
            self.along_y(blk, True, True)
            self.across(blk)
        if st == 1:
            for dy in (-1, 1):
                blk = self.arrived(dy, 0)
                self.along_y(blk, even and dy < 0, not even and dy > 0)
                self.along_z(blk, True, True)
                self.across(blk)
        if st == 2:
            blk = self.arrived(2, 0)
            self.along_z(blk, True, True)
            self.across(blk)
        for dy, first in ((0, 0), (-1, 1), (1, 1), (2, 2)):
            k = st - first
            turn_right = (self.number + dy) % 2 == 0
            if 1 <= k <= 3:
                for dz in (-k, k):
                    blk = self.arrived(dy, dz)
                    onward = k < 3 or (dz < 0) == turn_right
                    self.along_z(blk, onward and dz < 0, onward and dz > 0)
                    self.across(blk)
            if k == 4:
                self.across(self.arrived(dy, -4 if turn_right else 4))

    def step(self, st):
        if self.both_z:
            self.step_z_first(st)
            return

        @pl.when(self.torus.core == 0)
        def _():
            self.step_z_first(st)

        @pl.when(self.torus.core == 1)
        def _():
            self.step_y_first(st)

    def swap_copy(self, refs, row=0):
        return pltpu.make_async_remote_copy(
            src_ref=refs,
            dst_ref=refs,
            send_sem=self.swap[0],
            recv_sem=self.swap[1].at[row],
            device_id={"rep": 1 - self.torus.core},
            device_id_type=pl.DeviceIdType.MESH,
        )

    def sent_copy(self, refs):
        return pltpu.make_async_remote_copy(
            src_ref=refs,
            dst_ref=refs,
            send_sem=self.send_sem,
            recv_sem=self.recv_sem.at[0],
            device_id={"rep": 1 - self.torus.core},
            device_id_type=pl.DeviceIdType.MESH,
        )


STEPS_GATHER = 7
QUERY_LAG = 3
def friends(torus):
    ring = [(torus.at(0, dz), torus.core) for dz in (1, -1, 2, -2, 3, -3, 4)]
    ring += [(torus.at(0, dz), 1 - torus.core) for dz in (0, 1, -1, 2, -2, 3, -3, 4)]
    return ring, [(torus.at(dy, 0), torus.core) for dy in (1, -1, 2)]


def greet(torus):
    barrier = pltpu.get_barrier_semaphore()
    ring, column = friends(torus)
    for place, core in ring + column:
        pl.semaphore_signal(
            barrier,
            inc=1,
            device_id={"seq": place, "rep": core},
            device_id_type=pl.DeviceIdType.MESH,
        )
    pl.semaphore_wait(barrier, len(ring) + len(column))


SLOTS = 8


def find_pages(table, lengths):
    slots, requests = table.shape
    slot = lax.broadcasted_iota(jnp.int32, table.shape, 0)
    lane = lax.broadcasted_iota(jnp.int32, table.shape, 1)
    chip = lax.axis_index("seq")
    left = lengths - slot * PAGE
    mine = jnp.where((left > 0) & (table // (2 * PAGE) == chip), 1, 0)
    upto = mine
    for k in (1, 2, 4, 8, 16):
        upto = upto + jnp.where(slot >= k, pltpu.roll(upto, k, 0), 0)
    whole = jnp.broadcast_to(jnp.sum(mine, axis=0, keepdims=True), (8, requests))
    across = lax.broadcasted_iota(jnp.int32, whole.shape, 1) % 8
    before = whole
    for k in (1, 2, 4):
        before = before + jnp.where(across >= k, pltpu.roll(before, k, 1), 0)
    before = before - whole
    rank = jnp.where(mine > 0, upto - 1 + before[0:1], -1)
    fields = (lane % 8, table % (2 * PAGE), jnp.minimum(left, PAGE))
    picked = jnp.concatenate(
        [
            jnp.sum(jnp.where(rank == e, field, 0), axis=0, keepdims=True)
            for field in fields
            for e in range(SLOTS)
        ],
        axis=0,
    )
    side = lax.broadcasted_iota(jnp.int32, picked.shape, 1)
    for k in (1, 2, 4):
        other = jnp.where(
            side // k % 2 == 1, pltpu.roll(picked, k, 1), pltpu.roll(picked, requests - k, 1)
        )
        picked = picked + other
    return picked


Y_AXIS, Z_AXIS = 0, 1


def below(keys, queries):
    return lax.dot_general(
        keys, queries, (((1,), (1,)), ((), ())), preferred_element_type=jnp.float32
    )


def weighed(values, weights):
    return lax.dot_general(
        values, weights, (((0,), (0,)), ((), ())), preferred_element_type=jnp.float32
    )


def attend(jobs):
    scores = [
        jnp.where(mask, below(keys, queries) * HD ** (-0.5), NEGATIVE)
        for keys, _, queries, mask in jobs
    ]
    tops = [jnp.maximum(jnp.max(x, axis=0, keepdims=True), EMPTY) for x in scores]
    weights = [jnp.exp(x - top) for x, top in zip(scores, tops)]
    totals = [jnp.sum(x, axis=0, keepdims=True) for x in weights]
    sums = [weighed(job[1], x.astype(jnp.bfloat16)) for job, x in zip(jobs, weights)]
    return list(zip(tops, totals, sums))


def fold(parts):
    top = functools.reduce(jnp.maximum, [p[0] for p in parts])
    scales = [jnp.exp(p[0] - top) for p in parts]
    total = functools.reduce(jnp.add, [p[1] * s for p, s in zip(parts, scales)])
    summed = functools.reduce(jnp.add, [p[2] * s for p, s in zip(parts, scales)])
    return top, total, summed


class Partials:
    def __init__(self, torus, part, stat, out, out_stat, got, got_stat, send_sem, recv_sem):
        self.torus, self.part, self.stat = torus, part, stat
        self.out, self.out_stat = out, out_stat
        self.got, self.got_stat = got, got_stat
        self.send_sem, self.recv_sem = send_sem, recv_sem

    def copies(self, g, axis, way, slot=None, peer=None):
        step = 1 - 2 * way
        if peer is None:
            peer = self.torus.at(step, 0) if axis == Y_AXIS else self.torus.at(0, step)
        slot = g if slot is None else slot
        return [
            pltpu.make_async_remote_copy(
                src_ref=src.at[g],
                dst_ref=dst.at[axis, way, slot],
                send_sem=self.send_sem.at[k],
                recv_sem=self.recv_sem.at[k, axis, way, slot],
                device_id={"seq": peer},
                device_id_type=pl.DeviceIdType.MESH,
            )
            for k, (src, dst) in enumerate(
                ((self.out, self.got), (self.out_stat, self.got_stat))
            )
        ]

    def kept(self, at):
        return self.stat[at, 0:1], self.stat[at, 1:2], self.part[at]

    def keep(self, at, top, total, summed):
        self.part[at] = summed
        self.stat[at] = jnp.concatenate([top, total], axis=0)

    def gathered(self, g, arrivals, more=()):
        parts = [self.kept(g), *more]
        for axis, way, *direct in arrivals:
            slot = direct[0] if direct else g
            for copy in self.copies(g, axis, way, slot):
                copy.wait_recv()
            stat = self.got_stat[axis, way, slot]
            parts.append((stat[0:1], stat[1:2], self.got[axis, way, slot].astype(jnp.float32)))
        return fold(parts) if len(parts) > 1 else parts[0]

    def send(self, dy, dz, arrivals, axis, way, slot=None, peer=None):
        g = self.torus.at(dy, dz)
        top, total, summed = self.gathered(g, arrivals)
        self.out[g] = summed.astype(jnp.bfloat16)
        self.out_stat[g] = jnp.concatenate([top, total], axis=0)
        for copy in self.copies(g, axis, way, slot, peer):
            copy.start()

    def finish(self, arrivals, fresh):
        me = self.torus.at(0, 0)
        self.keep(me, *self.gathered(me, arrivals, more=(self.kept(fresh),)))

    def y_first(self, attend_at, chores):
        up, down = (Y_AXIS, 0), (Y_AXIS, 1)

        def far(k):
            dz = lax.rem(4 + 2 * k, NZ)
            attend_at((2, dz), (2, dz - 1))
            self.send(2, dz, (), *up)
            self.send(2, dz - 1, (), *down)

        def near(k):
            dz = lax.rem(4 + 2 * k, NZ)
            attend_at((1, dz - 1), (-1, dz))
            self.send(1, dz - 1, (), *up)
            self.send(-1, dz, (), *down)

        def near_passing(k):
            dz = lax.rem(4 + 2 * k, NZ)
            attend_at((1, dz), (-1, dz - 1))
            self.send(1, dz, (up,), *up)
            self.send(-1, dz - 1, (down,), *down)

        for body in (far, near, near_passing):
            repeat(NZ // 2, body)
        me = self.torus.at(0, 0)
        for pair in ((4, 3), (-2, -3), (0, -1), (2, 1)):
            attend_at(*((0, dz) for dz in pair))
            for dz in pair:
                if dz:
                    self.send(0, dz, (up, down), Z_AXIS, 0, me, self.torus.at(0, dz))
        for chore in chores:
            chore()
        straight = [(Z_AXIS, 0, self.torus.at(0, dz)) for dz in (1, -1, 2, -2, 3, -3, 4)]
        self.finish((up, down, *straight), CHIPS)

    def z_first(self, attend_at, chores):
        right, left = (Z_AXIS, 0), (Z_AXIS, 1)

        def far(k):
            dy = 2 - 2 * k
            attend_at((dy, 4), (dy - 1, 4))
            self.send(dy, 4, (), *right)
            self.send(dy - 1, 4, (), *left)

        def near(k):
            dy = 2 - 2 * k
            attend_at((dy, -3), (dy - 1, 3))
            self.send(dy, -3, (), *left)
            self.send(dy - 1, 3, (), *right)

        def near_passing(k):
            dy = 2 - 2 * k
            attend_at((dy, 3), (dy - 1, -3))
            self.send(dy, 3, (right,), *right)
            self.send(dy - 1, -3, (left,), *left)

        for body in (far, near, near_passing):
            repeat(NY // 2, body)

        def both(dz):
            def body(k):
                dy = 2 - k
                attend_at((dy, dz), (dy, -dz))
                self.send(dy, dz, (right,), *right)
                self.send(dy, -dz, (left,), *left)

            return body

        for dz in (2, 1):
            repeat(NY, both(dz))
        repeat(NY // 2, lambda k: attend_at((2 - 2 * k, 0), (1 - 2 * k, 0)))
        for chore in chores[:2]:
            chore()
        me = self.torus.at(0, 0)
        for dy in (2, 1, -1):
            self.send(dy, 0, (right, left), Y_AXIS, 0, me, self.torus.at(dy, 0))
        for chore in chores[2:]:
            chore()
        straight = [(Y_AXIS, 0, self.torus.at(dy, 0)) for dy in (1, -1, 2)]
        self.finish((right, left, *straight), CHIPS)


def repeat(count, body):
    def step(k, carry):
        body(k)
        return carry

    lax.fori_loop(0, count, step, 0)


def decode_kernel(
    hidden_hbm, wk_hbm, wv_hbm, query_hbm, scale_ref, new_ref, table_ref, length_ref,
    cache_ref, smooth_ref, att_ref,
    hid, wk, wv, mz, my, qs, acc, kraw, kbuf, vbuf, vout, fresh_kv, found_v, found_ref, part, stat, out, out_stat, got, got_stat,
    att_out,
    local_sem, hid_sem, send_sem, recv_sem, swap_send, swap_recv, peak_sem, half_sem,
    part_send, part_recv,
):
    torus = Torus()
    me, core = torus.at(0, 0), torus.core
    tokens, depth = hidden_hbm.shape
    columns = wk_hbm.shape[1]
    steps_reqs = query_hbm.shape[0]
    half_q = query_hbm.shape[1] // 2
    heads = half_q // HD
    pages = tokens // PAGE
    parts = 4
    width = depth // parts
    own_k = pltpu.make_async_copy(wk_hbm, wk.at[me, core], local_sem.at[0])
    own_v = pltpu.make_async_copy(wv_hbm, wv.at[me, core], local_sem.at[1])
    own_q = [
        pltpu.make_async_copy(
            query_hbm.at[
                pl.ds(k * (steps_reqs // 2), steps_reqs // 2),
                pl.ds(pl.multiple_of(core * half_q, half_q), half_q),
            ],
            qs.at[me, k],
            local_sem.at[2 + k],
        )
        for k in range(2)
    ]
    own_k.start()
    own_v.start()
    for copy in own_q:
        copy.start()
    hid_copies = [
        pltpu.make_async_copy(
            hidden_hbm.at[:, pl.ds(k * width, width)],
            hid.at[:, pl.ds(k * width, width)],
            hid_sem.at[k],
        )
        for k in range(parts)
    ]
    for copy in hid_copies:
        copy.start()
    greet(torus)
    own_k.wait()

    def stream(number, block, swap=True, both_z=False):
        return Stream(
            torus,
            number,
            block,
            send_sem.at[number],
            recv_sem.at[number],
            (swap_send.at[number], swap_recv.at[number]) if swap else None,
            both_z,
        )

    s_k = stream(0, lambda blk, c: wk.at[blk, c])
    s_v = stream(1, lambda blk, c: wv.at[blk, c])
    s_qa = stream(2, lambda blk, c: qs.at[blk, 0], swap=False)
    s_qb = stream(3, lambda blk, c: qs.at[blk, 1], swap=False, both_z=True)
    rows = 512

    def multiply(stream, weights, to, dy):
        y = lax.rem(torus.y + (dy + NY), NY)
        blocks = pl.ds(pl.multiple_of(y * NZ, NZ), NZ)
        stream.swap_copy(weights.at[blocks, 1 - core], y).wait_recv()

        def one(m, carry):
            at = pl.ds(pl.multiple_of(m * rows, rows), rows)
            w = weights[blocks].reshape(width, weights.shape[3])
            product = jnp.dot(
                hid[at, pl.ds(pl.multiple_of(y * width, width), width)],
                w,
                preferred_element_type=jnp.float32,
            )
            to[at, :] = product if dy == 0 else to[at, :] + product
            return carry

        lax.fori_loop(0, tokens // rows, one, 0)

    mine = pl.ds(pl.multiple_of(core * HD, HD), HD)
    theirs = pl.ds(pl.multiple_of((1 - core) * HD, HD), HD)
    my_pages = pl.ds(pl.multiple_of(core * pages, pages), pages)
    their_pages = pl.ds(pl.multiple_of((1 - core) * pages, pages), pages)

    def to_partner(k, src, dst):
        return pltpu.make_async_remote_copy(
            src_ref=src,
            dst_ref=dst,
            send_sem=half_sem.at[k, 0],
            recv_sem=half_sem.at[k, 1],
            device_id={"rep": 1 - core},
            device_id_type=pl.DeviceIdType.MESH,
        )

    def clip(x, kind, lanes):
        scale = scale_ref[kind : kind + 1, lanes]
        return jnp.clip(x, -8.0 * scale, 7.0 * scale).astype(jnp.bfloat16)

    keys_over = to_partner(0, acc.at[0, :, theirs], kraw)
    values_over = to_partner(1, vout, vbuf.at[my_pages])
    found_copy = pltpu.make_async_copy(found_v, found_ref, local_sem.at[4])

    ring, column = friends(torus)
    place = core * NZ + torus.z

    def peak_copy(refs, slot, k, target):
        return pltpu.make_async_remote_copy(
            src_ref=refs.at[slot],
            dst_ref=refs.at[slot],
            send_sem=peak_sem.at[k, 0],
            recv_sem=peak_sem.at[k, 1],
            device_id={"seq": target[0], "rep": target[1]},
            device_id_type=pl.DeviceIdType.MESH,
        )

    def tell(refs, slot, k, peers):
        for target in peers:
            peak_copy(refs, slot, k, target).start()

    def heard(refs, k, peers):
        return peak_copy(refs, pl.ds(0, len(peers)), k, peers[0])

    q_lag = QUERY_LAG
    for i in range(q_lag + STEPS_GATHER):
        if i == 0:
            own_v.wait()
        if i == q_lag:
            for copy in own_q:
                copy.wait()
        for stream_i, start in ((s_k, 0), (s_v, 1), (s_qa, q_lag), (s_qb, q_lag)):
            if i == 5 and stream_i is s_qa:
                for copy in hid_copies:
                    copy.wait()
                multiply(s_k, wk, acc.at[0], 0)
            if 0 <= i - start < STEPS_GATHER:
                stream_i.step(i - start)
        if i == 0:
            found_v[...] = find_pages(table_ref[...], length_ref[...])
            for kind in range(2):
                fresh_kv[kind] = (
                    new_ref[:, :, kind, :].astype(jnp.float32).reshape(steps_reqs, columns)
                )
        if i == 4:
            found_copy.start()
        if i == 5:
            multiply(s_k, wk, acc.at[0], 1)
            multiply(s_k, wk, acc.at[0], -1)
        if i == 6:
            multiply(s_k, wk, acc.at[0], 2)
            mz[place] = jnp.max(jnp.abs(acc[0]).reshape(tokens // 8, 8, columns), axis=0)
            tell(mz, place, 0, ring)
            keys_over.start()
            multiply(s_v, wv, acc.at[1], 0)
        if i == 7:
            multiply(s_v, wv, acc.at[1], 1)
            multiply(s_v, wv, acc.at[1], -1)
        if i == 8:
            heard(mz, 0, ring).wait_recv()
            my[torus.y] = jnp.max(mz[...], axis=0)
            tell(my, torus.y, 1, column)
            multiply(s_v, wv, acc.at[1], 2)
            vout[...] = clip(acc[1, :, theirs], 1, theirs).reshape(vout.shape)
            values_over.start()
            vbuf[my_pages] = clip(acc[1, :, mine], 1, mine).reshape(vout.shape)
    found_copy.wait()
    heard(my, 1, column).wait_recv()
    peak = jnp.max(my[...], axis=0)
    smooth_ref[...] = jnp.sqrt(jnp.max(peak, axis=0, keepdims=True) + EPSILON)
    my_smooth = smooth_ref[:, mine]

    def queries_of(g):
        return jnp.concatenate(
            [
                (
                    qs[g, :, :, h * HD : (h + 1) * HD]
                    .reshape(steps_reqs, HD)
                    .astype(jnp.float32)
                    * my_smooth
                ).astype(jnp.bfloat16)
                for h in range(heads)
            ],
            axis=0,
        )

    across = heads * steps_reqs
    lane = lax.broadcasted_iota(jnp.int32, (PAGE, across), 1)
    key = lax.broadcasted_iota(jnp.int32, (PAGE, across), 0)
    request = lane % 8

    kbuf[my_pages] = clip(acc[0, :, mine] / my_smooth, 0, mine).reshape(vout.shape)
    keys_over.wait_recv()
    kbuf[their_pages] = clip(kraw[...] / my_smooth, 0, mine).reshape(vout.shape)
    to_partner(1, vout, vbuf.at[their_pages]).wait_recv()

    def job_of(g):
        keys, values, masks = [], [], []
        for e in range(SLOTS):
            who, page, count = (found_ref[SLOTS * f + e, g * 8] for f in range(3))
            keys.append(kbuf[page])
            values.append(vbuf[page])
            masks.append((request == who) & (key < count))
        return (
            jnp.concatenate(keys, axis=0),
            jnp.concatenate(values, axis=0),
            queries_of(g),
            jnp.concatenate(masks, axis=0),
        )

    def attend_at(*places):
        groups = [torus.at(dy, dz) for dy, dz in places]
        for g, found in zip(groups, attend([job_of(g) for g in groups])):
            partials.keep(g, *found)

    partials = Partials(
        torus, part, stat, out, out_stat, got, got_stat, part_send, part_recv
    )

    def write_cache(quarter):
        def chore():
            at = pl.ds(quarter * (tokens // 4), tokens // 4)
            every = slice(None)
            cache_ref[at] = jnp.stack(
                [
                    clip(acc[0, at, :] / smooth_ref[...], 0, every),
                    clip(acc[1, at, :], 1, every),
                ],
                axis=1,
            )

        return chore

    def attend_fresh():
        mask = (key % 8 == request) & (key // 8 <= (lane // 8) % (steps_reqs // 8))
        job = (
            clip(fresh_kv[0, :, mine] / my_smooth, 0, mine),
            clip(fresh_kv[1, :, mine], 1, mine),
            queries_of(me),
            mask,
        )
        partials.keep(CHIPS, *attend([job])[0])

    chores = [*(write_cache(quarter) for quarter in range(4)), attend_fresh]

    @pl.when(core == 0)
    def _():
        partials.y_first(attend_at, chores)

    @pl.when(core == 1)
    def _():
        partials.z_first(attend_at, chores)

    top, total, summed = partials.kept(me)
    done = (summed / total).T.astype(jnp.bfloat16)
    for h in range(heads):
        att_out[:, h * HD : (h + 1) * HD] = done[h * steps_reqs : (h + 1) * steps_reqs]
    own_att = pl.ds(pl.multiple_of(core * half_q, half_q), half_q)
    last = to_partner(2, att_out, att_ref.at[:, own_att])
    last.start()
    att_ref[:, own_att] = att_out[...]

    for s, refs in ((s_k, wk), (s_v, wv)):
        s.sent_copy(refs.at[pl.ds(0, CHIPS - 1), core]).wait_send()
        s.swap_copy(refs.at[:, core]).wait_send()
    s_qa.sent_copy(qs.at[pl.ds(0, CHIPS - 1), 0]).wait_send()
    s_qb.sent_copy(qs.at[pl.ds(0, CHIPS - 1), 1]).wait_send()
    heard(mz, 0, ring).wait_send()
    heard(my, 1, column).wait_send()
    keys_over.wait_send()
    values_over.wait_send()
    for k, refs in enumerate((out, out_stat)):
        pltpu.make_async_remote_copy(
            src_ref=refs.at[pl.ds(0, CHIPS - 1)],
            dst_ref=refs.at[pl.ds(0, CHIPS - 1)],
            send_sem=part_send.at[k],
            recv_sem=part_recv.at[k, 0, 0, 0],
            device_id={"rep": 1 - core},
            device_id_type=pl.DeviceIdType.MESH,
        ).wait_send()
    last.wait()


def decode(hidden, key_weight, value_weight, queries, group_scale, new_kv, table, lengths):
    tokens, depth = hidden.shape
    rows, columns = key_weight.shape
    step_reqs, q_columns = queries.shape
    pages = tokens // PAGE
    across = q_columns // 2 // HD * step_reqs
    bf16, f32 = jnp.bfloat16, jnp.float32
    any_spec = pl.BlockSpec(memory_space=pl.ANY)
    vmem = pl.BlockSpec(memory_space=pltpu.VMEM)
    return pl.pallas_call(
        decode_kernel,
        out_shape=(
            jax.ShapeDtypeStruct((tokens, 2, columns), bf16),
            jax.ShapeDtypeStruct((1, columns), f32),
            jax.ShapeDtypeStruct((step_reqs, q_columns), bf16),
        ),
        in_specs=[any_spec, any_spec, any_spec, any_spec, vmem, vmem, vmem, vmem],
        out_specs=(vmem, vmem, vmem),
        scratch_shapes=[
            pltpu.VMEM((tokens, depth), bf16),
            pltpu.VMEM((CHIPS, 2, rows, columns), bf16),
            pltpu.VMEM((CHIPS, 2, rows, columns), bf16),
            pltpu.VMEM((2 * NZ, 8, columns), f32),
            pltpu.VMEM((NY, 8, columns), f32),
            pltpu.VMEM((CHIPS, 2, step_reqs // 2, q_columns // 2), bf16),
            pltpu.VMEM((2, tokens, columns), f32),
            pltpu.VMEM((tokens, HD), f32),
            pltpu.VMEM((2 * pages, PAGE, HD), bf16),
            pltpu.VMEM((2 * pages, PAGE, HD), bf16),
            pltpu.VMEM((pages, PAGE, HD), bf16),
            pltpu.VMEM((2, step_reqs, columns), f32),
            pltpu.VMEM((3 * SLOTS, lengths.shape[1]), jnp.int32),
            pltpu.SMEM((3 * SLOTS, lengths.shape[1]), jnp.int32),
            pltpu.VMEM((CHIPS + 1, HD, across), f32),
            pltpu.VMEM((CHIPS + 1, 2, across), f32),
            pltpu.VMEM((CHIPS, HD, across), bf16),
            pltpu.VMEM((CHIPS, 2, across), f32),
            pltpu.VMEM((2, 2, CHIPS, HD, across), bf16),
            pltpu.VMEM((2, 2, CHIPS, 2, across), f32),
            pltpu.VMEM((step_reqs, q_columns // 2), bf16),
            pltpu.SemaphoreType.DMA((5,)),
            pltpu.SemaphoreType.DMA((4,)),
            pltpu.SemaphoreType.DMA((4,)),
            pltpu.SemaphoreType.DMA((4, CHIPS)),
            pltpu.SemaphoreType.DMA((2,)),
            pltpu.SemaphoreType.DMA((2, NY)),
            pltpu.SemaphoreType.DMA((2, 2)),
            pltpu.SemaphoreType.DMA((3, 2)),
            pltpu.SemaphoreType.DMA((2,)),
            pltpu.SemaphoreType.DMA((2, 2, 2, CHIPS)),
        ],
        compiler_params=pltpu.CompilerParams(
            collective_id=0, has_side_effects=True, vmem_limit_bytes=60 * 2**20
        ),
        name="decode",
    )(hidden, key_weight, value_weight, queries, group_scale, new_kv, table, lengths)


def finish_kernel(*refs):
    outputs = len(refs) // 3
    sem = refs[-1]
    pieces = []
    for src, dst, via in zip(refs[:outputs], refs[outputs:], refs[2 * outputs :]):
        count = 4 if len(src.shape) == 3 else 1
        rows = src.shape[0] // count
        pieces += [
            tuple(r.at[pl.ds(k * rows, rows)] for r in (src, via, dst)) for k in range(count)
        ]
    legs = []
    for k, (src, via, dst) in enumerate(pieces):
        legs.append(
            (
                pltpu.make_async_copy(src, via, sem.at[k, 0]),
                pltpu.make_async_copy(via, dst, sem.at[k, 1]),
            )
        )
    for first, _ in legs:
        first.start()
    for first, second in legs:
        first.wait()
        second.start()
    for _, second in legs:
        second.wait()


def finish(*arrays):
    any_spec = pl.BlockSpec(memory_space=pl.ANY)
    return pl.pallas_call(
        finish_kernel,
        out_shape=tuple(jax.ShapeDtypeStruct(a.shape, a.dtype) for a in arrays),
        in_specs=[any_spec] * len(arrays),
        out_specs=(any_spec,) * len(arrays),
        scratch_shapes=[
            *(pltpu.VMEM(a.shape, a.dtype) for a in arrays),
            pltpu.SemaphoreType.DMA((6, 2)),
        ],
        name="finish",
    )(*arrays)


def on_device(
    hidden, key_weight, value_weight, group_scale, new_kv, decode_query, page_table, lengths
):
    steps, requests, q_columns = decode_query.shape
    columns = key_weight.shape[1]
    kv_cache, smoothing, attention = finish(
        *decode(
            hidden,
            key_weight,
            value_weight,
            decode_query.reshape(steps * requests, q_columns),
            group_scale,
            new_kv,
            page_table.T,
            lengths.reshape(1, -1),
        )
    )
    return (
        kv_cache,
        smoothing.reshape(columns),
        attention.reshape(steps, requests, q_columns),
    )


def solution(mesh):
    placed = (
        P(("seq", "rep"), None),
        P(("seq", "rep"), "head"),
        P(("seq", "rep"), "head"),
        P(None, "head"),
        P(None, "seq", None, "head"),
        P(None, "seq", "head"),
        P(),
        P(),
    )
    return jax.shard_map(
        on_device,
        mesh=mesh,
        in_specs=placed,
        out_specs=(P(("seq", "rep"), None, "head"), P("head"), P(None, "seq", "head")),
        check_vma=False,
    )
```

```python
import functools

import jax
import jax.numpy as jnp
from jax import lax
from jax.experimental import pallas as pl
from jax.experimental.pallas import tpu as pltpu
from jax.sharding import PartitionSpec as P

KVH = 8
HD = 128
QH = 64
PAGE = 32
NY = 4
NZ = 8
CHIPS = NY * NZ


EPSILON = 1e-05
NEGATIVE = -1e30
EMPTY = -1e29


class Torus:
    def __init__(self):
        seq = lax.axis_index("seq")
        self.y, self.z = lax.div(seq, NZ), lax.rem(seq, NZ)
        self.core = lax.axis_index("rep")

    def at(self, dy, dz):
        y = lax.rem(self.y + (dy + NY), NY)
        z = lax.rem(self.z + (dz + NZ), NZ)
        return y * NZ + z


class Stream:
    def __init__(self, torus, number, block, send_sem, recv_sem, swap, both_z=False):
        self.torus, self.number, self.block, self.both_z = torus, number, block, both_z
        self.send_sem, self.recv_sem, self.swap = send_sem, recv_sem, swap

    def copy(self, blk, dy, dz):
        ref = self.block(blk, self.torus.core)
        return pltpu.make_async_remote_copy(
            src_ref=ref,
            dst_ref=ref,
            send_sem=self.send_sem,
            recv_sem=self.recv_sem.at[blk],
            device_id={"seq": self.torus.at(dy, dz)},
            device_id_type=pl.DeviceIdType.MESH,
        )

    def across(self, blk):
        if self.swap is None:
            return
        ref = self.block(blk, self.torus.core)
        pltpu.make_async_remote_copy(
            src_ref=ref,
            dst_ref=ref,
            send_sem=self.swap[0],
            recv_sem=self.swap[1].at[lax.div(blk, NZ)],
            device_id={"rep": 1 - self.torus.core},
            device_id_type=pl.DeviceIdType.MESH,
        ).start()

    def arrived(self, dy, dz):
        blk = self.torus.at(dy, dz)
        self.copy(blk, 1, 0).wait_recv()
        return blk

    def along_z(self, blk, right, left):
        if right:
            self.copy(blk, 0, 1).start()
        if left:
            self.copy(blk, 0, -1).start()

    def along_y(self, blk, up, down):
        if up:
            self.copy(blk, 1, 0).start()
        if down:
            self.copy(blk, -1, 0).start()

    def step_z_first(self, st):
        turn_right = self.number % 2 == 0
        far = -4 if turn_right else 4
        reach = [[0], [-1, 1], [-2, 2], [-3, 3], [far]]
        if st == 0:
            blk = self.torus.at(0, 0)
            self.along_z(blk, True, True)
            self.along_y(blk, True, True)
            self.across(blk)
        if 1 <= st <= 4:
            for dz in reach[st]:
                blk = self.arrived(0, dz)
                onward = st < 3 or (st == 3 and (dz < 0) == turn_right)
                self.along_z(blk, onward and dz < 0, onward and dz > 0)
                self.along_y(blk, True, True)
                self.across(blk)
        if 1 <= st <= 5:
            for dz in reach[st - 1]:
                for dy in (-1, 1):
                    blk = self.arrived(dy, dz)
                    even = dz % 2 == 0
                    self.along_y(blk, even and dy < 0, not even and dy > 0)
                    self.across(blk)
        if 2 <= st <= 6:
            for dz in reach[st - 2]:
                self.across(self.arrived(2, dz))

    def step_y_first(self, st):
        even = self.number % 2 == 0
        if st == 0:
            blk = self.torus.at(0, 0)
            self.along_z(blk, True, True)
            self.along_y(blk, True, True)
            self.across(blk)
        if st == 1:
            for dy in (-1, 1):
                blk = self.arrived(dy, 0)
                self.along_y(blk, even and dy < 0, not even and dy > 0)
                self.along_z(blk, True, True)
                self.across(blk)
        if st == 2:
            blk = self.arrived(2, 0)
            self.along_z(blk, True, True)
            self.across(blk)
        for dy, first in ((0, 0), (-1, 1), (1, 1), (2, 2)):
            k = st - first
            turn_right = (self.number + dy) % 2 == 0
            if 1 <= k <= 3:
                for dz in (-k, k):
                    blk = self.arrived(dy, dz)
                    onward = k < 3 or (dz < 0) == turn_right
                    self.along_z(blk, onward and dz < 0, onward and dz > 0)
                    self.across(blk)
            if k == 4:
                self.across(self.arrived(dy, -4 if turn_right else 4))

    def step(self, st):
        if self.both_z:
            self.step_z_first(st)
            return

        @pl.when(self.torus.core == 0)
        def _():
            self.step_z_first(st)

        @pl.when(self.torus.core == 1)
        def _():
            self.step_y_first(st)

    def swap_copy(self, refs, row=0):
        return pltpu.make_async_remote_copy(
            src_ref=refs,
            dst_ref=refs,
            send_sem=self.swap[0],
            recv_sem=self.swap[1].at[row],
            device_id={"rep": 1 - self.torus.core},
            device_id_type=pl.DeviceIdType.MESH,
        )

    def sent_copy(self, refs):
        return pltpu.make_async_remote_copy(
            src_ref=refs,
            dst_ref=refs,
            send_sem=self.send_sem,
            recv_sem=self.recv_sem.at[0],
            device_id={"rep": 1 - self.torus.core},
            device_id_type=pl.DeviceIdType.MESH,
        )


STEPS_GATHER = 7
QUERY_LAG = 3
def friends(torus):
    ring = [(torus.at(0, dz), torus.core) for dz in (1, -1, 2, -2, 3, -3, 4)]
    ring += [(torus.at(0, dz), 1 - torus.core) for dz in (0, 1, -1, 2, -2, 3, -3, 4)]
    return ring, [(torus.at(dy, 0), torus.core) for dy in (1, -1, 2)]


def greet(torus):
    barrier = pltpu.get_barrier_semaphore()
    ring, column = friends(torus)
    for place, core in ring + column:
        pl.semaphore_signal(
            barrier,
            inc=1,
            device_id={"seq": place, "rep": core},
            device_id_type=pl.DeviceIdType.MESH,
        )
    pl.semaphore_wait(barrier, len(ring) + len(column))


SLOTS = 8


def find_pages(table, lengths):
    slots, requests = table.shape
    slot = lax.broadcasted_iota(jnp.int32, table.shape, 0)
    lane = lax.broadcasted_iota(jnp.int32, table.shape, 1)
    chip = lax.axis_index("seq")
    left = lengths - slot * PAGE
    mine = jnp.where((left > 0) & (table // (2 * PAGE) == chip), 1, 0)
    upto = mine
    for k in (1, 2, 4, 8, 16):
        upto = upto + jnp.where(slot >= k, pltpu.roll(upto, k, 0), 0)
    whole = jnp.broadcast_to(jnp.sum(mine, axis=0, keepdims=True), (8, requests))
    across = lax.broadcasted_iota(jnp.int32, whole.shape, 1) % 8
    before = whole
    for k in (1, 2, 4):
        before = before + jnp.where(across >= k, pltpu.roll(before, k, 1), 0)
    before = before - whole
    rank = jnp.where(mine > 0, upto - 1 + before[0:1], -1)
    fields = (lane % 8, table % (2 * PAGE), jnp.minimum(left, PAGE))
    picked = jnp.concatenate(
        [
            jnp.sum(jnp.where(rank == e, field, 0), axis=0, keepdims=True)
            for field in fields
            for e in range(SLOTS)
        ],
        axis=0,
    )
    side = lax.broadcasted_iota(jnp.int32, picked.shape, 1)
    for k in (1, 2, 4):
        other = jnp.where(
            side // k % 2 == 1, pltpu.roll(picked, k, 1), pltpu.roll(picked, requests - k, 1)
        )
        picked = picked + other
    return picked


Y_AXIS, Z_AXIS = 0, 1


def below(keys, queries):
    return lax.dot_general(
        keys, queries, (((1,), (1,)), ((), ())), preferred_element_type=jnp.float32
    )


def weighed(values, weights):
    return lax.dot_general(
        values, weights, (((0,), (0,)), ((), ())), preferred_element_type=jnp.float32
    )


def attend(jobs):
    scores = [
        jnp.where(mask, below(keys, queries) * HD ** (-0.5), NEGATIVE)
        for keys, _, queries, mask in jobs
    ]
    tops = [jnp.maximum(jnp.max(x, axis=0, keepdims=True), EMPTY) for x in scores]
    weights = [jnp.exp(x - top) for x, top in zip(scores, tops)]
    totals = [jnp.sum(x, axis=0, keepdims=True) for x in weights]
    sums = [weighed(job[1], x.astype(jnp.bfloat16)) for job, x in zip(jobs, weights)]
    return list(zip(tops, totals, sums))


def fold(parts):
    top = functools.reduce(jnp.maximum, [p[0] for p in parts])
    scales = [jnp.exp(p[0] - top) for p in parts]
    total = functools.reduce(jnp.add, [p[1] * s for p, s in zip(parts, scales)])
    summed = functools.reduce(jnp.add, [p[2] * s for p, s in zip(parts, scales)])
    return top, total, summed


class Partials:
    def __init__(self, torus, part, stat, out, out_stat, got, got_stat, send_sem, recv_sem):
        self.torus, self.part, self.stat = torus, part, stat
        self.out, self.out_stat = out, out_stat
        self.got, self.got_stat = got, got_stat
        self.send_sem, self.recv_sem = send_sem, recv_sem

    def copies(self, g, axis, way, slot=None, peer=None):
        step = 1 - 2 * way
        if peer is None:
            peer = self.torus.at(step, 0) if axis == Y_AXIS else self.torus.at(0, step)
        slot = g if slot is None else slot
        return [
            pltpu.make_async_remote_copy(
                src_ref=src.at[g],
                dst_ref=dst.at[axis, way, slot],
                send_sem=self.send_sem.at[k],
                recv_sem=self.recv_sem.at[k, axis, way, slot],
                device_id={"seq": peer},
                device_id_type=pl.DeviceIdType.MESH,
            )
            for k, (src, dst) in enumerate(
                ((self.out, self.got), (self.out_stat, self.got_stat))
            )
        ]

    def kept(self, at):
        return self.stat[at, 0:1], self.stat[at, 1:2], self.part[at]

    def keep(self, at, top, total, summed):
        self.part[at] = summed
        self.stat[at] = jnp.concatenate([top, total], axis=0)

    def gathered(self, g, arrivals, more=()):
        parts = [self.kept(g), *more]
        for axis, way, *direct in arrivals:
            slot = direct[0] if direct else g
            for copy in self.copies(g, axis, way, slot):
                copy.wait_recv()
            stat = self.got_stat[axis, way, slot]
            parts.append((stat[0:1], stat[1:2], self.got[axis, way, slot].astype(jnp.float32)))
        return fold(parts) if len(parts) > 1 else parts[0]

    def send(self, dy, dz, arrivals, axis, way, slot=None, peer=None):
        g = self.torus.at(dy, dz)
        top, total, summed = self.gathered(g, arrivals)
        self.out[g] = summed.astype(jnp.bfloat16)
        self.out_stat[g] = jnp.concatenate([top, total], axis=0)
        for copy in self.copies(g, axis, way, slot, peer):
            copy.start()

    def finish(self, arrivals, fresh):
        me = self.torus.at(0, 0)
        self.keep(me, *self.gathered(me, arrivals, more=(self.kept(fresh),)))

    def y_first(self, attend_at, chores):
        up, down = (Y_AXIS, 0), (Y_AXIS, 1)

        def far(k):
            dz = lax.rem(4 + 2 * k, NZ)
            attend_at((2, dz), (2, dz - 1))
            self.send(2, dz, (), *up)
            self.send(2, dz - 1, (), *down)

        def near(k):
            dz = lax.rem(4 + 2 * k, NZ)
            attend_at((1, dz - 1), (-1, dz))
            self.send(1, dz - 1, (), *up)
            self.send(-1, dz, (), *down)

        def near_passing(k):
            dz = lax.rem(4 + 2 * k, NZ)
            attend_at((1, dz), (-1, dz - 1))
            self.send(1, dz, (up,), *up)
            self.send(-1, dz - 1, (down,), *down)

        for body in (far, near, near_passing):
            repeat(NZ // 2, body)
        me = self.torus.at(0, 0)
        for pair in ((4, 3), (-2, -3), (0, -1), (2, 1)):
            attend_at(*((0, dz) for dz in pair))
            for dz in pair:
                if dz:
                    self.send(0, dz, (up, down), Z_AXIS, 0, me, self.torus.at(0, dz))
        for chore in chores:
            chore()
        straight = [(Z_AXIS, 0, self.torus.at(0, dz)) for dz in (1, -1, 2, -2, 3, -3, 4)]
        self.finish((up, down, *straight), CHIPS)

    def z_first(self, attend_at, chores):
        right, left = (Z_AXIS, 0), (Z_AXIS, 1)

        def far(k):
            dy = 2 - 2 * k
            attend_at((dy, 4), (dy - 1, 4))
            self.send(dy, 4, (), *right)
            self.send(dy - 1, 4, (), *left)

        def near(k):
            dy = 2 - 2 * k
            attend_at((dy, -3), (dy - 1, 3))
            self.send(dy, -3, (), *left)
            self.send(dy - 1, 3, (), *right)

        def near_passing(k):
            dy = 2 - 2 * k
            attend_at((dy, 3), (dy - 1, -3))
            self.send(dy, 3, (right,), *right)
            self.send(dy - 1, -3, (left,), *left)

        for body in (far, near, near_passing):
            repeat(NY // 2, body)

        def both(dz):
            def body(k):
                dy = 2 - k
                attend_at((dy, dz), (dy, -dz))
                self.send(dy, dz, (right,), *right)
                self.send(dy, -dz, (left,), *left)

            return body

        for dz in (2, 1):
            repeat(NY, both(dz))
        repeat(NY // 2, lambda k: attend_at((2 - 2 * k, 0), (1 - 2 * k, 0)))
        for chore in chores[:2]:
            chore()
        me = self.torus.at(0, 0)
        for dy in (2, 1, -1):
            self.send(dy, 0, (right, left), Y_AXIS, 0, me, self.torus.at(dy, 0))
        for chore in chores[2:]:
            chore()
        straight = [(Y_AXIS, 0, self.torus.at(dy, 0)) for dy in (1, -1, 2)]
        self.finish((right, left, *straight), CHIPS)


def repeat(count, body):
    def step(k, carry):
        body(k)
        return carry

    lax.fori_loop(0, count, step, 0)


def decode_kernel(
    hidden_hbm, wk_hbm, wv_hbm, query_hbm, scale_ref, new_ref, table_ref, length_ref,
    cache_ref, smooth_ref, att_ref,
    hid, wk, wv, mz, my, qs, acc, kraw, kbuf, vbuf, vout, fresh_kv, found_v, found_ref, part, stat, out, out_stat, got, got_stat,
    att_out,
    local_sem, hid_sem, send_sem, recv_sem, swap_send, swap_recv, peak_sem, half_sem,
    part_send, part_recv,
):
    torus = Torus()
    me, core = torus.at(0, 0), torus.core
    tokens, depth = hidden_hbm.shape
    columns = wk_hbm.shape[1]
    steps_reqs = query_hbm.shape[0]
    half_q = query_hbm.shape[1] // 2
    heads = half_q // HD
    pages = tokens // PAGE
    parts = 4
    width = depth // parts
    own_k = pltpu.make_async_copy(wk_hbm, wk.at[me, core], local_sem.at[0])
    own_v = pltpu.make_async_copy(wv_hbm, wv.at[me, core], local_sem.at[1])
    own_q = [
        pltpu.make_async_copy(
            query_hbm.at[
                pl.ds(k * (steps_reqs // 2), steps_reqs // 2),
                pl.ds(pl.multiple_of(core * half_q, half_q), half_q),
            ],
            qs.at[me, k],
            local_sem.at[2 + k],
        )
        for k in range(2)
    ]
    own_k.start()
    own_v.start()
    for copy in own_q:
        copy.start()
    hid_copies = [
        pltpu.make_async_copy(
            hidden_hbm.at[:, pl.ds(k * width, width)],
            hid.at[:, pl.ds(k * width, width)],
            hid_sem.at[k],
        )
        for k in range(parts)
    ]
    for copy in hid_copies:
        copy.start()
    greet(torus)
    own_k.wait()

    def stream(number, block, swap=True, both_z=False):
        return Stream(
            torus,
            number,
            block,
            send_sem.at[number],
            recv_sem.at[number],
            (swap_send.at[number], swap_recv.at[number]) if swap else None,
            both_z,
        )

    s_k = stream(0, lambda blk, c: wk.at[blk, c])
    s_v = stream(1, lambda blk, c: wv.at[blk, c])
    s_qa = stream(2, lambda blk, c: qs.at[blk, 0], swap=False)
    s_qb = stream(3, lambda blk, c: qs.at[blk, 1], swap=False, both_z=True)
    rows = 512

    def multiply(stream, weights, to, dy):
        y = lax.rem(torus.y + (dy + NY), NY)
        blocks = pl.ds(pl.multiple_of(y * NZ, NZ), NZ)
        stream.swap_copy(weights.at[blocks, 1 - core], y).wait_recv()

        def one(m, carry):
            at = pl.ds(pl.multiple_of(m * rows, rows), rows)
            w = weights[blocks].reshape(width, weights.shape[3])
            product = jnp.dot(
                hid[at, pl.ds(pl.multiple_of(y * width, width), width)],
                w,
                preferred_element_type=jnp.float32,
            )
            to[at, :] = product if dy == 0 else to[at, :] + product
            return carry

        lax.fori_loop(0, tokens // rows, one, 0)

    mine = pl.ds(pl.multiple_of(core * HD, HD), HD)
    theirs = pl.ds(pl.multiple_of((1 - core) * HD, HD), HD)
    my_pages = pl.ds(pl.multiple_of(core * pages, pages), pages)
    their_pages = pl.ds(pl.multiple_of((1 - core) * pages, pages), pages)

    def to_partner(k, src, dst):
        return pltpu.make_async_remote_copy(
            src_ref=src,
            dst_ref=dst,
            send_sem=half_sem.at[k, 0],
            recv_sem=half_sem.at[k, 1],
            device_id={"rep": 1 - core},
            device_id_type=pl.DeviceIdType.MESH,
        )

    def clip(x, kind, lanes):
        scale = scale_ref[kind : kind + 1, lanes]
        return jnp.clip(x, -8.0 * scale, 7.0 * scale).astype(jnp.bfloat16)

    keys_over = to_partner(0, acc.at[0, :, theirs], kraw)
    values_over = to_partner(1, vout, vbuf.at[my_pages])
    found_copy = pltpu.make_async_copy(found_v, found_ref, local_sem.at[4])

    ring, column = friends(torus)
    place = core * NZ + torus.z

    def peak_copy(refs, slot, k, target):
        return pltpu.make_async_remote_copy(
            src_ref=refs.at[slot],
            dst_ref=refs.at[slot],
            send_sem=peak_sem.at[k, 0],
            recv_sem=peak_sem.at[k, 1],
            device_id={"seq": target[0], "rep": target[1]},
            device_id_type=pl.DeviceIdType.MESH,
        )

    def tell(refs, slot, k, peers):
        for target in peers:
            peak_copy(refs, slot, k, target).start()

    def heard(refs, k, peers):
        return peak_copy(refs, pl.ds(0, len(peers)), k, peers[0])

    q_lag = QUERY_LAG
    for i in range(q_lag + STEPS_GATHER):
        if i == 0:
            own_v.wait()
        if i == q_lag:
            for copy in own_q:
                copy.wait()
        for stream_i, start in ((s_k, 0), (s_v, 1), (s_qa, q_lag), (s_qb, q_lag)):
            if i == 5 and stream_i is s_qa:
                for copy in hid_copies:
                    copy.wait()
                multiply(s_k, wk, acc.at[0], 0)
            if 0 <= i - start < STEPS_GATHER:
                stream_i.step(i - start)
        if i == 0:
            found_v[...] = find_pages(table_ref[...], length_ref[...])
            for kind in range(2):
                fresh_kv[kind] = (
                    new_ref[:, :, kind, :].astype(jnp.float32).reshape(steps_reqs, columns)
                )
        if i == 4:
            found_copy.start()
        if i == 5:
            multiply(s_k, wk, acc.at[0], 1)
            multiply(s_k, wk, acc.at[0], -1)
        if i == 6:
            multiply(s_k, wk, acc.at[0], 2)
            mz[place] = jnp.max(jnp.abs(acc[0]), axis=0, keepdims=True)
            tell(mz, place, 0, ring)
            keys_over.start()
            multiply(s_v, wv, acc.at[1], 0)
        if i == 7:
            multiply(s_v, wv, acc.at[1], 1)
            multiply(s_v, wv, acc.at[1], -1)
        if i == 8:
            heard(mz, 0, ring).wait_recv()
            my[torus.y] = jnp.max(mz[...], axis=0)
            tell(my, torus.y, 1, column)
            multiply(s_v, wv, acc.at[1], 2)
            vout[...] = clip(acc[1, :, theirs], 1, theirs).reshape(vout.shape)
            values_over.start()
            vbuf[my_pages] = clip(acc[1, :, mine], 1, mine).reshape(vout.shape)
    found_copy.wait()
    heard(my, 1, column).wait_recv()
    peak = jnp.max(my[...], axis=0)
    smooth_ref[...] = jnp.sqrt(peak + EPSILON)
    my_smooth = smooth_ref[:, mine]

    def queries_of(g):
        return jnp.concatenate(
            [
                (
                    qs[g, :, :, h * HD : (h + 1) * HD]
                    .reshape(steps_reqs, HD)
                    .astype(jnp.float32)
                    * my_smooth
                ).astype(jnp.bfloat16)
                for h in range(heads)
            ],
            axis=0,
        )

    across = heads * steps_reqs
    lane = lax.broadcasted_iota(jnp.int32, (PAGE, across), 1)
    key = lax.broadcasted_iota(jnp.int32, (PAGE, across), 0)
    request = lane % 8

    kbuf[my_pages] = clip(acc[0, :, mine] / my_smooth, 0, mine).reshape(vout.shape)
    keys_over.wait_recv()
    kbuf[their_pages] = clip(kraw[...] / my_smooth, 0, mine).reshape(vout.shape)
    to_partner(1, vout, vbuf.at[their_pages]).wait_recv()

    def job_of(g):
        keys, values, masks = [], [], []
        for e in range(SLOTS):
            who, page, count = (found_ref[SLOTS * f + e, g * 8] for f in range(3))
            keys.append(kbuf[page])
            values.append(vbuf[page])
            masks.append((request == who) & (key < count))
        return (
            jnp.concatenate(keys, axis=0),
            jnp.concatenate(values, axis=0),
            queries_of(g),
            jnp.concatenate(masks, axis=0),
        )

    def attend_at(*places):
        groups = [torus.at(dy, dz) for dy, dz in places]
        for g, found in zip(groups, attend([job_of(g) for g in groups])):
            partials.keep(g, *found)

    partials = Partials(
        torus, part, stat, out, out_stat, got, got_stat, part_send, part_recv
    )

    def write_cache(quarter):
        def chore():
            at = pl.ds(quarter * (tokens // 4), tokens // 4)
            every = slice(None)
            cache_ref[at] = jnp.stack(
                [
                    clip(acc[0, at, :] / smooth_ref[...], 0, every),
                    clip(acc[1, at, :], 1, every),
                ],
                axis=1,
            )

        return chore

    def attend_fresh():
        mask = (key % 8 == request) & (key // 8 <= (lane // 8) % (steps_reqs // 8))
        job = (
            clip(fresh_kv[0, :, mine] / my_smooth, 0, mine),
            clip(fresh_kv[1, :, mine], 1, mine),
            queries_of(me),
            mask,
        )
        partials.keep(CHIPS, *attend([job])[0])

    chores = [*(write_cache(quarter) for quarter in range(4)), attend_fresh]

    @pl.when(core == 0)
    def _():
        partials.y_first(attend_at, chores)

    @pl.when(core == 1)
    def _():
        partials.z_first(attend_at, chores)

    top, total, summed = partials.kept(me)
    done = (summed / total).T.astype(jnp.bfloat16)
    for h in range(heads):
        att_out[:, h * HD : (h + 1) * HD] = done[h * steps_reqs : (h + 1) * steps_reqs]
    own_att = pl.ds(pl.multiple_of(core * half_q, half_q), half_q)
    last = to_partner(2, att_out, att_ref.at[:, own_att])
    last.start()
    att_ref[:, own_att] = att_out[...]

    for s, refs in ((s_k, wk), (s_v, wv)):
        s.sent_copy(refs.at[pl.ds(0, CHIPS - 1), core]).wait_send()
        s.swap_copy(refs.at[:, core]).wait_send()
    s_qa.sent_copy(qs.at[pl.ds(0, CHIPS - 1), 0]).wait_send()
    s_qb.sent_copy(qs.at[pl.ds(0, CHIPS - 1), 1]).wait_send()
    heard(mz, 0, ring).wait_send()
    heard(my, 1, column).wait_send()
    keys_over.wait_send()
    values_over.wait_send()
    for k, refs in enumerate((out, out_stat)):
        pltpu.make_async_remote_copy(
            src_ref=refs.at[pl.ds(0, CHIPS - 1)],
            dst_ref=refs.at[pl.ds(0, CHIPS - 1)],
            send_sem=part_send.at[k],
            recv_sem=part_recv.at[k, 0, 0, 0],
            device_id={"rep": 1 - core},
            device_id_type=pl.DeviceIdType.MESH,
        ).wait_send()
    last.wait()


def decode(hidden, key_weight, value_weight, queries, group_scale, new_kv, table, lengths):
    tokens, depth = hidden.shape
    rows, columns = key_weight.shape
    step_reqs, q_columns = queries.shape
    pages = tokens // PAGE
    across = q_columns // 2 // HD * step_reqs
    bf16, f32 = jnp.bfloat16, jnp.float32
    any_spec = pl.BlockSpec(memory_space=pl.ANY)
    vmem = pl.BlockSpec(memory_space=pltpu.VMEM)
    return pl.pallas_call(
        decode_kernel,
        out_shape=(
            jax.ShapeDtypeStruct((tokens, 2, columns), bf16),
            jax.ShapeDtypeStruct((1, columns), f32),
            jax.ShapeDtypeStruct((step_reqs, q_columns), bf16),
        ),
        in_specs=[any_spec, any_spec, any_spec, any_spec, vmem, vmem, vmem, vmem],
        out_specs=(vmem, vmem, vmem),
        scratch_shapes=[
            pltpu.VMEM((tokens, depth), bf16),
            pltpu.VMEM((CHIPS, 2, rows, columns), bf16),
            pltpu.VMEM((CHIPS, 2, rows, columns), bf16),
            pltpu.VMEM((2 * NZ, 1, columns), f32),
            pltpu.VMEM((NY, 1, columns), f32),
            pltpu.VMEM((CHIPS, 2, step_reqs // 2, q_columns // 2), bf16),
            pltpu.VMEM((2, tokens, columns), f32),
            pltpu.VMEM((tokens, HD), f32),
            pltpu.VMEM((2 * pages, PAGE, HD), bf16),
            pltpu.VMEM((2 * pages, PAGE, HD), bf16),
            pltpu.VMEM((pages, PAGE, HD), bf16),
            pltpu.VMEM((2, step_reqs, columns), f32),
            pltpu.VMEM((3 * SLOTS, lengths.shape[1]), jnp.int32),
            pltpu.SMEM((3 * SLOTS, lengths.shape[1]), jnp.int32),
            pltpu.VMEM((CHIPS + 1, HD, across), f32),
            pltpu.VMEM((CHIPS + 1, 2, across), f32),
            pltpu.VMEM((CHIPS, HD, across), bf16),
            pltpu.VMEM((CHIPS, 2, across), f32),
            pltpu.VMEM((2, 2, CHIPS, HD, across), bf16),
            pltpu.VMEM((2, 2, CHIPS, 2, across), f32),
            pltpu.VMEM((step_reqs, q_columns // 2), bf16),
            pltpu.SemaphoreType.DMA((5,)),
            pltpu.SemaphoreType.DMA((4,)),
            pltpu.SemaphoreType.DMA((4,)),
            pltpu.SemaphoreType.DMA((4, CHIPS)),
            pltpu.SemaphoreType.DMA((2,)),
            pltpu.SemaphoreType.DMA((2, NY)),
            pltpu.SemaphoreType.DMA((2, 2)),
            pltpu.SemaphoreType.DMA((3, 2)),
            pltpu.SemaphoreType.DMA((2,)),
            pltpu.SemaphoreType.DMA((2, 2, 2, CHIPS)),
        ],
        compiler_params=pltpu.CompilerParams(
            collective_id=0, has_side_effects=True, vmem_limit_bytes=60 * 2**20
        ),
        name="decode",
    )(hidden, key_weight, value_weight, queries, group_scale, new_kv, table, lengths)


def finish_kernel(*refs):
    outputs = len(refs) // 3
    sem = refs[-1]
    pieces = []
    for src, dst, via in zip(refs[:outputs], refs[outputs:], refs[2 * outputs :]):
        count = 4 if len(src.shape) == 3 else 1
        rows = src.shape[0] // count
        pieces += [
            tuple(r.at[pl.ds(k * rows, rows)] for r in (src, via, dst)) for k in range(count)
        ]
    legs = []
    for k, (src, via, dst) in enumerate(pieces):
        legs.append(
            (
                pltpu.make_async_copy(src, via, sem.at[k, 0]),
                pltpu.make_async_copy(via, dst, sem.at[k, 1]),
            )
        )
    for first, _ in legs:
        first.start()
    for first, second in legs:
        first.wait()
        second.start()
    for _, second in legs:
        second.wait()


def finish(*arrays):
    any_spec = pl.BlockSpec(memory_space=pl.ANY)
    return pl.pallas_call(
        finish_kernel,
        out_shape=tuple(jax.ShapeDtypeStruct(a.shape, a.dtype) for a in arrays),
        in_specs=[any_spec] * len(arrays),
        out_specs=(any_spec,) * len(arrays),
        scratch_shapes=[
            *(pltpu.VMEM(a.shape, a.dtype) for a in arrays),
            pltpu.SemaphoreType.DMA((6, 2)),
        ],
        name="finish",
    )(*arrays)


def on_device(
    hidden, key_weight, value_weight, group_scale, new_kv, decode_query, page_table, lengths
):
    steps, requests, q_columns = decode_query.shape
    columns = key_weight.shape[1]
    kv_cache, smoothing, attention = finish(
        *decode(
            hidden,
            key_weight,
            value_weight,
            decode_query.reshape(steps * requests, q_columns),
            group_scale,
            new_kv,
            page_table.T,
            lengths.reshape(1, -1),
        )
    )
    return (
        kv_cache,
        smoothing.reshape(columns),
        attention.reshape(steps, requests, q_columns),
    )


def solution(mesh):
    placed = (
        P(("seq", "rep"), None),
        P(("seq", "rep"), "head"),
        P(("seq", "rep"), "head"),
        P(None, "head"),
        P(None, "seq", None, "head"),
        P(None, "seq", "head"),
        P(),
        P(),
    )
    return jax.shard_map(
        on_device,
        mesh=mesh,
        in_specs=placed,
        out_specs=(P(("seq", "rep"), None, "head"), P("head"), P(None, "seq", "head")),
        check_vma=False,
    )
```
